256 devices in a mesh: band: 8 (over z), ga: 32 (over x, y, core).
Axes of the slice: x: 4, y: 4, z: 8, core: 2. Of those that a mesh axis runs over, the one named last changes fastest.
Arguments:
- coeffs: float32 [2, 8, 73728], P(None, 'band', 'ga'), may hold values from -8 to 8
- cell_map: int32 [73728], P('ga'), may hold values from 0 to 27647, as said below
- potential: float32 [96, 96, 96], P(None, 'ga'), may hold values from -2 to 1
- projectors: float32 [2, 64, 73728], P(None, None, 'ga'), may hold values from -6 to 6
- strengths: float32 [8, 8, 8], replicated, may hold values from -2 to 2
- proj_atom: int32 [64], replicated, may hold values from 0 to 7, as said below
- proj_chan: int32 [64], replicated, may hold values from 0 to 7, as said below
Outputs:
- new_bands: float32 [2, 8, 73728], P(None, 'band', 'ga')
- energy: float32 [8], P('band')
- residual_norm: float32 [8], P('band')
- correlation: float32 [2, 8, 8], P(None, 'band')
- subspace: float32 [2, 8, 8], P(None, 'band')
The draws below stay inside these ranges and needn't reach their ends.
Inputs may be any that keep to these rules, and one draw needn't show every extreme that they name: `cell_map`: in block d (entries d * 2304 to (d + 1) * 2304 - 1) the entries are distinct cells (i * 96 + y) * 96 + z of grid planes x = d + 32 * i. `proj_atom`: each pair of atom and channel belongs to exactly one projector. `proj_chan`: each pair of atom and channel belongs to exactly one projector.
All inputs are finite; a program needn't handle non-finite values.
Results may differ from the reference program's by a relative error of at most 0.0002.
Values sent between devices are 32-bit elements; how exact they have to be, the bound alone decides.
A program may use at most 64 MiB of HBM per device.

```python
import jax
import jax.numpy as jnp
from jax import lax

NG = 96
PW_DEV = 2304
NATOM = 8
NCH = 8
NPROJ = 64
PW_BLOCKS = 32
NPW = 73728
NBANDS = 8


kin_unit = 0.02


def signed_freq_drawn(index_arr):
    return jnp.where(index_arr < NG // 2, index_arr, index_arr - NG)


def sphere_cells(key):
    block_count = NPW // PW_DEV
    planes = NG // block_count
    slab_cells = planes * NG * NG
    cell_ids = jnp.arange(slab_cells, dtype=jnp.int32)
    plane_num = cell_ids // (NG * NG)
    freq_y = signed_freq_drawn(cell_ids // NG % NG)
    freq_z = signed_freq_drawn(cell_ids % NG)

    def pick_cells(block_key, block_num):
        freq_x = signed_freq_drawn(block_num + block_count * plane_num)
        radius_sq = freq_x * freq_x + freq_y * freq_y + freq_z * freq_z
        jitter_key, order_key = jax.random.split(block_key)
        jitter_score = radius_sq * 8 + jax.random.randint(jitter_key, (slab_cells,), 0, 192, dtype=jnp.int32)
        chosen = jnp.argsort(jitter_score, stable=True)[:PW_DEV]
        shuffle = jax.random.permutation(order_key, PW_DEV)
        return chosen[shuffle].astype(jnp.int32)
    block_keys = jax.random.split(key, block_count)
    block_nums = jnp.arange(block_count, dtype=jnp.int32)
    return jax.vmap(pick_cells)(block_keys, block_nums).reshape(NPW)


def cell_energy(cells):
    block_count = NPW // PW_DEV
    owner = jnp.arange(NPW, dtype=jnp.int32) // PW_DEV
    freq_x = signed_freq_drawn(owner + block_count * (cells // (NG * NG)))
    freq_y = signed_freq_drawn(cells // NG % NG)
    freq_z = signed_freq_drawn(cells % NG)
    return kin_unit * (freq_x * freq_x + freq_y * freq_y + freq_z * freq_z).astype(jnp.float32)


def projector_values(key):
    cells = sphere_cells(jax.random.fold_in(key, 11))
    energy = cell_energy(cells)
    shape_key, scale_key = jax.random.split(jax.random.fold_in(key, 23))
    raw_values = jax.random.truncated_normal(shape_key, -6.0, 6.0, (2, NPROJ, NPW), jnp.float32)
    row_scale = jnp.exp(jax.random.uniform(scale_key, (NPROJ,), jnp.float32, -0.7, 0.7))
    shaped = raw_values * row_scale[None, :, None] / (1.0 + energy / 8.0)[None, None, :]
    return (jnp.clip(shaped, -6.0, 6.0), energy)


def draw_cell_map(key, part):
    return sphere_cells(jax.random.fold_in(key, 11))


def draw_projectors(key, part):
    return projector_values(key)[0]


def draw_coeffs(key, part):
    projectors, energy = projector_values(key)
    noise_key, mix_key, common_key, scale_key = jax.random.split(jax.random.fold_in(key, 37), 4)
    envelope = 1.0 / (1.0 + energy / 4.0)
    noise = jax.random.truncated_normal(noise_key, -6.0, 6.0, (2, NBANDS, NPW), jnp.float32)
    mixing = jax.random.truncated_normal(mix_key, -4.0, 4.0, (2, NBANDS, NPROJ), jnp.float32) * (0.5 / NPROJ ** 0.5)
    along_re = jnp.einsum('bp,pg->bg', mixing[0], projectors[0]) - jnp.einsum('bp,pg->bg', mixing[1], projectors[1])
    along_im = jnp.einsum('bp,pg->bg', mixing[0], projectors[1]) + jnp.einsum('bp,pg->bg', mixing[1], projectors[0])
    values = noise * envelope[None, None, :] + jnp.stack([along_re, along_im])
    return jnp.clip(values, -8.0, 8.0)


def projector_slots(key):
    ordering = jax.random.permutation(jax.random.fold_in(key, 51), NPROJ).astype(jnp.int32)
    return (ordering // NCH, ordering % NCH)


def draw_proj_atom(key, part):
    return projector_slots(key)[0]


def draw_proj_chan(key, part):
    return projector_slots(key)[1]


def shard_levels(key, extent, cuts, low, top_value):
    loudness = 1.0
    for axis_at, shards_of in cuts:
        heights = jax.random.uniform(jax.random.fold_in(jax.random.fold_in(key, 6), axis_at), (shards_of,), jnp.float32, low / len(cuts), top_value / len(cuts))
        loudness = loudness * jnp.repeat(jnp.exp(heights), extent[axis_at] // shards_of).reshape((-1,) + (1,) * (len(extent) - 1 - axis_at))
    return loudness


def setup_inputs(seed: int = 0) -> dict:
    arg_keys = jax.random.split(jax.random.key(seed), 8)
    coeffs = draw_coeffs(jax.random.fold_in(arg_keys[7], 71), 0)
    cell_map = draw_cell_map(jax.random.fold_in(arg_keys[7], 71), 0)
    potential = jnp.clip(-2.0 + 3.0 * jax.random.uniform(arg_keys[2], (NG, NG, NG), jnp.float32) ** shard_levels(arg_keys[2], (NG, NG, NG), ((1, 32),), -0.2, 0.2), -2.0, 1.0)
    projectors = draw_projectors(jax.random.fold_in(arg_keys[7], 71), 0)
    strengths = jnp.clip(jax.random.uniform(arg_keys[4], (NATOM, NCH, NCH), jnp.float32, -2.0, 2.0), -2.0, 2.0)
    proj_atom = draw_proj_atom(jax.random.fold_in(arg_keys[7], 71), 0)
    proj_chan = draw_proj_chan(jax.random.fold_in(arg_keys[7], 71), 0)
    return dict(coeffs=coeffs, cell_map=cell_map, potential=potential, projectors=projectors, strengths=strengths, proj_atom=proj_atom, proj_chan=proj_chan)


top_precision = lax.Precision.HIGHEST
kin_unit = 0.02
small_eps = 1e-6


def signed_freq(index_arr):
    return jnp.where(index_arr < NG // 2, index_arr, index_arr - NG)


def coupling_matrix(proj_atom, proj_chan, strengths):
    symmetric = 0.5 * (strengths + jnp.swapaxes(strengths, 1, 2))
    atom_hot = (proj_atom[:, None] == jnp.arange(NATOM, dtype=jnp.int32)[None, :]).astype(jnp.float32)
    chan_hot = (proj_chan[:, None] == jnp.arange(NCH, dtype=jnp.int32)[None, :]).astype(jnp.float32)
    rows_d = jnp.einsum("pa,pc,acd->pd", atom_hot, chan_hot, symmetric, precision=top_precision)
    same_atom = jnp.dot(atom_hot, atom_hot.T, precision=top_precision, preferred_element_type=jnp.float32)
    return same_atom * jnp.dot(rows_d, chan_hot.T, precision=top_precision, preferred_element_type=jnp.float32)


def band_dot(left_vec, right_vec, weight):
    return jnp.sum(left_vec * right_vec * weight, axis=(0, 2)) / NPW


def per_band(values):
    return values[None, :, None]


def precondition(residual, kinetic, kin_level):
    x_ratio = kinetic[None, :] / (1.5 * kin_level[:, None] + 1.0)
    numer_poly = 27.0 + x_ratio * (18.0 + x_ratio * (12.0 + 8.0 * x_ratio))
    square = x_ratio * x_ratio
    return residual * (numer_poly / (numer_poly + 16.0 * square * square))[None]


def pair_products(left_vec, right_vec):
    def contract(first_part, second_part):
        return jnp.einsum("bg,cg->bc", first_part, second_part, precision=top_precision)
    real_part = contract(left_vec[0], right_vec[0]) + contract(left_vec[1], right_vec[1])
    imag_part = contract(left_vec[0], right_vec[1]) - contract(left_vec[1], right_vec[0])
    return jnp.stack([real_part, imag_part])


def local_one(vector, flat_cells, potential):
    values = vector[0] + 1j * vector[1]
    grid_g = jnp.zeros((NG * NG * NG,), values.dtype).at[flat_cells].set(values)
    space = jnp.fft.ifftn(grid_g.reshape(NG, NG, NG)) * potential
    back = jnp.fft.fftn(space).reshape(NG * NG * NG)[flat_cells]
    return jnp.stack([jnp.real(back), jnp.imag(back)])


def reference(coeffs, cell_map, potential, projectors, strengths, proj_atom, proj_chan):
    owner = jnp.arange(NPW, dtype=jnp.int32) // PW_DEV
    x_index = owner + PW_BLOCKS * (cell_map // (NG * NG))
    y_index = (cell_map // NG) % NG
    z_index = cell_map % NG
    flat_cells = (x_index * NG + y_index) * NG + z_index
    freq_x = signed_freq(x_index)
    freq_y = signed_freq(y_index)
    freq_z = signed_freq(z_index)
    kinetic = kin_unit * (freq_x * freq_x + freq_y * freq_y + freq_z * freq_z).astype(jnp.float32)
    kin_weight = kinetic[None, None, :]
    coupling = coupling_matrix(proj_atom, proj_chan, strengths)

    def contract(first_part, second_part):
        return jnp.einsum("pg,bg->pb", first_part, second_part, precision=top_precision)

    def spread(weights, proj_table):
        return jnp.einsum("pb,pg->bg", weights, proj_table, precision=top_precision)

    def apply_h(vectors):
        local_term = lax.map(lambda vector: local_one(vector, flat_cells, potential), jnp.swapaxes(vectors, 0, 1))
        local_term = jnp.swapaxes(local_term, 0, 1)
        proj_re = (contract(projectors[0], vectors[0]) + contract(projectors[1], vectors[1])) / NPW
        proj_im = (contract(projectors[0], vectors[1]) - contract(projectors[1], vectors[0])) / NPW
        mixed_re = jnp.dot(coupling, proj_re, precision=top_precision, preferred_element_type=jnp.float32)
        mixed_im = jnp.dot(coupling, proj_im, precision=top_precision, preferred_element_type=jnp.float32)
        out_re = spread(mixed_re, projectors[0]) - spread(mixed_im, projectors[1])
        out_im = spread(mixed_re, projectors[1]) + spread(mixed_im, projectors[0])
        return kin_weight * vectors + local_term + jnp.stack([out_re, out_im])

    h_zero = apply_h(coeffs)
    eps_zero = band_dot(coeffs, h_zero, 1.0) / (band_dot(coeffs, coeffs, 1.0) + small_eps)
    r_zero = h_zero - per_band(eps_zero) * coeffs
    level_zero = band_dot(r_zero, r_zero, kin_weight) / (band_dot(r_zero, r_zero, 1.0) + small_eps)
    p_zero = precondition(r_zero, kinetic, level_zero)
    g_zero = apply_h(p_zero)
    q_zero = g_zero - per_band(eps_zero) * p_zero
    lam_zero = -band_dot(r_zero, q_zero, 1.0) / (band_dot(q_zero, q_zero, 1.0) + small_eps)
    psi_one = coeffs + per_band(lam_zero) * p_zero
    h_one = h_zero + per_band(lam_zero) * g_zero
    eps_one = band_dot(psi_one, h_one, 1.0) / (band_dot(psi_one, psi_one, 1.0) + small_eps)
    r_one = h_one - per_band(eps_one) * psi_one
    change = r_zero - r_one
    weight_one = band_dot(r_zero, change, 1.0) / (band_dot(change, change, 1.0) + small_eps)
    step_mid = weight_one * lam_zero
    psi_mid = coeffs + per_band(step_mid) * p_zero
    h_mid = h_zero + per_band(step_mid) * g_zero
    r_mid = r_zero - per_band(weight_one) * change
    eps_mid = band_dot(psi_mid, h_mid, 1.0) / (band_dot(psi_mid, psi_mid, 1.0) + small_eps)
    level_mid = band_dot(r_mid, r_mid, kin_weight) / (band_dot(r_mid, r_mid, 1.0) + small_eps)
    p_one = precondition(r_mid, kinetic, level_mid)
    g_one = apply_h(p_one)
    q_one = g_one - per_band(eps_mid) * p_one
    lam_one = -band_dot(r_mid, q_one, 1.0) / (band_dot(q_one, q_one, 1.0) + small_eps)
    new_bands = psi_mid + per_band(lam_one) * p_one
    new_ham = h_mid + per_band(lam_one) * g_one
    norm_new = band_dot(new_bands, new_bands, 1.0) + small_eps
    energy = band_dot(new_bands, new_ham, 1.0) / norm_new
    residual = new_ham - per_band(energy) * new_bands
    residual_norm = band_dot(residual, residual, 1.0) / norm_new
    correlation = pair_products(new_bands, new_bands) / NPW
    subspace = pair_products(new_bands, new_ham) / NPW
    return new_bands, energy, residual_norm, correlation, subspace
```

```python
import functools

import jax
import jax.numpy as jnp
import numpy as np
from jax import lax
from jax.experimental import pallas as pl
from jax.experimental.pallas import tpu as pltpu
from jax.sharding import PartitionSpec as P

F32 = jnp.float32
BF16 = jnp.bfloat16
HIGHEST = lax.Precision.HIGHEST
MESH = pl.DeviceIdType.MESH
kin_unit = 0.02
small_eps = 1e-06

NN = (((1,), (0,)), ((), ()))
NT = (((1,), (1,)), ((), ()))
TN = (((0,), (0,)), ((), ()))


def parts_of(table, count):
    out = []
    left = np.asarray(table, np.float64)
    for _ in range(count):
        piece = left.astype(np.float32).astype(BF16)
        out.append(piece)
        left = left - piece.astype(np.float64)
    return out


def make_tables(grid_len, groups):
    planes = grid_len // groups
    natural = np.arange(grid_len)
    slab = (natural % groups) * planes + natural // groups

    def angles(rows, cols):
        return 2.0 * np.pi / grid_len * ((rows[:, None] * cols[None, :]) % grid_len)

    z_ang = angles(natural, natural)
    z_tab = np.concatenate([np.cos(z_ang), np.sin(z_ang)], axis=0)
    z_parts = np.concatenate(parts_of(z_tab, 3), axis=0)
    y_ang = angles(slab, natural)
    y_fwd = np.concatenate([np.cos(y_ang), np.sin(y_ang)], axis=1)
    x_cos, x_sin = np.cos(z_ang), np.sin(z_ang)
    x_fwd = np.block([[x_cos, -x_sin], [x_sin, x_cos]])
    x_back = np.block([[x_cos, x_sin], [-x_sin, x_cos]]) / grid_len
    pad = np.zeros((grid_len, 128 - grid_len))
    y_cos, y_sin = np.cos(y_ang), np.sin(y_ang)
    y_back = np.block([[y_cos, pad, -y_sin, pad], [y_sin, pad, y_cos, pad]]) / grid_len**2
    tables = [z_parts]
    for tab in (y_fwd, x_fwd, x_back, y_back):
        tables += parts_of(tab, 2)
    return tables


def dot(a, b, dims=NN):
    return lax.dot_general(a, b, dims, preferred_element_type=F32)


def dot_full(a, b, dims=NN):
    return lax.dot_general(a, b, dims, precision=HIGHEST, preferred_element_type=F32)


def split(x):
    hi = x.astype(BF16)
    return hi, (x - hi.astype(F32)).astype(BF16)


def iota(shape, axis):
    return lax.broadcasted_iota(jnp.int32, shape, axis)


def kernel(sizes, cf, cm, pot, pj, st, pa, pc, zt, yfh, yfl, xfh, xfl, xbh, xbl, ybh, ybl,
           nb_out, small_out,
           at_s, at_g, e_tab, x_hi, x_lo, v_tab, gt_hi, gt_lo, big, coup, vecs, hvec, kin_ref,
           send, recv, row_send, row_recv, gram_send, gram_recv, bands, lam_send, lam_recv,
           send_sem, recv_sem):
    ga_n, band_n, grid_len, total_pw = sizes
    planes = grid_len // ga_n
    me = lax.axis_index("ga")
    my_band = lax.axis_index("band")
    pw = cf.shape[2]
    tiles = pw // 128

    barrier = pltpu.get_barrier_semaphore()

    def greet_ga(k, _):
        pl.semaphore_signal(barrier, inc=1, device_id={"ga": lax.rem(me + k, ga_n)}, device_id_type=MESH)
        return 0

    def greet_band(k, _):
        pl.semaphore_signal(barrier, inc=1, device_id={"band": lax.rem(my_band + k, band_n)}, device_id_type=MESH)
        return 0

    lax.fori_loop(1, ga_n, greet_ga, 0)
    lax.fori_loop(1, band_n, greet_band, 0)

    cells = cm[...]
    py = lax.shift_right_logical(cells * 43691, 22)
    z_idx = cells - py * grid_len
    plane = (py >= grid_len).astype(jnp.int32) + (py >= 2 * grid_len).astype(jnp.int32)
    y_idx = py - plane * grid_len
    x_idx = me + ga_n * plane

    def freq(k):
        return jnp.where(2 * k < grid_len, k, k - grid_len).astype(F32)

    kin = kin_unit * (freq(x_idx) * freq(x_idx) + freq(y_idx) * freq(y_idx) + freq(z_idx) * freq(z_idx))
    kin_ref[...] = kin
    py_pad = plane * 128 + y_idx
    for k in range(tiles):
        lanes = slice(k * 128, k * 128 + 128)
        hot = (iota((3 * grid_len, 128), 0) == py[:, lanes])
        at_s[:, lanes] = jnp.where(hot, 1.0, 0.0).astype(BF16)
        hot = (iota((3 * 128, 128), 0) == py_pad[:, lanes])
        at_g[:, lanes] = jnp.where(hot, 1.0, 0.0).astype(BF16)
    for k in range(0, pw, 256):
        hot = (iota((grid_len, 256), 0) == z_idx[:, k : k + 256])
        got = dot(zt[...], jnp.where(hot, 1.0, 0.0).astype(BF16))
        rows = 2 * grid_len
        e_tab[:, k : k + 256] = got[:rows] + got[rows : 2 * rows] + got[2 * rows :]
    x_hi[...] = jnp.zeros_like(x_hi)
    x_lo[...] = jnp.zeros_like(x_lo)
    v_tab[...] = jnp.zeros_like(v_tab)
    for j in range(planes):
        v_tab[:, j * 128 : j * 128 + grid_len] = pot[:, j, :]

    proj_n = pa.shape[1]
    chans = st.shape[1]
    sym_rows = st[...].reshape(st.shape[0] * chans, chans)
    slot = pa[...] * chans + pc[...]
    hot_p = jnp.where(iota((proj_n, proj_n), 0) == slot, 1.0, 0.0)
    hot_c = jnp.where(iota((chans, proj_n), 0) == pc[...], 1.0, 0.0)
    reach = dot_full(sym_rows, hot_c)
    reach = jnp.where(iota((proj_n, proj_n), 0) // chans == pa[...], reach, 0.0)
    half = 0.5 * (dot_full(hot_p, reach, TN) + dot_full(reach, hot_p, TN))
    coup[...] = jnp.concatenate([half, half], axis=1)

    lane = iota((1, 128), 1)
    lane32 = iota((ga_n, 128), 1)

    def roll(x, by):
        return pltpu.roll(x, by, 1)

    def pack(a, b, c, d, e, f):
        rb, rc, rd, rf = roll(b, 96), roll(c, 64), roll(d, 32), roll(f, 96)
        return (
            jnp.where(lane32 < 96, a, rb),
            jnp.where(lane32 < 64, rb, rc),
            jnp.where(lane32 < 32, rc, rd),
            jnp.where(lane32 < 96, e, rf),
            rf,
        )

    def unpack(t0, t1, t2, t3, t4):
        b = roll(jnp.where(lane32 < 64, t1, t0), 32)
        c = roll(jnp.where(lane32 < 32, t2, t1), 64)
        d = roll(t2, 96)
        f = roll(jnp.where(lane32 < 64, t4, t3), 32)
        return t0, b, c, d, t3, f

    stride = big.shape[0] // 16

    def put_big(block, value):
        big[block * stride : block * stride + ga_n, :] = value

    def exchange(phase):
        def build(d, _):
            send[phase, pl.ds(pl.multiple_of(d * 16, 16), 16), :] = big[pl.ds(d, 16, stride=stride), :]
            return 0

        for d in range(ga_n):
            send[phase, d * 16 : d * 16 + 16, :] = big[pl.ds(d, 16, stride=stride), :]
        mine = pl.ds(pl.multiple_of(me * 16, 16), 16)

        def go(k, _):
            other = lax.rem(me + k, ga_n)
            pltpu.make_async_remote_copy(
                src_ref=send.at[phase, pl.ds(pl.multiple_of(other * 16, 16), 16), :],
                dst_ref=recv.at[phase, mine, :],
                send_sem=send_sem.at[phase],
                recv_sem=recv_sem.at[phase],
                device_id={"ga": other},
                device_id_type=MESH,
            ).start()
            return 0

        lax.fori_loop(1, ga_n, go, 0)
        recv[phase, mine, :] = send[phase, mine, :]

    def wait_exchange(phase):
        span = pl.ds(0, (ga_n - 1) * 16)
        both = pltpu.make_async_remote_copy(
            src_ref=send.at[phase, span, :],
            dst_ref=recv.at[phase, span, :],
            send_sem=send_sem.at[phase],
            recv_sem=recv_sem.at[phase],
            device_id={"ga": lax.rem(me + 1, ga_n)},
            device_id_type=MESH,
        )
        both.wait()

    def got_rows(phase, row):
        return recv[phase, pl.ds(row, ga_n, stride=16), :]

    def spread_rows(ref_send, ref_recv, sem):
        def go(k, _):
            other = lax.rem(me + k, ga_n)
            pltpu.make_async_remote_copy(
                src_ref=ref_send, dst_ref=ref_recv.at[me], send_sem=send_sem.at[sem], recv_sem=recv_sem.at[sem],
                device_id={"ga": other}, device_id_type=MESH,
            ).start()
            return 0

        lax.fori_loop(1, ga_n, go, 0)

    def wait_rows(ref_recv, sem, count, axis, size, mine):
        span = ref_recv.at[pl.ds(0, count)]
        pltpu.make_async_remote_copy(
            src_ref=span, dst_ref=span, send_sem=send_sem.at[sem], recv_sem=recv_sem.at[sem],
            device_id={axis: lax.rem(mine + 1, size)}, device_id_type=MESH,
        ).wait()

    def cell(row, at):
        return jnp.sum(jnp.where(lane == at, row, 0.0), axis=1, keepdims=True)

    def fold(x):
        total = x[:, :128]
        for k in range(1, tiles):
            total = total + x[:, k * 128 : k * 128 + 128]
        return total[0:1] + total[1:2]

    def as_row(folded):
        stack = jnp.concatenate(folded + [jnp.zeros((1, 128), F32)] * (-len(folded) % 8), axis=0)
        col = jnp.sum(stack, axis=1, keepdims=True)
        hit = iota(stack.shape, 0) == iota(stack.shape, 1)
        return jnp.sum(jnp.where(hit, col, 0.0), axis=0, keepdims=True)

    def all_sums(which, folded):
        row_send[which] = as_row(folded)
        spread_rows(row_send.at[which], row_recv.at[which], 6 + which)
        row_recv[which, me] = row_send[which]
        wait_rows(row_recv.at[which], 6 + which, ga_n - 1, "ga", ga_n, me)
        total = jnp.sum(row_recv[which], axis=0)
        return total * (1.0 / total_pw)

    def apply_h(turn, v):
        acc_re = jnp.zeros((proj_n, 128), F32)
        acc_im = jnp.zeros((proj_n, 128), F32)
        for k in range(tiles):
            lanes = slice(k * 128, k * 128 + 128)
            p_re, p_im = pj[0, :, lanes], pj[1, :, lanes]
            v_re, v_im = v[0:1, lanes], v[1:2, lanes]
            acc_re = acc_re + (p_re * v_re + p_im * v_im)
            acc_im = acc_im + (p_re * v_im - p_im * v_re)
        col_re = jnp.sum(acc_re, axis=1, keepdims=True)
        col_im = jnp.sum(acc_im, axis=1, keepdims=True)
        row64, lane64 = iota((proj_n, 128), 0), iota((proj_n, 128), 1)
        diag = jnp.where(lane64 == row64, col_re, jnp.where(lane64 == row64 + proj_n, col_im, 0.0))
        proj_row = jnp.sum(diag, axis=0, keepdims=True)

        for k in range(tiles):
            lanes = slice(k * 128, k * 128 + 128)
            e_c, e_s = e_tab[:grid_len, lanes], e_tab[grid_len:, lanes]
            v_re, v_im = v[0:1, lanes], v[1:2, lanes]
            hi, lo = split(e_c * v_re - e_s * v_im)
            x_hi[:grid_len, lanes] = hi
            x_lo[:grid_len, lanes] = lo
            hi, lo = split(e_s * v_re + e_c * v_im)
            x_hi[128 : 128 + grid_len, lanes] = hi
            x_lo[128 : 128 + grid_len, lanes] = lo
        t_all = dot(at_s[...], x_hi[...], NT) + dot(at_s[...], x_lo[...], NT)

        u = []
        for i in range(planes):
            t_i = t_all[i * grid_len : (i + 1) * grid_len]
            turned = jnp.concatenate([-t_i[:, 128:], t_i[:, :128]], axis=1)
            hi, lo = split(jnp.concatenate([t_i, turned], axis=0))
            u.append(dot(yfh[...], hi) + dot(yfh[...], lo) + dot(yfl[...], hi))
        for j in range(planes):
            rows = slice(j * ga_n, (j + 1) * ga_n)
            six = []
            for i in range(planes):
                six += [u[i][rows, :128], u[i][rows, 128:]]
            for t, piece in enumerate(pack(*six)):
                put_big(j * 5 + t, piece)
        put_big(15, jnp.broadcast_to(proj_row, (ga_n, 128)))
        if turn == 0:
            pl.semaphore_wait(barrier, ga_n - 1 + band_n - 1)
        exchange(2 * turn)
        norm_row = None
        if turn == 0:
            norm_row = as_row([fold(v * v), fold(v * v * kin_ref[...])])
        wait_exchange(2 * turn)

        cols = []
        for j in range(planes):
            pieces = unpack(*[got_rows(2 * turn, j * 5 + t) for t in range(5)])
            cols.append(jnp.concatenate(pieces[0::2] + pieces[1::2], axis=0))
        hi, lo = split(jnp.concatenate(cols, axis=1))
        w = dot(xfh[...], hi) + dot(xfh[...], lo) + dot(xfl[...], hi)
        w_re, w_im = w[:grid_len], w[grid_len:]
        vw_re, vw_im = v_tab[...] * w_re, v_tab[...] * w_im
        if turn == 0:
            dens = jnp.sum(vw_re * w_re + vw_im * w_im, axis=0, keepdims=True)
            dens = dens[:, :128] + dens[:, 128:256] + dens[:, 256:]
            dens = jnp.sum(dens, axis=1, keepdims=True)
            put_big(15, jnp.broadcast_to(jnp.where(lane == 2, dens, norm_row), (ga_n, 128)))
        hi, lo = split(jnp.concatenate([vw_re, vw_im], axis=0))
        back = dot(xbh[...], hi) + dot(xbh[...], lo) + dot(xbl[...], hi)
        for j in range(planes):
            lanes = slice(j * 128, j * 128 + 128)
            six = []
            for i in range(planes):
                for c in range(2):
                    at = c * grid_len + i * ga_n
                    six.append(back[at : at + ga_n, lanes])
            for t, piece in enumerate(pack(*six)):
                put_big(j * 5 + t, piece)
        exchange(2 * turn + 1)

        tot = jnp.sum(got_rows(2 * turn, 15), axis=0, keepdims=True) * (1.0 / total_pw)
        prod = coup[...] * tot
        mix_re = jnp.sum(jnp.where(lane64 < proj_n, prod, 0.0), axis=1, keepdims=True)
        mix_im = jnp.sum(jnp.where(lane64 < proj_n, 0.0, prod), axis=1, keepdims=True)
        c_n = None
        if turn == 0:
            diag_row = jnp.where(lane64 == row64, mix_re, jnp.where(lane64 == row64 + proj_n, mix_im, 0.0))
            c_n = jnp.sum(jnp.sum(diag_row, axis=0, keepdims=True) * tot, axis=1, keepdims=True)
        for k in range(tiles):
            lanes = slice(k * 128, k * 128 + 128)
            p_re, p_im = pj[0, :, lanes], pj[1, :, lanes]
            n_re = jnp.sum(p_re * mix_re - p_im * mix_im, axis=0, keepdims=True)
            n_im = jnp.sum(p_im * mix_re + p_re * mix_im, axis=0, keepdims=True)
            hvec[:, lanes] = jnp.concatenate([n_re, n_im], axis=0) + kin_ref[:, lanes] * v[:, lanes]
        wait_exchange(2 * turn + 1)

        zs = [[None] * planes for _ in range(2 * planes)]
        for j in range(planes):
            pieces = unpack(*[got_rows(2 * turn + 1, j * 5 + t) for t in range(5)])
            for n, piece in enumerate(pieces):
                zs[n][j] = piece
        for i in range(planes):
            stack = jnp.concatenate(zs[2 * i] + zs[2 * i + 1], axis=0)
            hi, lo = split(stack.T)
            out = dot(hi, ybh[...]) + dot(lo, ybh[...]) + dot(hi, ybl[...])
            for c in range(2):
                hi, lo = split(out[:grid_len, c * 128 : c * 128 + 128])
                gt_hi[c * grid_len : (c + 1) * grid_len, i * 128 : i * 128 + 128] = hi
                gt_lo[c * grid_len : (c + 1) * grid_len, i * 128 : i * 128 + 128] = lo
        for k in range(0, pw, 256):
            lanes = slice(k, k + 256)
            q = dot(gt_hi[...], at_g[:, lanes]) + dot(gt_lo[...], at_g[:, lanes])
            q_re, q_im = q[:grid_len], q[grid_len:]
            e_c, e_s = e_tab[:grid_len, lanes], e_tab[grid_len:, lanes]
            l_re = jnp.sum(e_c * q_re + e_s * q_im, axis=0, keepdims=True)
            l_im = jnp.sum(e_c * q_im - e_s * q_re, axis=0, keepdims=True)
            hvec[:, lanes] = hvec[:, lanes] + jnp.concatenate([l_re, l_im], axis=0)
        return c_n

    def precondition(r, level):
        ratio = kin_ref[...] / (1.5 * level + 1.0)
        numer = 27.0 + ratio * (18.0 + ratio * (12.0 + 8.0 * ratio))
        square = ratio * ratio
        return r * (numer / (numer + 16.0 * square * square))

    eps = small_eps

    vecs[0] = jnp.concatenate([cf[0], cf[1]], axis=0)
    c_n = apply_h(0, vecs[0])
    tot = jnp.sum(got_rows(1, 15), axis=0, keepdims=True) * (1.0 / total_pw)
    guess_cc = cell(tot, 0)
    guess = (cell(tot, 1) + cell(tot, 2) * (1.0 / grid_len**3) + c_n) / (guess_cc + eps)
    c = vecs[0]
    h0 = hvec[...]
    s = h0 - guess * c
    kc, ks = kin_ref[...] * c, kin_ref[...] * s
    tot = all_sums(0, [fold(c * c), fold(c * s), fold(s * s), fold(kc * c), fold(kc * s), fold(ks * s)])
    cc, cs, ss, kcc, kcs, kss = [cell(tot, n) for n in range(6)]
    shift = (cs - guess * eps) / (cc + eps)
    e0 = guess + shift
    r0 = s - shift * c
    rr = ss - 2.0 * shift * cs + shift * shift * cc
    krr = kss - 2.0 * shift * kcs + shift * shift * kcc
    rc = cs - shift * cc
    krc = kcs - shift * kcc
    p0 = precondition(r0, krr / (rr + eps))
    vecs[1] = r0
    vecs[2] = p0
    vecs[3] = h0

    apply_h(1, vecs[2])
    c, r0, p0, h0 = vecs[0], vecs[1], vecs[2], vecs[3]
    g0 = hvec[...]
    q0 = g0 - e0 * p0
    pairs = [(r0, q0), (r0, p0), (q0, q0), (q0, c), (q0, p0), (c, p0), (p0, p0)]
    prods = [a * b for a, b in pairs]
    tot = all_sums(1, [fold(x) for x in prods] + [fold(x * kin_ref[...]) for x in prods])
    rq, rp, qq, qc, qp, cp, pp = [cell(tot, n) for n in range(7)]
    krq, krp, kqq, kqc, kqp, kcp, kpp = [cell(tot, n) for n in range(7, 14)]
    l0 = -rq / (qq + eps)
    bb = cc + 2.0 * l0 * cp + l0 * l0 * pp
    b_rho = rc + l0 * (qc + rp) + l0 * l0 * qp
    d1 = (b_rho - e0 * eps) / (bb + eps)
    fa, fb, fc = -l0, d1, d1 * l0
    r_dr = fa * rq + fb * rc + fc * rp
    dr_dr = fa * fa * qq + fb * fb * cc + fc * fc * pp + 2.0 * (fa * fb * qc + fa * fc * qp + fb * fc * cp)
    kr_dr = fa * krq + fb * krc + fc * krp
    kdr_dr = fa * fa * kqq + fb * fb * kcc + fc * fc * kpp + 2.0 * (fa * fb * kqc + fa * fc * kqp + fb * fc * kcp)
    wt = r_dr / (dr_dr + eps)
    lm = wt * l0
    bmbm = cc + 2.0 * lm * cp + lm * lm * pp
    bm_rho = rc + lm * (qc + rp) + lm * lm * qp
    dm = (bm_rho - e0 * eps) / (bmbm + eps)
    em = e0 + dm
    mm = rr - 2.0 * wt * r_dr + wt * wt * dr_dr
    kmm = krr - 2.0 * wt * kr_dr + wt * wt * kdr_dr
    bm = c + lm * p0
    hm = h0 + lm * g0
    rm = r0 - wt * (fa * q0 + fb * c + fc * p0)
    sm = r0 + lm * q0 - dm * bm
    p1 = precondition(rm, kmm / (mm + eps))
    vecs[4] = bm
    vecs[5] = hm
    vecs[6] = rm
    vecs[7] = sm
    vecs[8] = p1
    slot8 = pl.ds(pl.multiple_of(my_band * 8, 8), 8)
    bands[slot8, :] = jnp.concatenate([bm, p1, bm, p1], axis=0)

    def send_band(k, _):
        other = lax.rem(my_band + k, band_n)
        pltpu.make_async_remote_copy(
            src_ref=bands.at[slot8, :], dst_ref=bands.at[slot8, :], send_sem=send_sem.at[9], recv_sem=recv_sem.at[9],
            device_id={"band": other}, device_id_type=MESH,
        ).start()
        return 0

    lax.fori_loop(1, band_n, send_band, 0)

    apply_h(2, vecs[8])
    bm, hm, rm, sm, p1 = vecs[4], vecs[5], vecs[6], vecs[7], vecs[8]
    g1 = hvec[...]
    q1 = g1 - em * p1
    span = bands.at[pl.ds(0, (band_n - 1) * 8), :]
    pltpu.make_async_remote_copy(
        src_ref=span, dst_ref=span, send_sem=send_sem.at[9], recv_sem=recv_sem.at[9],
        device_id={"band": lax.rem(my_band + 1, band_n)}, device_id_type=MESH,
    ).wait()
    left = jnp.concatenate([bm, p1, hm, g1], axis=0)
    gram = dot_full(left, bands[...], NT)
    wide = (band_n * 8, 128)
    moved = iota(wide, 0) % 8 * band_n + iota(wide, 0) // 8
    gram = dot_full(gram, jnp.where(moved == iota(wide, 1), 1.0, 0.0))
    pairs = [(rm, q1), (q1, q1), (sm, sm), (sm, q1), (sm, bm), (sm, p1), (q1, bm), (q1, p1), (bm, bm), (bm, p1), (p1, p1)]
    row = as_row([fold(a * b) for a, b in pairs])
    gram_send[:8, :] = gram
    gram_send[8:, :] = jnp.broadcast_to(row, (8, 128))
    spread_rows(gram_send, gram_recv, 8)
    gram_recv[me] = gram_send[...]
    wait_rows(gram_recv, 8, ga_n - 1, "ga", ga_n, me)
    summed = jnp.sum(gram_recv[...], axis=0) * (1.0 / total_pw)
    gram, tot = summed[:8], summed[8:9]
    rq, qq, ss, sq, sb, sp, qb, qp, bb, bp, pp = [cell(tot, n) for n in range(11)]
    l1 = -rq / (qq + eps)

    lam_send[...] = jnp.broadcast_to(l1, (1, 128))

    def send_lam(k, _):
        other = lax.rem(my_band + k, band_n)
        pltpu.make_async_remote_copy(
            src_ref=lam_send, dst_ref=lam_recv.at[my_band], send_sem=send_sem.at[10], recv_sem=recv_sem.at[10],
            device_id={"band": other}, device_id_type=MESH,
        ).start()
        return 0

    lax.fori_loop(1, band_n, send_lam, 0)
    lam_recv[my_band] = lam_send[...]

    new = bm + l1 * p1
    nb_out[0] = new[0:1]
    nb_out[1] = new[1:2]
    nn = bb + 2.0 * l1 * bp + l1 * l1 * pp
    n_sig = sb + l1 * (sp + qb) + l1 * l1 * qp
    sig_sig = ss + 2.0 * l1 * sq + l1 * l1 * qq
    shift = (n_sig - em * eps) / (nn + eps)
    energy = em + shift
    res = (sig_sig - 2.0 * shift * n_sig + shift * shift * nn) / (nn + eps)

    wait_rows(lam_recv, 10, band_n - 1, "band", band_n, my_band)
    lams = jnp.zeros((1, 128), F32)
    for j in range(band_n):
        lams = jnp.where(lane == j, lam_recv[j], lams)

    def part(rows, v):
        return rows[:, v * band_n : (v + 1) * band_n]

    lam8 = lams[:, :band_n]

    def finish(rows):
        a = rows[0:2] + l1 * rows[2:4]
        against_re = part(a, 0) + lam8 * part(a, 2)
        against_im = part(a, 1) + lam8 * part(a, 3)
        return (against_re[0:1] + against_im[1:2], against_im[0:1] - against_re[1:2])

    cor_re, cor_im = finish(gram[0:4])
    sub_re, sub_im = finish(gram[4:8])
    tail = jnp.concatenate([jnp.broadcast_to(energy, (1, band_n)), jnp.broadcast_to(res, (1, band_n))], axis=0)
    block = jnp.concatenate([cor_re, cor_im, sub_re, sub_im, tail, tail], axis=0)
    small_out[...] = jnp.concatenate([block, jnp.zeros((8, 128 - band_n), F32)], axis=1)


def body(tables, coeffs, cell_map, potential, projectors, strengths, proj_atom, proj_chan):
    ga_n = lax.axis_size("ga")
    band_n = lax.axis_size("band")
    grid_len = potential.shape[0]
    pw = coeffs.shape[2]
    proj_n = proj_atom.shape[0]
    total_pw = pw * ga_n
    vmem = pl.BlockSpec(memory_space=pltpu.VMEM)
    args = (coeffs, cell_map.reshape(1, pw), potential, projectors, strengths,
            proj_atom.reshape(1, proj_n), proj_chan.reshape(1, proj_n)) + tuple(tables)
    V = pltpu.VMEM
    scratch = [
        V((3 * grid_len, pw), BF16), V((3 * 128, pw), BF16), V((2 * grid_len, pw), F32),
        V((256, pw), BF16), V((256, pw), BF16), V((grid_len, 3 * 128), F32),
        V((2 * grid_len, 3 * 128), BF16), V((2 * grid_len, 3 * 128), BF16),
        V((16 * 40, 128), F32), V((proj_n, 2 * proj_n), F32), V((9, 2, pw), F32), V((2, pw), F32), V((1, pw), F32),
        V((6, ga_n * 16, 128), F32), V((6, ga_n * 16, 128), F32),
        V((2, 1, 128), F32), V((2, ga_n, 1, 128), F32),
        V((16, 128), F32), V((ga_n, 16, 128), F32),
        V((band_n * 8, pw), F32), V((1, 128), F32), V((band_n, 1, 128), F32),
        pltpu.SemaphoreType.DMA((11,)), pltpu.SemaphoreType.DMA((11,)),
    ]
    new_bands, small = pl.pallas_call(
        functools.partial(kernel, (ga_n, band_n, grid_len, total_pw)),
        out_shape=(
            jax.ShapeDtypeStruct((2, 1, pw), F32),
            jax.ShapeDtypeStruct((8, 128), F32),
        ),
        in_specs=[vmem] * len(args),
        out_specs=(vmem, vmem),
        scratch_shapes=scratch,
        compiler_params=pltpu.CompilerParams(collective_id=0, has_side_effects=True, vmem_limit_bytes=60000 * 1024),
    )(*args)
    corr = small[0:2, :band_n].reshape(2, 1, band_n)
    sub = small[2:4, :band_n].reshape(2, 1, band_n)
    return new_bands, small[4, :1], small[5, :1], corr, sub


def solution(mesh):
    tables = make_tables(96, mesh.shape["ga"])
    placed = (P(None, "band", "ga"), P("ga"), P(None, "ga", None), P(None, None, "ga"), P(), P(), P())
    return jax.shard_map(
        functools.partial(body, tables),
        mesh=mesh,
        in_specs=placed,
        out_specs=(P(None, "band", "ga"), P("band"), P("band"), P(None, "band", None), P(None, "band", None)),
        check_vma=False,
    )
```

```python
import functools

import jax
import jax.numpy as jnp
import numpy as np
from jax import lax
from jax.experimental import pallas as pl
from jax.experimental.pallas import tpu as pltpu
from jax.sharding import PartitionSpec as P

F32 = jnp.float32
BF16 = jnp.bfloat16
HIGHEST = lax.Precision.HIGHEST
MESH = pl.DeviceIdType.MESH
kin_unit = 0.02
small_eps = 1e-06

NN = (((1,), (0,)), ((), ()))
NT = (((1,), (1,)), ((), ()))
TN = (((0,), (0,)), ((), ()))


def parts_of(table, count):
    out = []
    left = np.asarray(table, np.float64)
    for _ in range(count):
        piece = left.astype(np.float32).astype(BF16)
        out.append(piece)
        left = left - piece.astype(np.float64)
    return out


def make_tables(grid_len, groups):
    planes = grid_len // groups
    natural = np.arange(grid_len)
    slab = (natural % groups) * planes + natural // groups

    def angles(rows, cols):
        return 2.0 * np.pi / grid_len * ((rows[:, None] * cols[None, :]) % grid_len)

    z_ang = angles(natural, natural)
    x_cos, x_sin = np.cos(z_ang), np.sin(z_ang)
    z_high, z_low = parts_of(np.concatenate([x_cos, x_sin], axis=0), 2)
    y_ang = angles(slab, natural)
    y_cos, y_sin = np.cos(y_ang), np.sin(y_ang)
    pad = np.zeros((grid_len, 128 - grid_len))
    side = np.zeros((2 * grid_len, 256 - 2 * grid_len))
    y_fwd = np.block([[y_cos, pad, -y_sin, pad], [y_sin, pad, y_cos, pad]])
    x_fwd = np.block([[x_cos, -x_sin], [x_sin, x_cos]])
    x_back = np.block([[x_cos, x_sin], [-x_sin, x_cos]]) / grid_len
    x_fwd, x_back = np.concatenate([x_fwd, side], axis=1), np.concatenate([x_back, side], axis=1)
    y_back = y_fwd / grid_len**2
    rest = []
    for tab in (y_fwd, x_fwd, x_back, y_back):
        rest += parts_of(tab, 2)
    return [np.concatenate([z_high, z_low], axis=1), np.stack(rest)]


def dot(a, b, dims=NN):
    return lax.dot_general(a, b, dims, preferred_element_type=F32)


def dot_full(a, b, dims=NN):
    return lax.dot_general(a, b, dims, precision=HIGHEST, preferred_element_type=F32)


def split(x):
    hi = x.astype(BF16)
    return hi, (x - hi.astype(F32)).astype(BF16)


def iota(shape, axis):
    return lax.broadcasted_iota(jnp.int32, shape, axis)


def ring_steps(groups):
    side = 4
    cores = groups // (side * side)

    def hops(k):
        return min(k, side - k)

    steps = [(i, j, c) for i in range(side) for j in range(side) for c in range(cores) if (i, j, c) != (0, 0, 0)]
    return sorted(steps, key=lambda s: -(hops(s[0]) + hops(s[1])))


def kernel(sizes, cf, cm, zt, st, pa, pc, pot_any, pj_any, tabs_any,
           nb_out, small_out,
           pot, pj, tabs, at_s, at_g, e_tab, x_all, gt, big, coup, vecs, hvec, kin_ref,
           send, recv, row_send, row_recv, gram_send, gram_recv, bands, lam_send, lam_recv,
           send_sem, recv_sem, load_sem):
    ga_n, band_n, grid_len, total_pw = sizes
    planes = grid_len // ga_n
    me = lax.axis_index("ga")
    my_band = lax.axis_index("band")
    pw = cf.shape[2]
    tiles = pw // 128
    loads = [
        pltpu.make_async_copy(pj_any, pj, load_sem.at[0]),
        pltpu.make_async_copy(tabs_any, tabs, load_sem.at[1]),
        pltpu.make_async_copy(pot_any, pot, load_sem.at[2]),
    ]
    for load in loads:
        load.start()

    barrier = pltpu.get_barrier_semaphore()
    m_x, m_y, m_c = me // 8, me // 2 % 4, me % 2

    def at_step(step):
        return ((m_x + step[0]) % 4) * 8 + ((m_y + step[1]) % 4) * 2 + (m_c + step[2]) % 2

    others = [at_step(step) for step in ring_steps(ga_n)]
    band_order = sorted(range(1, band_n), key=lambda k: -min(k, band_n - k))
    other_bands = [lax.rem(my_band + k, band_n) for k in band_order]

    for other in others:
        pl.semaphore_signal(barrier, inc=1, device_id={"ga": other}, device_id_type=MESH)
    for other in other_bands:
        pl.semaphore_signal(barrier, inc=1, device_id={"band": other}, device_id_type=MESH)

    cells = cm[...]
    py = lax.shift_right_logical(cells * 43691, 22)
    z_idx = cells - py * grid_len
    plane = (py >= grid_len).astype(jnp.int32) + (py >= 2 * grid_len).astype(jnp.int32)
    y_idx = py - plane * grid_len
    x_idx = me + ga_n * plane
    py_pad = plane * 128 + y_idx

    def freq(k):
        return jnp.where(2 * k < grid_len, k, k - grid_len).astype(F32)

    kin = kin_unit * (freq(x_idx) * freq(x_idx) + freq(y_idx) * freq(y_idx) + freq(z_idx) * freq(z_idx))
    for k in range(tiles):
        lanes = slice(k * 128, k * 128 + 128)
        kin_ref[:, lanes] = kin[k : k + 1]
        hot = (iota((grid_len, 128), 0) == z_idx[k : k + 1])
        hot = jnp.where(hot, 1.0, 0.0).astype(BF16)
        e_tab[:, lanes] = dot(zt[...], jnp.concatenate([hot, hot], axis=0))
    upright = jnp.transpose(jnp.concatenate([py_pad, jnp.zeros((128 - tiles, 128), jnp.int32)], axis=0))
    for k in range(tiles):
        hot = (iota((128, 3 * 128), 1) == upright[:, k : k + 1])
        at_s[k * 128 : k * 128 + 128, :] = jnp.where(hot, 1.0, 0.0).astype(BF16)

    def later_tables():
        for k in range(tiles):
            hot = (iota((3 * 128, 128), 0) == py_pad[k : k + 1])
            at_g[:, k * 128 : k * 128 + 128] = jnp.where(hot, 1.0, 0.0).astype(BF16)
        chans = st.shape[1]
        sym_rows = st[...].reshape(st.shape[0] * chans, chans)
        slot = pa[...] * chans + pc[...]
        hot_p = jnp.where(iota((proj_n, proj_n), 0) == slot, 1.0, 0.0)
        hot_c = jnp.where(iota((chans, proj_n), 0) == pc[...], 1.0, 0.0)
        reach = dot_full(sym_rows, hot_c)
        reach = jnp.where(iota((proj_n, proj_n), 0) // chans == pa[...], reach, 0.0)
        half = 0.5 * (dot_full(hot_p, reach, TN) + dot_full(reach, hot_p, TN))
        coup[...] = jnp.concatenate([half, half], axis=1)

    proj_n = pa.shape[1]
    lane = iota((1, 128), 1)
    lane32 = iota((ga_n, 128), 1)

    def roll(x, by):
        return pltpu.roll(x, by, 1)

    def pack(a, b, c, d, e, f):
        rb, rc, rd, rf = roll(b, 96), roll(c, 64), roll(d, 32), roll(f, 96)
        return (
            jnp.where(lane32 < 96, a, rb),
            jnp.where(lane32 < 64, rb, rc),
            jnp.where(lane32 < 32, rc, rd),
            jnp.where(lane32 < 96, e, rf),
            rf,
        )

    def unpack(t0, t1, t2, t3, t4):
        b = roll(jnp.where(lane32 < 64, t1, t0), 32)
        c = roll(jnp.where(lane32 < 32, t2, t1), 64)
        d = roll(t2, 96)
        f = roll(jnp.where(lane32 < 64, t4, t3), 32)
        return t0, b, c, d, t3, f

    stride = big.shape[0] // 16

    def put_big(block, value):
        big[block * stride : block * stride + ga_n, :] = value

    def exchange(phase):
        for d in range(ga_n):
            send[phase, d * 16 : d * 16 + 16, :] = big[pl.ds(d, 16, stride=stride), :]
        mine = pl.ds(pl.multiple_of(me * 16, 16), 16)
        for other in others:
            pltpu.make_async_remote_copy(
                src_ref=send.at[phase, pl.ds(pl.multiple_of(other * 16, 16), 16), :],
                dst_ref=recv.at[phase, mine, :],
                send_sem=send_sem.at[phase],
                recv_sem=recv_sem.at[phase],
                device_id={"ga": other},
                device_id_type=MESH,
            ).start()
        recv[phase, mine, :] = send[phase, mine, :]

    def wait_exchange(phase):
        span = pl.ds(0, (ga_n - 1) * 16)
        both = pltpu.make_async_remote_copy(
            src_ref=send.at[phase, span, :],
            dst_ref=recv.at[phase, span, :],
            send_sem=send_sem.at[phase],
            recv_sem=recv_sem.at[phase],
            device_id={"ga": lax.rem(me + 1, ga_n)},
            device_id_type=MESH,
        )
        both.wait()

    def got_rows(phase, row):
        return recv[phase, pl.ds(row, ga_n, stride=16), :]

    def spread_rows(ref_send, ref_recv, sem):
        for other in others:
            pltpu.make_async_remote_copy(
                src_ref=ref_send, dst_ref=ref_recv.at[me], send_sem=send_sem.at[sem], recv_sem=recv_sem.at[sem],
                device_id={"ga": other}, device_id_type=MESH,
            ).start()

    def spread_band(ref_send, ref_recv, sem):
        for other in other_bands:
            pltpu.make_async_remote_copy(
                src_ref=ref_send, dst_ref=ref_recv, send_sem=send_sem.at[sem], recv_sem=recv_sem.at[sem],
                device_id={"band": other}, device_id_type=MESH,
            ).start()

    def wait_rows(ref_recv, sem, count, axis, size, mine):
        span = ref_recv.at[pl.ds(0, count)]
        pltpu.make_async_remote_copy(
            src_ref=span, dst_ref=span, send_sem=send_sem.at[sem], recv_sem=recv_sem.at[sem],
            device_id={axis: lax.rem(mine + 1, size)}, device_id_type=MESH,
        ).wait()

    def cell(row, at):
        return jnp.sum(jnp.where(lane == at, row, 0.0), axis=1, keepdims=True)

    def fold(x):
        total = x[:, :128]
        for k in range(1, tiles):
            total = total + x[:, k * 128 : k * 128 + 128]
        return total[0:1] + total[1:2]

    def as_row(folded):
        stack = jnp.concatenate(folded + [jnp.zeros((1, 128), F32)] * (-len(folded) % 8), axis=0)
        col = jnp.sum(stack, axis=1, keepdims=True)
        hit = iota(stack.shape, 0) == iota(stack.shape, 1)
        return jnp.sum(jnp.where(hit, col, 0.0), axis=0, keepdims=True)

    def start_sums(which, row):
        row_send[which] = row
        spread_rows(row_send.at[which], row_recv.at[which], 6 + which)
        row_recv[which, me] = row_send[which]

    def end_sums(which):
        wait_rows(row_recv.at[which], 6 + which, ga_n - 1, "ga", ga_n, me)
        return jnp.sum(row_recv[which], axis=0) * (1.0 / total_pw)

    def all_sums(which, folded):
        start_sums(which, as_row(folded))
        total = end_sums(which)
        return total

    def apply_h(turn, v):
        for k in range(tiles):
            lanes = slice(k * 128, k * 128 + 128)
            e_c, e_s = e_tab[:grid_len, lanes], e_tab[grid_len:, lanes]
            v_re, v_im = v[0:1, lanes], v[1:2, lanes]
            hi, lo = split(e_c * v_re - e_s * v_im)
            x_all[:grid_len, lanes] = hi
            x_all[2 * grid_len : 3 * grid_len, lanes] = lo
            hi, lo = split(e_s * v_re + e_c * v_im)
            x_all[grid_len : 2 * grid_len, lanes] = hi
            x_all[3 * grid_len :, lanes] = lo
        t_all = dot(x_all[...], at_s[...])
        t_all = t_all[: 2 * grid_len] + t_all[2 * grid_len :]

        if turn == 0:
            loads[1].wait()
        u = []
        for i in range(planes):
            lanes = slice(i * 128, i * 128 + 128)
            t_i = jnp.concatenate([t_all[:grid_len, lanes], t_all[grid_len:, lanes]], axis=1)
            hi, lo = split(jnp.concatenate([t_i, jnp.zeros((128 - grid_len, 256), F32)], axis=0))
            u.append(dot(tabs[0], hi, NT) + dot(tabs[0], lo, NT) + dot(tabs[1], hi, NT))
        for j in range(planes):
            six = []
            for i in range(planes):
                for c in range(2):
                    at = c * grid_len + j * ga_n
                    six.append(u[i][at : at + ga_n])
            for t, piece in enumerate(pack(*six)):
                put_big(j * 5 + t, piece)
        if turn == 0:
            put_big(15, jnp.zeros((ga_n, 128), F32))
            pl.semaphore_wait(barrier, ga_n - 1 + band_n - 1)
        exchange(2 * turn)

        if turn == 0:
            loads[0].wait()
        acc_re = jnp.zeros((proj_n, 128), F32)
        acc_im = jnp.zeros((proj_n, 128), F32)
        for k in range(tiles):
            lanes = slice(k * 128, k * 128 + 128)
            p_re, p_im = pj[0, :, lanes], pj[1, :, lanes]
            v_re, v_im = v[0:1, lanes], v[1:2, lanes]
            acc_re = acc_re + (p_re * v_re + p_im * v_im)
            acc_im = acc_im + (p_re * v_im - p_im * v_re)
        col_re = jnp.sum(acc_re, axis=1, keepdims=True)
        col_im = jnp.sum(acc_im, axis=1, keepdims=True)
        row64, lane64 = iota((proj_n, 128), 0), iota((proj_n, 128), 1)
        diag = jnp.where(lane64 == row64, col_re, jnp.where(lane64 == row64 + proj_n, col_im, 0.0))
        start_sums(3 + turn, jnp.sum(diag, axis=0, keepdims=True))
        norm_row = None
        if turn == 0:
            norm_row = as_row([fold(v * v), fold(v * v * kin_ref[...])])
            later_tables()
            loads[2].wait()
        wait_exchange(2 * turn)

        cols = []
        for j in range(planes):
            pieces = unpack(*[got_rows(2 * turn, j * 5 + t) for t in range(5)])
            cols.append(jnp.concatenate(pieces[0::2] + pieces[1::2], axis=0))
        hi, lo = split(jnp.concatenate(cols, axis=1))
        x_h, x_l = tabs[2, :, : 2 * grid_len], tabs[3, :, : 2 * grid_len]
        w = dot(x_h, hi) + dot(x_h, lo) + dot(x_l, hi)
        w_re, w_im = w[:grid_len], w[grid_len:]
        blank = jnp.zeros((grid_len, 128 - grid_len), F32)
        v_tab = jnp.concatenate([x for j in range(planes) for x in (pot[j], blank)], axis=1)
        vw_re, vw_im = v_tab * w_re, v_tab * w_im
        if turn == 0:
            dens = jnp.sum(vw_re * w_re + vw_im * w_im, axis=0, keepdims=True)
            dens = dens[:, :128] + dens[:, 128:256] + dens[:, 256:]
            dens = jnp.sum(dens, axis=1, keepdims=True)
            put_big(15, jnp.broadcast_to(jnp.where(lane == 2, dens, norm_row), (ga_n, 128)))
        hi, lo = split(jnp.concatenate([vw_re, vw_im], axis=0))
        x_h, x_l = tabs[4, :, : 2 * grid_len], tabs[5, :, : 2 * grid_len]
        back = dot(x_h, hi) + dot(x_h, lo) + dot(x_l, hi)
        for j in range(planes):
            lanes = slice(j * 128, j * 128 + 128)
            six = []
            for i in range(planes):
                for c in range(2):
                    at = c * grid_len + i * ga_n
                    six.append(back[at : at + ga_n, lanes])
            for t, piece in enumerate(pack(*six)):
                put_big(j * 5 + t, piece)
        exchange(2 * turn + 1)

        tot = end_sums(3 + turn)
        prod = coup[...] * tot
        mix_re = jnp.sum(jnp.where(lane64 < proj_n, prod, 0.0), axis=1, keepdims=True)
        mix_im = jnp.sum(jnp.where(lane64 < proj_n, 0.0, prod), axis=1, keepdims=True)
        c_n = None
        if turn == 0:
            diag_row = jnp.where(lane64 == row64, mix_re, jnp.where(lane64 == row64 + proj_n, mix_im, 0.0))
            c_n = jnp.sum(jnp.sum(diag_row, axis=0, keepdims=True) * tot, axis=1, keepdims=True)
        for k in range(tiles):
            lanes = slice(k * 128, k * 128 + 128)
            p_re, p_im = pj[0, :, lanes], pj[1, :, lanes]
            n_re = jnp.sum(p_re * mix_re - p_im * mix_im, axis=0, keepdims=True)
            n_im = jnp.sum(p_im * mix_re + p_re * mix_im, axis=0, keepdims=True)
            hvec[:, lanes] = jnp.concatenate([n_re, n_im], axis=0) + kin_ref[:, lanes] * v[:, lanes]
        wait_exchange(2 * turn + 1)

        zs = [[None] * planes for _ in range(2 * planes)]
        for j in range(planes):
            pieces = unpack(*[got_rows(2 * turn + 1, j * 5 + t) for t in range(5)])
            for n, piece in enumerate(pieces):
                zs[n][j] = piece
        for i in range(planes):
            stack = jnp.concatenate(zs[2 * i] + zs[2 * i + 1], axis=0)
            hi, lo = split(stack.T)
            out = dot(hi, tabs[6]) + dot(lo, tabs[6]) + dot(hi, tabs[7])
            for c in range(2):
                hi, lo = split(out[:grid_len, c * 128 : c * 128 + 128])
                gt[c * grid_len : (c + 1) * grid_len, i * 128 : i * 128 + 128] = hi
                gt[(2 + c) * grid_len : (3 + c) * grid_len, i * 128 : i * 128 + 128] = lo
        for k in range(0, pw, 256):
            lanes = slice(k, k + 256)
            q = dot(gt[...], at_g[:, lanes])
            q = q[: 2 * grid_len] + q[2 * grid_len :]
            q_re, q_im = q[:grid_len], q[grid_len:]
            e_c, e_s = e_tab[:grid_len, lanes], e_tab[grid_len:, lanes]
            l_re = jnp.sum(e_c * q_re + e_s * q_im, axis=0, keepdims=True)
            l_im = jnp.sum(e_c * q_im - e_s * q_re, axis=0, keepdims=True)
            hvec[:, lanes] = hvec[:, lanes] + jnp.concatenate([l_re, l_im], axis=0)
        return c_n

    def precondition(r, level):
        ratio = kin_ref[...] / (1.5 * level + 1.0)
        numer = 27.0 + ratio * (18.0 + ratio * (12.0 + 8.0 * ratio))
        square = ratio * ratio
        return r * (numer / (numer + 16.0 * square * square))

    eps = small_eps

    vecs[0] = jnp.concatenate([cf[0], cf[1]], axis=0)
    c_n = apply_h(0, vecs[0])
    tot = jnp.sum(got_rows(1, 15), axis=0, keepdims=True) * (1.0 / total_pw)
    guess_cc = cell(tot, 0)
    guess = (cell(tot, 1) + cell(tot, 2) * (1.0 / grid_len**3) + c_n) / (guess_cc + eps)
    c = vecs[0]
    h0 = hvec[...]
    s = h0 - guess * c
    kc, ks = kin_ref[...] * c, kin_ref[...] * s
    tot = all_sums(0, [fold(c * c), fold(c * s), fold(s * s), fold(kc * c), fold(kc * s), fold(ks * s)])
    cc, cs, ss, kcc, kcs, kss = [cell(tot, n) for n in range(6)]
    shift = (cs - guess * eps) / (cc + eps)
    e0 = guess + shift
    r0 = s - shift * c
    rr = ss - 2.0 * shift * cs + shift * shift * cc
    krr = kss - 2.0 * shift * kcs + shift * shift * kcc
    rc = cs - shift * cc
    krc = kcs - shift * kcc
    p0 = precondition(r0, krr / (rr + eps))
    vecs[1] = r0
    vecs[2] = p0
    vecs[3] = h0

    apply_h(1, vecs[2])
    c, r0, p0, h0 = vecs[0], vecs[1], vecs[2], vecs[3]
    g0 = hvec[...]
    q0 = g0 - e0 * p0
    pairs = [(r0, q0), (r0, p0), (q0, q0), (q0, c), (q0, p0), (c, p0), (p0, p0)]
    prods = [a * b for a, b in pairs]
    tot = all_sums(1, [fold(x) for x in prods] + [fold(x * kin_ref[...]) for x in prods])
    rq, rp, qq, qc, qp, cp, pp = [cell(tot, n) for n in range(7)]
    krq, krp, kqq, kqc, kqp, kcp, kpp = [cell(tot, n) for n in range(7, 14)]
    l0 = -rq / (qq + eps)
    bb = cc + 2.0 * l0 * cp + l0 * l0 * pp
    b_rho = rc + l0 * (qc + rp) + l0 * l0 * qp
    d1 = (b_rho - e0 * eps) / (bb + eps)
    fa, fb, fc = -l0, d1, d1 * l0
    r_dr = fa * rq + fb * rc + fc * rp
    dr_dr = fa * fa * qq + fb * fb * cc + fc * fc * pp + 2.0 * (fa * fb * qc + fa * fc * qp + fb * fc * cp)
    kr_dr = fa * krq + fb * krc + fc * krp
    kdr_dr = fa * fa * kqq + fb * fb * kcc + fc * fc * kpp + 2.0 * (fa * fb * kqc + fa * fc * kqp + fb * fc * kcp)
    wt = r_dr / (dr_dr + eps)
    lm = wt * l0
    bmbm = cc + 2.0 * lm * cp + lm * lm * pp
    bm_rho = rc + lm * (qc + rp) + lm * lm * qp
    dm = (bm_rho - e0 * eps) / (bmbm + eps)
    em = e0 + dm
    mm = rr - 2.0 * wt * r_dr + wt * wt * dr_dr
    kmm = krr - 2.0 * wt * kr_dr + wt * wt * kdr_dr
    bm = c + lm * p0
    hm = h0 + lm * g0
    rm = r0 - wt * (fa * q0 + fb * c + fc * p0)
    sm = r0 + lm * q0 - dm * bm
    p1 = precondition(rm, kmm / (mm + eps))
    vecs[4] = bm
    vecs[5] = hm
    vecs[6] = rm
    vecs[7] = sm
    vecs[8] = p1
    slot8 = pl.ds(pl.multiple_of(my_band * 8, 8), 8)
    bands[slot8, :] = jnp.concatenate([bm, p1, bm, p1], axis=0)

    spread_band(bands.at[slot8, :], bands.at[slot8, :], 13)

    apply_h(2, vecs[8])
    bm, hm, rm, sm, p1 = vecs[4], vecs[5], vecs[6], vecs[7], vecs[8]
    g1 = hvec[...]
    q1 = g1 - em * p1
    start_sums(2, as_row([fold(rm * q1), fold(q1 * q1)]))
    span = bands.at[pl.ds(0, (band_n - 1) * 8), :]
    pltpu.make_async_remote_copy(
        src_ref=span, dst_ref=span, send_sem=send_sem.at[13], recv_sem=recv_sem.at[13],
        device_id={"band": other_bands[0]}, device_id_type=MESH,
    ).wait()
    left = jnp.concatenate([bm, p1, hm, g1], axis=0)
    gram = dot_full(left, bands[...], NT)
    wide = (band_n * 8, 128)
    moved = iota(wide, 0) % 8 * band_n + iota(wide, 0) // 8
    gram = dot_full(gram, jnp.where(moved == iota(wide, 1), 1.0, 0.0))
    pairs = [(sm, sm), (sm, q1), (sm, bm), (sm, p1), (q1, bm), (q1, p1), (bm, bm), (bm, p1), (p1, p1)]
    row = as_row([fold(a * b) for a, b in pairs])
    gram_send[:8, :] = gram
    gram_send[8:, :] = jnp.broadcast_to(row, (8, 128))
    spread_rows(gram_send, gram_recv, 9 + 3)
    gram_recv[me] = gram_send[...]
    tot = end_sums(2)
    rq, qq = cell(tot, 0), cell(tot, 1)
    l1 = -rq / (qq + eps)
    lam_send[...] = jnp.broadcast_to(l1, (1, 128))
    spread_band(lam_send, lam_recv.at[my_band], 14)
    lam_recv[my_band] = lam_send[...]
    wait_rows(gram_recv, 9 + 3, ga_n - 1, "ga", ga_n, me)
    summed = jnp.sum(gram_recv[...], axis=0) * (1.0 / total_pw)
    gram, tot = summed[:8], summed[8:9]
    ss, sq, sb, sp, qb, qp, bb, bp, pp = [cell(tot, n) for n in range(9)]

    new = bm + l1 * p1
    nb_out[0] = new[0:1]
    nb_out[1] = new[1:2]
    nn = bb + 2.0 * l1 * bp + l1 * l1 * pp
    n_sig = sb + l1 * (sp + qb) + l1 * l1 * qp
    sig_sig = ss + 2.0 * l1 * sq + l1 * l1 * qq
    shift = (n_sig - em * eps) / (nn + eps)
    energy = em + shift
    res = (sig_sig - 2.0 * shift * n_sig + shift * shift * nn) / (nn + eps)

    wait_rows(lam_recv, 14, band_n - 1, "band", band_n, my_band)
    lams = jnp.zeros((1, 128), F32)
    for j in range(band_n):
        lams = jnp.where(lane == j, lam_recv[j], lams)

    def part(rows, v):
        return rows[:, v * band_n : (v + 1) * band_n]

    lam8 = lams[:, :band_n]

    def finish(rows):
        a = rows[0:2] + l1 * rows[2:4]
        against_re = part(a, 0) + lam8 * part(a, 2)
        against_im = part(a, 1) + lam8 * part(a, 3)
        return (against_re[0:1] + against_im[1:2], against_im[0:1] - against_re[1:2])

    cor_re, cor_im = finish(gram[0:4])
    sub_re, sub_im = finish(gram[4:8])
    tail = jnp.concatenate([jnp.broadcast_to(energy, (1, band_n)), jnp.broadcast_to(res, (1, band_n))], axis=0)
    block = jnp.concatenate([cor_re, cor_im, sub_re, sub_im, tail, tail], axis=0)
    small_out[...] = jnp.concatenate([block, jnp.zeros((8, 128 - band_n), F32)], axis=1)


def body(tables, coeffs, cell_map, potential, projectors, strengths, proj_atom, proj_chan):
    ga_n = lax.axis_size("ga")
    band_n = lax.axis_size("band")
    grid_len = potential.shape[0]
    pw = coeffs.shape[2]
    proj_n = proj_atom.shape[0]
    total_pw = pw * ga_n
    vmem = pl.BlockSpec(memory_space=pltpu.VMEM)
    any_ = pl.BlockSpec(memory_space=pl.ANY)
    z_tab, tabs = tables
    args = (coeffs, cell_map.reshape(pw // 128, 128), z_tab, strengths,
            proj_atom.reshape(1, proj_n), proj_chan.reshape(1, proj_n),
            jnp.transpose(potential, (1, 0, 2)), projectors, tabs)
    V = pltpu.VMEM
    planes = grid_len // ga_n
    scratch = [
        V((planes, grid_len, grid_len), F32), V(projectors.shape, F32), V(tabs.shape, BF16),
        V((pw, 3 * 128), BF16), V((3 * 128, pw), BF16), V((2 * grid_len, pw), F32),
        V((4 * grid_len, pw), BF16), V((4 * grid_len, 3 * 128), BF16),
        V((16 * 40, 128), F32), V((proj_n, 2 * proj_n), F32), V((9, 2, pw), F32), V((2, pw), F32), V((1, pw), F32),
        V((6, ga_n * 16, 128), F32), V((6, ga_n * 16, 128), F32),
        V((6, 1, 128), F32), V((6, ga_n, 1, 128), F32),
        V((16, 128), F32), V((ga_n, 16, 128), F32),
        V((band_n * 8, pw), F32), V((1, 128), F32), V((band_n, 1, 128), F32),
        pltpu.SemaphoreType.DMA((15,)), pltpu.SemaphoreType.DMA((15,)), pltpu.SemaphoreType.DMA((3,)),
    ]
    new_bands, small = pl.pallas_call(
        functools.partial(kernel, (ga_n, band_n, grid_len, total_pw)),
        out_shape=(
            jax.ShapeDtypeStruct((2, 1, pw), F32),
            jax.ShapeDtypeStruct((8, 128), F32),
        ),
        in_specs=[vmem] * 6 + [any_] * 3,
        out_specs=(vmem, vmem),
        scratch_shapes=scratch,
        compiler_params=pltpu.CompilerParams(collective_id=0, has_side_effects=True, vmem_limit_bytes=60000 * 1024),
    )(*args)

    def deal(nb, sm, nb_o, en_o, re_o, co_o, su_o):
        nb_o[...] = nb[...]
        co_o[0], co_o[1] = sm[0:1, :band_n], sm[1:2, :band_n]
        su_o[0], su_o[1] = sm[2:3, :band_n], sm[3:4, :band_n]
        en_o[...] = sm[4:5, :1]
        re_o[...] = sm[5:6, :1]

    one = jax.ShapeDtypeStruct((1, 1), F32)
    rows = jax.ShapeDtypeStruct((2, 1, band_n), F32)
    new_bands, energy, res, corr, sub = pl.pallas_call(
        deal,
        out_shape=(jax.ShapeDtypeStruct((2, 1, pw), F32), one, one, rows, rows),
        in_specs=[vmem] * 2,
        out_specs=(vmem,) * 5,
    )(new_bands, small)
    return new_bands, energy.reshape(1), res.reshape(1), corr, sub


def solution(mesh):
    tables = make_tables(96, mesh.shape["ga"])
    placed = (P(None, "band", "ga"), P("ga"), P(None, "ga", None), P(None, None, "ga"), P(), P(), P())
    return jax.shard_map(
        functools.partial(body, tables),
        mesh=mesh,
        in_specs=placed,
        out_specs=(P(None, "band", "ga"), P("band"), P("band"), P(None, "band", None), P(None, "band", None)),
        check_vma=False,
    )
```

```python
import functools

import jax
import jax.numpy as jnp
import numpy as np
from jax import lax
from jax.experimental import pallas as pl
from jax.experimental.pallas import tpu as pltpu
from jax.sharding import PartitionSpec as P

F32 = jnp.float32
BF16 = jnp.bfloat16
HIGHEST = lax.Precision.HIGHEST
MESH = pl.DeviceIdType.MESH
kin_unit = 0.02
small_eps = 1e-06

NN = (((1,), (0,)), ((), ()))
NT = (((1,), (1,)), ((), ()))
TN = (((0,), (0,)), ((), ()))


def parts_of(table, count):
    out = []
    left = np.asarray(table, np.float64)
    for _ in range(count):
        piece = left.astype(np.float32).astype(BF16)
        out.append(piece)
        left = left - piece.astype(np.float64)
    return out


def make_tables(grid_len, groups):
    planes = grid_len // groups
    natural = np.arange(grid_len)
    slab = (natural % groups) * planes + natural // groups

    def angles(rows, cols):
        return 2.0 * np.pi / grid_len * ((rows[:, None] * cols[None, :]) % grid_len)

    z_ang = angles(natural, natural)
    x_cos, x_sin = np.cos(z_ang), np.sin(z_ang)
    z_high, z_low = parts_of(np.concatenate([x_cos, x_sin], axis=0), 2)
    y_ang = angles(slab, natural)
    y_cos, y_sin = np.cos(y_ang), np.sin(y_ang)
    pad = np.zeros((grid_len, 128 - grid_len))
    side = np.zeros((2 * grid_len, 256 - 2 * grid_len))
    y_fwd = np.block([[y_cos, pad, -y_sin, pad], [y_sin, pad, y_cos, pad]])
    x_fwd = np.block([[x_cos, -x_sin], [x_sin, x_cos]])
    x_back = np.block([[x_cos, x_sin], [-x_sin, x_cos]]) / grid_len
    x_fwd, x_back = np.concatenate([x_fwd, side], axis=1), np.concatenate([x_back, side], axis=1)
    y_back = y_fwd / grid_len**2
    rest = []
    for tab in (y_fwd, x_fwd, x_back, y_back):
        rest += parts_of(tab, 2)
    return [np.concatenate([z_high, z_low], axis=1), np.stack(rest)]


def dot(a, b, dims=NN):
    return lax.dot_general(a, b, dims, preferred_element_type=F32)


def dot_full(a, b, dims=NN):
    return lax.dot_general(a, b, dims, precision=HIGHEST, preferred_element_type=F32)


def split(x):
    hi = x.astype(BF16)
    return hi, (x - hi.astype(F32)).astype(BF16)


def iota(shape, axis):
    return lax.broadcasted_iota(jnp.int32, shape, axis)


def ring_steps(groups):
    side = 4
    cores = groups // (side * side)

    def hops(k):
        return min(k, side - k)

    steps = [(i, j, c) for i in range(side) for j in range(side) for c in range(cores) if (i, j, c) != (0, 0, 0)]
    return sorted(steps, key=lambda s: -(hops(s[0]) + hops(s[1])))


def kernel(sizes, cm_far, zt_far, cf_far, tabs_far, pj_far, pot_far, st_far, pa_far, pc_far,
           nb_out, small_out,
           cm, zt, cf, tabs, pj, pot, st, pa, pc, at_s, at_g, e_tab, gt, gt_rest, coup, vecs, hvec, kin_ref,
           send, recv, row_send, row_recv, gram_send, gram_recv, bands, lam_send, lam_recv,
           send_sem, recv_sem, load_sem):
    ga_n, band_n, grid_len, total_pw = sizes
    planes = grid_len // ga_n
    me = lax.axis_index("ga")
    my_band = lax.axis_index("band")
    pw = cf.shape[2]
    tiles = pw // 128
    far = (cm_far, zt_far, cf_far, tabs_far, pj_far, pot_far, st_far, pa_far, pc_far)
    near = (cm, zt, cf, tabs, pj, pot, st, pa, pc)
    loads = [pltpu.make_async_copy(a, b, load_sem.at[n]) for n, (a, b) in enumerate(zip(far, near))]
    loads[0].start()
    loads[1].start()

    barrier = pltpu.get_barrier_semaphore()
    m_x, m_y, m_c = me // 8, me // 2 % 4, me % 2

    def at_step(step):
        return ((m_x + step[0]) % 4) * 8 + ((m_y + step[1]) % 4) * 2 + (m_c + step[2]) % 2

    others = [at_step(step) for step in ring_steps(ga_n)]
    band_order = sorted(range(1, band_n), key=lambda k: -min(k, band_n - k))
    other_bands = [lax.rem(my_band + k, band_n) for k in band_order]

    for other in others:
        pl.semaphore_signal(barrier, inc=1, device_id={"ga": other}, device_id_type=MESH)
    for other in other_bands:
        pl.semaphore_signal(barrier, inc=1, device_id={"band": other}, device_id_type=MESH)

    for load in loads[2:]:
        load.start()
    zeros = jnp.zeros((ga_n, 128), F32)
    for phase in range(6):
        send[phase, pl.ds(15, ga_n, stride=16), :] = zeros
    loads[0].wait()
    loads[1].wait()

    cells = cm[...]
    py = lax.shift_right_logical(cells * 43691, 22)
    z_idx = cells - py * grid_len
    plane = (py >= grid_len).astype(jnp.int32) + (py >= 2 * grid_len).astype(jnp.int32)
    y_idx = py - plane * grid_len
    x_idx = me + ga_n * plane
    py_pad = plane * 128 + y_idx

    def freq(k):
        return jnp.where(2 * k < grid_len, k, k - grid_len).astype(F32)

    kin = kin_unit * (freq(x_idx) * freq(x_idx) + freq(y_idx) * freq(y_idx) + freq(z_idx) * freq(z_idx))
    for k in range(tiles):
        lanes = slice(k * 128, k * 128 + 128)
        kin_ref[:, lanes] = kin[k : k + 1]
        hot = (iota((grid_len, 128), 0) == z_idx[k : k + 1])
        hot = jnp.where(hot, 1.0, 0.0).astype(BF16)
        e_tab[:, lanes] = dot(zt[...], jnp.concatenate([hot, hot], axis=0))
    upright = jnp.transpose(jnp.concatenate([py_pad, jnp.zeros((128 - tiles, 128), jnp.int32)], axis=0))
    for k in range(tiles):
        hot = (iota((128, 3 * 128), 1) == upright[:, k : k + 1])
        at_s[k * 128 : k * 128 + 128, :] = jnp.where(hot, 1.0, 0.0).astype(BF16)

    def later_tables():
        for load in loads[6:]:
            load.wait()
        place = jnp.where(plane == 2, jnp.where(y_idx < 32, 96 + y_idx, 192 + y_idx), plane * 128 + y_idx)
        for k in range(tiles):
            lanes = slice(k * 128, k * 128 + 128)
            hot = jnp.where(iota((288, 128), 0) == place[k : k + 1], 1.0, 0.0).astype(BF16)
            at_g[:288, lanes] = hot
            at_g[288:, lanes] = hot[256:]
        chans = st.shape[1]
        sym_rows = st[...].reshape(st.shape[0] * chans, chans)
        slot = pa[...] * chans + pc[...]
        hot_p = jnp.where(iota((proj_n, proj_n), 0) == slot, 1.0, 0.0)
        hot_c = jnp.where(iota((chans, proj_n), 0) == pc[...], 1.0, 0.0)
        reach = dot_full(sym_rows, hot_c)
        reach = jnp.where(iota((proj_n, proj_n), 0) // chans == pa[...], reach, 0.0)
        half = 0.5 * (dot_full(hot_p, reach, TN) + dot_full(reach, hot_p, TN))
        coup[...] = jnp.concatenate([half, half], axis=1)

    proj_n = pa.shape[1]
    lane = iota((1, 128), 1)
    lane32 = iota((ga_n, 128), 1)

    def roll(x, by):
        return pltpu.roll(x, by, 1)

    def pack(a, b, c, d, e, f):
        rb, rc, rd, rf = roll(b, 96), roll(c, 64), roll(d, 32), roll(f, 96)
        return (
            jnp.where(lane32 < 96, a, rb),
            jnp.where(lane32 < 64, rb, rc),
            jnp.where(lane32 < 32, rc, rd),
            jnp.where(lane32 < 96, e, rf),
            rf,
        )

    def unpack(t0, t1, t2, t3, t4):
        b = roll(jnp.where(lane32 < 64, t1, t0), 32)
        c = roll(jnp.where(lane32 < 32, t2, t1), 64)
        d = roll(t2, 96)
        f = roll(jnp.where(lane32 < 64, t4, t3), 32)
        return t0, b, c, d, t3, f

    def put(phase, row, value):
        send[phase, pl.ds(row, ga_n, stride=16), :] = value

    def exchange(phase):
        mine = pl.ds(pl.multiple_of(me * 16, 16), 16)
        for other in others:
            pltpu.make_async_remote_copy(
                src_ref=send.at[phase, pl.ds(pl.multiple_of(other * 16, 16), 16), :],
                dst_ref=recv.at[phase, mine, :],
                send_sem=send_sem.at[phase],
                recv_sem=recv_sem.at[phase],
                device_id={"ga": other},
                device_id_type=MESH,
            ).start()
        recv[phase, mine, :] = send[phase, mine, :]

    def wait_exchange(phase):
        span = pl.ds(0, (ga_n - 1) * 16)
        both = pltpu.make_async_remote_copy(
            src_ref=send.at[phase, span, :],
            dst_ref=recv.at[phase, span, :],
            send_sem=send_sem.at[phase],
            recv_sem=recv_sem.at[phase],
            device_id={"ga": lax.rem(me + 1, ga_n)},
            device_id_type=MESH,
        )
        both.wait()

    def got_rows(phase, row):
        return recv[phase, pl.ds(row, ga_n, stride=16), :]

    def spread_rows(ref_send, ref_recv, sem):
        for other in others:
            pltpu.make_async_remote_copy(
                src_ref=ref_send, dst_ref=ref_recv.at[me], send_sem=send_sem.at[sem], recv_sem=recv_sem.at[sem],
                device_id={"ga": other}, device_id_type=MESH,
            ).start()

    def spread_band(ref_send, ref_recv, sem):
        for other in other_bands:
            pltpu.make_async_remote_copy(
                src_ref=ref_send, dst_ref=ref_recv, send_sem=send_sem.at[sem], recv_sem=recv_sem.at[sem],
                device_id={"band": other}, device_id_type=MESH,
            ).start()

    def wait_rows(ref_recv, sem, count, axis, size, mine):
        span = ref_recv.at[pl.ds(0, count)]
        pltpu.make_async_remote_copy(
            src_ref=span, dst_ref=span, send_sem=send_sem.at[sem], recv_sem=recv_sem.at[sem],
            device_id={axis: lax.rem(mine + 1, size)}, device_id_type=MESH,
        ).wait()

    def cell(row, at):
        return jnp.sum(jnp.where(lane == at, row, 0.0), axis=1, keepdims=True)

    def fold(x):
        total = x[:, :128]
        for k in range(1, tiles):
            total = total + x[:, k * 128 : k * 128 + 128]
        return total[0:1] + total[1:2]

    def as_row(folded):
        stack = jnp.concatenate(folded + [jnp.zeros((1, 128), F32)] * (-len(folded) % 8), axis=0)
        col = jnp.sum(stack, axis=1, keepdims=True)
        hit = iota(stack.shape, 0) == iota(stack.shape, 1)
        return jnp.sum(jnp.where(hit, col, 0.0), axis=0, keepdims=True)

    def start_sums(which, row):
        row_send[which] = row
        spread_rows(row_send.at[which], row_recv.at[which], 6 + which)
        row_recv[which, me] = row_send[which]

    def end_sums(which):
        wait_rows(row_recv.at[which], 6 + which, ga_n - 1, "ga", ga_n, me)
        return jnp.sum(row_recv[which], axis=0) * (1.0 / total_pw)

    def all_sums(which, folded):
        start_sums(which, as_row(folded))
        total = end_sums(which)
        return total

    def apply_h(turn, v):
        t_all = None
        for k in range(0, pw, 256):
            lanes = slice(k, k + 256)
            e_c, e_s = e_tab[:grid_len, lanes], e_tab[grid_len:, lanes]
            v_re, v_im = v[0:1, lanes], v[1:2, lanes]
            hi_re, lo_re = split(e_c * v_re - e_s * v_im)
            hi_im, lo_im = split(e_s * v_re + e_c * v_im)
            got = dot(jnp.concatenate([hi_re, hi_im, lo_re, lo_im], axis=0), at_s[lanes, :])
            t_all = got if t_all is None else t_all + got
        t_all = t_all[: 2 * grid_len] + t_all[2 * grid_len :]

        if turn == 0:
            loads[3].wait()
        u = []
        for i in range(planes):
            lanes = slice(i * 128, i * 128 + 128)
            t_i = jnp.concatenate([t_all[:grid_len, lanes], t_all[grid_len:, lanes]], axis=1)
            hi, lo = split(jnp.concatenate([t_i, jnp.zeros((128 - grid_len, 256), F32)], axis=0))
            u.append(dot(tabs[0], hi, NT) + dot(tabs[0], lo, NT) + dot(tabs[1], hi, NT))
        for j in range(planes):
            six = []
            for i in range(planes):
                for c in range(2):
                    at = c * grid_len + j * ga_n
                    six.append(u[i][at : at + ga_n])
            for t, piece in enumerate(pack(*six)):
                put(2 * turn, j * 5 + t, piece)
        if turn == 0:
            pl.semaphore_wait(barrier, ga_n - 1 + band_n - 1)
        exchange(2 * turn)

        if turn == 0:
            loads[4].wait()
        acc_re = jnp.zeros((proj_n, 128), F32)
        acc_im = jnp.zeros((proj_n, 128), F32)
        for k in range(tiles):
            lanes = slice(k * 128, k * 128 + 128)
            p_re, p_im = pj[0, :, lanes], pj[1, :, lanes]
            v_re, v_im = v[0:1, lanes], v[1:2, lanes]
            acc_re = acc_re + (p_re * v_re + p_im * v_im)
            acc_im = acc_im + (p_re * v_im - p_im * v_re)
        col_re = jnp.sum(acc_re, axis=1, keepdims=True)
        col_im = jnp.sum(acc_im, axis=1, keepdims=True)
        row64, lane64 = iota((proj_n, 128), 0), iota((proj_n, 128), 1)
        diag = jnp.where(lane64 == row64, col_re, jnp.where(lane64 == row64 + proj_n, col_im, 0.0))
        start_sums(3 + turn, jnp.sum(diag, axis=0, keepdims=True))
        norm_row = None
        if turn == 0:
            norm_row = as_row([fold(v * v), fold(v * v * kin_ref[...])])
            later_tables()
            loads[5].wait()
        wait_exchange(2 * turn)

        cols = []
        for j in range(planes):
            pieces = unpack(*[got_rows(2 * turn, j * 5 + t) for t in range(5)])
            cols.append(jnp.concatenate(pieces[0::2] + pieces[1::2], axis=0))
        hi, lo = split(jnp.concatenate(cols, axis=1))
        x_h, x_l = tabs[2, :, : 2 * grid_len], tabs[3, :, : 2 * grid_len]
        w = dot(x_h, hi) + dot(x_h, lo) + dot(x_l, hi)
        w_re, w_im = w[:grid_len], w[grid_len:]
        blank = jnp.zeros((grid_len, 128 - grid_len), F32)
        v_tab = jnp.concatenate([x for j in range(planes) for x in (pot[j], blank)], axis=1)
        vw_re, vw_im = v_tab * w_re, v_tab * w_im
        if turn == 0:
            dens = jnp.sum(vw_re * w_re + vw_im * w_im, axis=0, keepdims=True)
            dens = dens[:, :128] + dens[:, 128:256] + dens[:, 256:]
            dens = jnp.sum(dens, axis=1, keepdims=True)
            put(1, 15, jnp.broadcast_to(jnp.where(lane == 2, dens, norm_row), (ga_n, 128)))
        hi, lo = split(jnp.concatenate([vw_re, vw_im], axis=0))
        x_h, x_l = tabs[4, :, : 2 * grid_len], tabs[5, :, : 2 * grid_len]
        back = dot(x_h, hi) + dot(x_h, lo) + dot(x_l, hi)
        for j in range(planes):
            lanes = slice(j * 128, j * 128 + 128)
            six = []
            for i in range(planes):
                for c in range(2):
                    at = c * grid_len + i * ga_n
                    six.append(back[at : at + ga_n, lanes])
            for t, piece in enumerate(pack(*six)):
                put(2 * turn + 1, j * 5 + t, piece)
        exchange(2 * turn + 1)

        tot = end_sums(3 + turn)
        prod = coup[...] * tot
        mix_re = jnp.sum(jnp.where(lane64 < proj_n, prod, 0.0), axis=1, keepdims=True)
        mix_im = jnp.sum(jnp.where(lane64 < proj_n, 0.0, prod), axis=1, keepdims=True)
        c_n = None
        if turn == 0:
            diag_row = jnp.where(lane64 == row64, mix_re, jnp.where(lane64 == row64 + proj_n, mix_im, 0.0))
            c_n = jnp.sum(jnp.sum(diag_row, axis=0, keepdims=True) * tot, axis=1, keepdims=True)
        for k in range(tiles):
            lanes = slice(k * 128, k * 128 + 128)
            p_re, p_im = pj[0, :, lanes], pj[1, :, lanes]
            n_re = jnp.sum(p_re * mix_re - p_im * mix_im, axis=0, keepdims=True)
            n_im = jnp.sum(p_im * mix_re + p_re * mix_im, axis=0, keepdims=True)
            hvec[:, lanes] = jnp.concatenate([n_re, n_im], axis=0) + kin_ref[:, lanes] * v[:, lanes]
        wait_exchange(2 * turn + 1)

        zs = [[None] * planes for _ in range(2 * planes)]
        for j in range(planes):
            pieces = unpack(*[got_rows(2 * turn + 1, j * 5 + t) for t in range(5)])
            for n, piece in enumerate(pieces):
                zs[n][j] = piece
        outs = []
        for i in range(planes):
            stack = jnp.concatenate(zs[2 * i] + zs[2 * i + 1], axis=0)
            hi, lo = split(stack.T)
            out = dot(hi, tabs[6]) + dot(lo, tabs[6]) + dot(hi, tabs[7])
            outs.append(out[:grid_len])
        for c in range(2):
            first, second, third = [out[:, c * 128 : c * 128 + 128] for out in outs]
            late = roll(third, 64)
            rows, rows_lo = slice(c * grid_len, (c + 1) * grid_len), slice((2 + c) * grid_len, (3 + c) * grid_len)
            wide = lane < 96
            hi, lo = split(jnp.concatenate([jnp.where(wide, first, roll(third, 96)), jnp.where(wide, second, late)], axis=1))
            gt[rows, :] = hi
            gt[rows_lo, :] = lo
            high = late.astype(BF16).astype(F32)
            gt_rest[rows, :] = jnp.where(lane < 32, high, roll(late - high, 32)).astype(BF16)
        for k in range(0, pw, 256):
            lanes = slice(k, k + 256)
            q = dot(gt[...], at_g[:256, lanes])
            q = q[: 2 * grid_len] + q[2 * grid_len :] + dot(gt_rest[:, :64], at_g[256:, lanes])
            q_re, q_im = q[:grid_len], q[grid_len:]
            e_c, e_s = e_tab[:grid_len, lanes], e_tab[grid_len:, lanes]
            l_re = jnp.sum(e_c * q_re + e_s * q_im, axis=0, keepdims=True)
            l_im = jnp.sum(e_c * q_im - e_s * q_re, axis=0, keepdims=True)
            hvec[:, lanes] = hvec[:, lanes] + jnp.concatenate([l_re, l_im], axis=0)
        return c_n

    def precondition(r, level):
        ratio = kin_ref[...] / (1.5 * level + 1.0)
        numer = 27.0 + ratio * (18.0 + ratio * (12.0 + 8.0 * ratio))
        square = ratio * ratio
        return r * (numer / (numer + 16.0 * square * square))

    eps = small_eps

    loads[2].wait()
    vecs[0] = jnp.concatenate([cf[0], cf[1]], axis=0)
    c_n = apply_h(0, vecs[0])
    tot = jnp.sum(got_rows(1, 15), axis=0, keepdims=True) * (1.0 / total_pw)
    guess_cc = cell(tot, 0)
    guess = (cell(tot, 1) + cell(tot, 2) * (1.0 / grid_len**3) + c_n) / (guess_cc + eps)
    c = vecs[0]
    h0 = hvec[...]
    s = h0 - guess * c
    kc, ks = kin_ref[...] * c, kin_ref[...] * s
    tot = all_sums(0, [fold(c * c), fold(c * s), fold(s * s), fold(kc * c), fold(kc * s), fold(ks * s)])
    cc, cs, ss, kcc, kcs, kss = [cell(tot, n) for n in range(6)]
    shift = (cs - guess * eps) / (cc + eps)
    e0 = guess + shift
    r0 = s - shift * c
    rr = ss - 2.0 * shift * cs + shift * shift * cc
    krr = kss - 2.0 * shift * kcs + shift * shift * kcc
    rc = cs - shift * cc
    krc = kcs - shift * kcc
    p0 = precondition(r0, krr / (rr + eps))
    vecs[1] = r0
    vecs[2] = p0
    vecs[3] = h0

    apply_h(1, vecs[2])
    c, r0, p0, h0 = vecs[0], vecs[1], vecs[2], vecs[3]
    g0 = hvec[...]
    q0 = g0 - e0 * p0
    pairs = [(r0, q0), (r0, p0), (q0, q0), (q0, c), (q0, p0), (c, p0), (p0, p0)]
    prods = [a * b for a, b in pairs]
    tot = all_sums(1, [fold(x) for x in prods] + [fold(x * kin_ref[...]) for x in prods])
    rq, rp, qq, qc, qp, cp, pp = [cell(tot, n) for n in range(7)]
    krq, krp, kqq, kqc, kqp, kcp, kpp = [cell(tot, n) for n in range(7, 14)]
    l0 = -rq / (qq + eps)
    bb = cc + 2.0 * l0 * cp + l0 * l0 * pp
    b_rho = rc + l0 * (qc + rp) + l0 * l0 * qp
    d1 = (b_rho - e0 * eps) / (bb + eps)
    fa, fb, fc = -l0, d1, d1 * l0
    r_dr = fa * rq + fb * rc + fc * rp
    dr_dr = fa * fa * qq + fb * fb * cc + fc * fc * pp + 2.0 * (fa * fb * qc + fa * fc * qp + fb * fc * cp)
    kr_dr = fa * krq + fb * krc + fc * krp
    kdr_dr = fa * fa * kqq + fb * fb * kcc + fc * fc * kpp + 2.0 * (fa * fb * kqc + fa * fc * kqp + fb * fc * kcp)
    wt = r_dr / (dr_dr + eps)
    lm = wt * l0
    bmbm = cc + 2.0 * lm * cp + lm * lm * pp
    bm_rho = rc + lm * (qc + rp) + lm * lm * qp
    dm = (bm_rho - e0 * eps) / (bmbm + eps)
    em = e0 + dm
    mm = rr - 2.0 * wt * r_dr + wt * wt * dr_dr
    kmm = krr - 2.0 * wt * kr_dr + wt * wt * kdr_dr
    bm = c + lm * p0
    hm = h0 + lm * g0
    rm = r0 - wt * (fa * q0 + fb * c + fc * p0)
    sm = r0 + lm * q0 - dm * bm
    p1 = precondition(rm, kmm / (mm + eps))
    vecs[4] = bm
    vecs[5] = hm
    vecs[6] = rm
    vecs[7] = sm
    vecs[8] = p1
    slot8 = pl.ds(pl.multiple_of(my_band * 8, 8), 8)
    bands[slot8, :] = jnp.concatenate([bm, p1, bm, p1], axis=0)

    spread_band(bands.at[slot8, :], bands.at[slot8, :], 13)

    apply_h(2, vecs[8])
    bm, hm, rm, sm, p1 = vecs[4], vecs[5], vecs[6], vecs[7], vecs[8]
    g1 = hvec[...]
    q1 = g1 - em * p1
    start_sums(2, as_row([fold(rm * q1), fold(q1 * q1)]))
    span = bands.at[pl.ds(0, (band_n - 1) * 8), :]
    pltpu.make_async_remote_copy(
        src_ref=span, dst_ref=span, send_sem=send_sem.at[13], recv_sem=recv_sem.at[13],
        device_id={"band": other_bands[0]}, device_id_type=MESH,
    ).wait()
    left = jnp.concatenate([bm, p1, hm, g1], axis=0)
    gram = dot_full(left, bands[...], NT)
    wide = (band_n * 8, 128)
    moved = iota(wide, 0) % 8 * band_n + iota(wide, 0) // 8
    gram = dot_full(gram, jnp.where(moved == iota(wide, 1), 1.0, 0.0))
    pairs = [(sm, sm), (sm, q1), (sm, bm), (sm, p1), (q1, bm), (q1, p1), (bm, bm), (bm, p1), (p1, p1)]
    row = as_row([fold(a * b) for a, b in pairs])
    gram_send[:8, :] = gram
    gram_send[8:, :] = jnp.broadcast_to(row, (8, 128))
    spread_rows(gram_send, gram_recv, 9 + 3)
    gram_recv[me] = gram_send[...]
    tot = end_sums(2)
    rq, qq = cell(tot, 0), cell(tot, 1)
    l1 = -rq / (qq + eps)
    lam_send[...] = jnp.broadcast_to(l1, (1, 128))
    spread_band(lam_send, lam_recv.at[my_band], 14)
    lam_recv[my_band] = lam_send[...]
    wait_rows(gram_recv, 9 + 3, ga_n - 1, "ga", ga_n, me)
    summed = jnp.sum(gram_recv[...], axis=0) * (1.0 / total_pw)
    gram, tot = summed[:8], summed[8:9]
    ss, sq, sb, sp, qb, qp, bb, bp, pp = [cell(tot, n) for n in range(9)]

    new = bm + l1 * p1
    nb_out[0] = new[0:1]
    nb_out[1] = new[1:2]
    nn = bb + 2.0 * l1 * bp + l1 * l1 * pp
    n_sig = sb + l1 * (sp + qb) + l1 * l1 * qp
    sig_sig = ss + 2.0 * l1 * sq + l1 * l1 * qq
    shift = (n_sig - em * eps) / (nn + eps)
    energy = em + shift
    res = (sig_sig - 2.0 * shift * n_sig + shift * shift * nn) / (nn + eps)

    wait_rows(lam_recv, 14, band_n - 1, "band", band_n, my_band)
    lams = jnp.zeros((1, 128), F32)
    for j in range(band_n):
        lams = jnp.where(lane == j, lam_recv[j], lams)

    def part(rows, v):
        return rows[:, v * band_n : (v + 1) * band_n]

    lam8 = lams[:, :band_n]

    def finish(rows):
        a = rows[0:2] + l1 * rows[2:4]
        against_re = part(a, 0) + lam8 * part(a, 2)
        against_im = part(a, 1) + lam8 * part(a, 3)
        return (against_re[0:1] + against_im[1:2], against_im[0:1] - against_re[1:2])

    cor_re, cor_im = finish(gram[0:4])
    sub_re, sub_im = finish(gram[4:8])
    tail = jnp.concatenate([jnp.broadcast_to(energy, (1, band_n)), jnp.broadcast_to(res, (1, band_n))], axis=0)
    block = jnp.concatenate([cor_re, cor_im, sub_re, sub_im, tail, tail], axis=0)
    small_out[...] = jnp.concatenate([block, jnp.zeros((8, 128 - band_n), F32)], axis=1)


def body(tables, coeffs, cell_map, potential, projectors, strengths, proj_atom, proj_chan):
    ga_n = lax.axis_size("ga")
    band_n = lax.axis_size("band")
    grid_len = potential.shape[0]
    pw = coeffs.shape[2]
    proj_n = proj_atom.shape[0]
    total_pw = pw * ga_n
    vmem = pl.BlockSpec(memory_space=pltpu.VMEM)
    hbm = pl.BlockSpec(memory_space=pltpu.HBM)
    z_tab, tabs = tables
    args = (cell_map.reshape(pw // 128, 128), z_tab, coeffs, tabs, projectors, jnp.transpose(potential, (1, 0, 2)),
            strengths, proj_atom.reshape(1, proj_n), proj_chan.reshape(1, proj_n))
    V = pltpu.VMEM
    scratch = [V(a.shape, a.dtype) for a in args] + [
        V((pw, 3 * 128), BF16), V((320, pw), BF16), V((2 * grid_len, pw), F32),
        V((4 * grid_len, 256), BF16), V((2 * grid_len, 128), BF16),
        V((proj_n, 2 * proj_n), F32), V((9, 2, pw), F32), V((2, pw), F32), V((1, pw), F32),
        V((6, ga_n * 16, 128), F32), V((6, ga_n * 16, 128), F32),
        V((6, 1, 128), F32), V((6, ga_n, 1, 128), F32),
        V((16, 128), F32), V((ga_n, 16, 128), F32),
        V((band_n * 8, pw), F32), V((1, 128), F32), V((band_n, 1, 128), F32),
        pltpu.SemaphoreType.DMA((15,)), pltpu.SemaphoreType.DMA((15,)), pltpu.SemaphoreType.DMA((len(args),)),
    ]
    args = [pltpu.with_memory_space_constraint(a, pltpu.HBM) for a in args]
    new_bands, small = pl.pallas_call(
        functools.partial(kernel, (ga_n, band_n, grid_len, total_pw)),
        out_shape=(
            jax.ShapeDtypeStruct((2, 1, pw), F32),
            jax.ShapeDtypeStruct((8, 128), F32),
        ),
        in_specs=[hbm] * len(args),
        out_specs=(vmem, vmem),
        scratch_shapes=scratch,
        compiler_params=pltpu.CompilerParams(collective_id=0, has_side_effects=True, vmem_limit_bytes=24 * 2**20),
    )(*args)

    def deal(nb, sm, nb_o, en_o, re_o, co_o, su_o):
        nb_o[...] = nb[...]
        co_o[0], co_o[1] = sm[0:1, :band_n], sm[1:2, :band_n]
        su_o[0], su_o[1] = sm[2:3, :band_n], sm[3:4, :band_n]
        en_o[...] = sm[4:5, :1]
        re_o[...] = sm[5:6, :1]

    one = jax.ShapeDtypeStruct((1, 1), F32)
    rows = jax.ShapeDtypeStruct((2, 1, band_n), F32)
    new_bands, energy, res, corr, sub = pl.pallas_call(
        deal,
        out_shape=(jax.ShapeDtypeStruct((2, 1, pw), F32), one, one, rows, rows),
        in_specs=[vmem] * 2,
        out_specs=(vmem,) * 5,
        compiler_params=pltpu.CompilerParams(vmem_limit_bytes=2**20),
    )(new_bands, small)
    return new_bands, energy.reshape(1), res.reshape(1), corr, sub


def solution(mesh):
    tables = make_tables(96, mesh.shape["ga"])
    placed = (P(None, "band", "ga"), P("ga"), P(None, "ga", None), P(None, None, "ga"), P(), P(), P())
    return jax.shard_map(
        functools.partial(body, tables),
        mesh=mesh,
        in_specs=placed,
        out_specs=(P(None, "band", "ga"), P("band"), P("band"), P(None, "band", None), P(None, "band", None)),
        check_vma=False,
    )
```

```python
import functools

import jax
import jax.numpy as jnp
import numpy as np
from jax import lax
from jax.experimental import pallas as pl
from jax.experimental.pallas import tpu as pltpu
from jax.sharding import PartitionSpec as P

F32 = jnp.float32
BF16 = jnp.bfloat16
HIGHEST = lax.Precision.HIGHEST
MESH = pl.DeviceIdType.MESH
kin_unit = 0.02
small_eps = 1e-06

NN = (((1,), (0,)), ((), ()))
NT = (((1,), (1,)), ((), ()))
TN = (((0,), (0,)), ((), ()))


def parts_of(table, count):
    out = []
    left = np.asarray(table, np.float64)
    for _ in range(count):
        piece = left.astype(np.float32).astype(BF16)
        out.append(piece)
        left = left - piece.astype(np.float64)
    return out


def make_tables(grid_len, groups):
    planes = grid_len // groups
    natural = np.arange(grid_len)
    slab = (natural % groups) * planes + natural // groups

    def angles(rows, cols):
        return 2.0 * np.pi / grid_len * ((rows[:, None] * cols[None, :]) % grid_len)

    z_ang = angles(natural, natural)
    x_cos, x_sin = np.cos(z_ang), np.sin(z_ang)
    half = grid_len // 2
    z_high, z_low = parts_of(np.concatenate([x_cos[:half], x_sin[:half], x_cos[half:], x_sin[half:]], axis=0), 2)
    y_ang = angles(slab, natural)
    y_cos, y_sin = np.cos(y_ang), np.sin(y_ang)
    pad = np.zeros((grid_len, 128 - grid_len))
    side = np.zeros((2 * grid_len, 256 - 2 * grid_len))
    y_fwd = np.block([[y_cos, pad, -y_sin, pad], [y_sin, pad, y_cos, pad]])
    x_fwd = np.block([[x_cos, -x_sin], [x_sin, x_cos]])
    x_back = np.block([[x_cos, x_sin], [-x_sin, x_cos]]) / grid_len
    x_fwd, x_back = np.concatenate([x_fwd, side], axis=1), np.concatenate([x_back, side], axis=1)
    y_back = y_fwd / grid_len**2
    rest = []
    for tab in (y_fwd, x_fwd, x_back, y_back):
        rest += parts_of(tab, 2)
    return [np.concatenate([z_high, z_low], axis=1), np.stack(rest)]


def dot(a, b, dims=NN):
    return lax.dot_general(a, b, dims, preferred_element_type=F32)


def dot_full(a, b, dims=NN):
    return lax.dot_general(a, b, dims, precision=HIGHEST, preferred_element_type=F32)


def split(x):
    hi = x.astype(BF16)
    return hi, (x - hi.astype(F32)).astype(BF16)


def iota(shape, axis):
    return lax.broadcasted_iota(jnp.int32, shape, axis)


def ring_steps(groups):
    side = 4
    cores = groups // (side * side)

    def hops(k):
        return min(k, side - k)

    steps = [(i, j, c) for i in range(side) for j in range(side) for c in range(cores) if (i, j, c) != (0, 0, 0)]
    return sorted(steps, key=lambda s: -(hops(s[0]) + hops(s[1])))


def kernel(sizes, cm_far, zt_far, cf_far, tabs_far, pj_far, pot_far, st_far, pa_far, pc_far,
           nb_out, small_out,
           cm, zt, cf, tabs, pj, pot, st, pa, pc, at_s, at_g, e_tab, gt, gt_rest, v_tab, coup, vecs, hvec, kin_ref,
           send, recv, row_send, row_recv, gram_send, gram_recv, bands, lam_send, lam_recv,
           send_sem, recv_sem, load_sem):
    ga_n, band_n, grid_len, total_pw = sizes
    planes = grid_len // ga_n
    me = lax.axis_index("ga")
    my_band = lax.axis_index("band")
    pw = cf.shape[2]
    tiles = pw // 128
    far = (cm_far, zt_far, cf_far, tabs_far, pj_far, pot_far, st_far, pa_far, pc_far)
    near = (cm, zt, cf, tabs, pj, pot, st, pa, pc)
    loads = [pltpu.make_async_copy(a, b, load_sem.at[n]) for n, (a, b) in enumerate(zip(far, near))]
    loads[0].start()
    loads[1].start()

    barrier = pltpu.get_barrier_semaphore()
    m_x, m_y, m_c = me // 8, me // 2 % 4, me % 2

    def at_step(step):
        return ((m_x + step[0]) % 4) * 8 + ((m_y + step[1]) % 4) * 2 + (m_c + step[2]) % 2

    others = [at_step(step) for step in ring_steps(ga_n)]
    band_order = sorted(range(1, band_n), key=lambda k: -min(k, band_n - k))
    other_bands = [lax.rem(my_band + k, band_n) for k in band_order]

    for other in others:
        pl.semaphore_signal(barrier, inc=1, device_id={"ga": other}, device_id_type=MESH)
    for other in other_bands:
        pl.semaphore_signal(barrier, inc=1, device_id={"band": other}, device_id_type=MESH)

    for load in loads[2:]:
        load.start()
    zeros = jnp.zeros((ga_n, 128), F32)
    for lot in range(12):
        send[lot, pl.ds(7, ga_n, stride=8), :] = zeros
    loads[0].wait()
    loads[1].wait()

    cells = cm[...]
    py = lax.shift_right_logical(cells * 43691, 22)
    z_idx = cells - py * grid_len
    plane = (py >= grid_len).astype(jnp.int32) + (py >= 2 * grid_len).astype(jnp.int32)
    y_idx = py - plane * grid_len
    x_idx = me + ga_n * plane
    py_pad = plane * 128 + y_idx

    def freq(k):
        return jnp.where(2 * k < grid_len, k, k - grid_len).astype(F32)

    kin = kin_unit * (freq(x_idx) * freq(x_idx) + freq(y_idx) * freq(y_idx) + freq(z_idx) * freq(z_idx))
    for k in range(tiles):
        lanes = slice(k * 128, k * 128 + 128)
        kin_ref[:, lanes] = kin[k : k + 1]
        hot = (iota((grid_len, 128), 0) == z_idx[k : k + 1])
        hot = jnp.where(hot, 1.0, 0.0).astype(BF16)
        e_tab[:, lanes] = dot(zt[...], jnp.concatenate([hot, hot], axis=0))
    upright = jnp.transpose(jnp.concatenate([py_pad, jnp.zeros((128 - tiles, 128), jnp.int32)], axis=0))
    for k in range(tiles):
        hot = (iota((128, 3 * 128), 1) == upright[:, k : k + 1])
        at_s[k * 128 : k * 128 + 128, :] = jnp.where(hot, 1.0, 0.0).astype(BF16)
    half_len = grid_len // 2

    def later_tables():
        for load in loads[5:]:
            load.wait()
        blank = jnp.zeros((grid_len, 128 - grid_len), F32)
        at = iota((grid_len, 128), 1)
        slabs = [jnp.concatenate([pot[j], blank], axis=1) for j in range(planes)]
        for h in range(2):
            first, second, third = [moved_by(slabs[j], 48 * j - 48 * h) for j in range(planes)]
            v_tab[h, :, :128] = jnp.where(at < 48, first, jnp.where(at < 96, second, third))
            v_tab[h, :, 128:] = jnp.where(at < 16, moved_by(slabs[2], -48 * h - 32), 0.0)
        place = jnp.where(plane == 2, jnp.where(y_idx < 32, 96 + y_idx, 192 + y_idx), plane * 128 + y_idx)
        for k in range(tiles):
            lanes = slice(k * 128, k * 128 + 128)
            hot = jnp.where(iota((288, 128), 0) == place[k : k + 1], 1.0, 0.0).astype(BF16)
            at_g[:288, lanes] = hot
            at_g[288:, lanes] = hot[256:]
        chans = st.shape[1]
        sym_rows = st[...].reshape(st.shape[0] * chans, chans)
        slot = pa[...] * chans + pc[...]
        hot_p = jnp.where(iota((proj_n, proj_n), 0) == slot, 1.0, 0.0)
        hot_c = jnp.where(iota((chans, proj_n), 0) == pc[...], 1.0, 0.0)
        reach = dot_full(sym_rows, hot_c)
        reach = jnp.where(iota((proj_n, proj_n), 0) // chans == pa[...], reach, 0.0)
        half = 0.5 * (dot_full(hot_p, reach, TN) + dot_full(reach, hot_p, TN))
        coup[...] = jnp.concatenate([half, half], axis=1)

    proj_n = pa.shape[1]
    lane = iota((1, 128), 1)
    lane32 = iota((ga_n, 128), 1)

    def roll(x, by):
        return pltpu.roll(x, by, 1)

    lane16 = lane32 // 16

    def gather_rest(pieces):
        rest = pieces[0]
        for n in range(1, 6):
            rest = jnp.where(lane16 == n, roll(pieces[n], 16 * n), rest)
        return rest

    def moved_by(x, by):
        return x if by % 128 == 0 else roll(x, by % 128)

    def put(lot, row, value):
        send[lot, pl.ds(row, ga_n, stride=8), :] = value

    def exchange(lot):
        mine = pl.ds(pl.multiple_of(me * 8, 8), 8)
        for other in others:
            pltpu.make_async_remote_copy(
                src_ref=send.at[lot, pl.ds(pl.multiple_of(other * 8, 8), 8), :],
                dst_ref=recv.at[lot, mine, :],
                send_sem=send_sem.at[lot],
                recv_sem=recv_sem.at[lot],
                device_id={"ga": other},
                device_id_type=MESH,
            ).start()
        recv[lot, mine, :] = send[lot, mine, :]

    def wait_exchange(lot):
        span = pl.ds(0, (ga_n - 1) * 8)
        pltpu.make_async_remote_copy(
            src_ref=send.at[lot, span, :],
            dst_ref=recv.at[lot, span, :],
            send_sem=send_sem.at[lot],
            recv_sem=recv_sem.at[lot],
            device_id={"ga": others[0]},
            device_id_type=MESH,
        ).wait()

    def got_rows(lot, row):
        return recv[lot, pl.ds(row, ga_n, stride=8), :]

    def spread_rows(ref_send, ref_recv, sem):
        for other in others:
            pltpu.make_async_remote_copy(
                src_ref=ref_send, dst_ref=ref_recv.at[me], send_sem=send_sem.at[sem], recv_sem=recv_sem.at[sem],
                device_id={"ga": other}, device_id_type=MESH,
            ).start()

    def spread_band(ref_send, ref_recv, sem):
        for other in other_bands:
            pltpu.make_async_remote_copy(
                src_ref=ref_send, dst_ref=ref_recv, send_sem=send_sem.at[sem], recv_sem=recv_sem.at[sem],
                device_id={"band": other}, device_id_type=MESH,
            ).start()

    def wait_rows(ref_recv, sem, count, axis, size, mine):
        span = ref_recv.at[pl.ds(0, count)]
        pltpu.make_async_remote_copy(
            src_ref=span, dst_ref=span, send_sem=send_sem.at[sem], recv_sem=recv_sem.at[sem],
            device_id={axis: lax.rem(mine + 1, size)}, device_id_type=MESH,
        ).wait()

    def cell(row, at):
        return jnp.sum(jnp.where(lane == at, row, 0.0), axis=1, keepdims=True)

    def fold(x):
        total = x[:, :128]
        for k in range(1, tiles):
            total = total + x[:, k * 128 : k * 128 + 128]
        return total[0:1] + total[1:2]

    def as_row(folded):
        stack = jnp.concatenate(folded + [jnp.zeros((1, 128), F32)] * (-len(folded) % 8), axis=0)
        col = jnp.sum(stack, axis=1, keepdims=True)
        hit = iota(stack.shape, 0) == iota(stack.shape, 1)
        return jnp.sum(jnp.where(hit, col, 0.0), axis=0, keepdims=True)

    def start_sums(which, row):
        row_send[which] = row
        spread_rows(row_send.at[which], row_recv.at[which], 12 + which)
        row_recv[which, me] = row_send[which]

    def end_sums(which):
        wait_rows(row_recv.at[which], 12 + which, ga_n - 1, "ga", ga_n, me)
        return jnp.sum(row_recv[which], axis=0) * (1.0 / total_pw)

    def all_sums(which, folded):
        start_sums(which, as_row(folded))
        total = end_sums(which)
        return total

    def apply_h(turn, v):
        base = (0, 48, 0)
        for h in range(2):
            t_all = None
            for k in range(0, pw, 256):
                lanes = slice(k, k + 256)
                e_c = e_tab[h * grid_len : h * grid_len + half_len, lanes]
                e_s = e_tab[h * grid_len + half_len : (h + 1) * grid_len, lanes]
                v_re, v_im = v[0:1, lanes], v[1:2, lanes]
                hi_re, lo_re = split(e_c * v_re - e_s * v_im)
                hi_im, lo_im = split(e_s * v_re + e_c * v_im)
                got = dot(jnp.concatenate([hi_re, hi_im, lo_re, lo_im], axis=0), at_s[lanes, :])
                t_all = got if t_all is None else t_all + got
            t_all = t_all[:grid_len] + t_all[grid_len:]
            if turn == 0 and h == 0:
                loads[3].wait()
            rows = []
            for i in range(planes):
                lanes = slice(i * 128, i * 128 + 128)
                rows.append(jnp.concatenate([t_all[:half_len, lanes], t_all[half_len:, lanes]], axis=1))
            rows.insert(2, jnp.zeros((32, 256), F32))
            hi, lo = split(jnp.concatenate(rows, axis=0))
            u = dot(tabs[0], hi, NT) + dot(tabs[0], lo, NT) + dot(tabs[1], hi, NT)
            u = (u[:, :128], u[:, 128:])
            rest = []
            for c in range(2):
                for i in range(planes):
                    spread = []
                    for j in range(planes):
                        at = c * grid_len + j * ga_n
                        piece = u[i // 2][at : at + ga_n]
                        if i == 2:
                            piece = jnp.concatenate([piece, jnp.zeros((ga_n, 128 - half_len), F32)], axis=1)
                        spread.append(moved_by(piece, 48 * j - base[i]))
                    put(4 * turn + h, c * planes + i,
                        jnp.where(lane32 < 48, spread[0], jnp.where(lane32 < 96, spread[1], spread[2])))
                    rest.append(spread[2])
            put(4 * turn + h, 6, gather_rest(rest))
            if turn == 0 and h == 0:
                pl.semaphore_wait(barrier, ga_n - 1 + band_n - 1)
            exchange(4 * turn + h)

        if turn == 0:
            loads[4].wait()
        acc_re = jnp.zeros((proj_n, 128), F32)
        acc_im = jnp.zeros((proj_n, 128), F32)
        for k in range(tiles):
            lanes = slice(k * 128, k * 128 + 128)
            p_re, p_im = pj[0, :, lanes], pj[1, :, lanes]
            v_re, v_im = v[0:1, lanes], v[1:2, lanes]
            acc_re = acc_re + (p_re * v_re + p_im * v_im)
            acc_im = acc_im + (p_re * v_im - p_im * v_re)
        col_re = jnp.sum(acc_re, axis=1, keepdims=True)
        col_im = jnp.sum(acc_im, axis=1, keepdims=True)
        row64, lane64 = iota((proj_n, 128), 0), iota((proj_n, 128), 1)
        diag = jnp.where(lane64 == row64, col_re, jnp.where(lane64 == row64 + proj_n, col_im, 0.0))
        start_sums(3 + turn, jnp.sum(diag, axis=0, keepdims=True))
        norm_row = None
        if turn == 0:
            norm_row = as_row([fold(v * v), fold(v * v * kin_ref[...])])
            later_tables()
        if turn == 2:
            spread_band(bands.at[my_band], bands.at[my_band], 19)
        for h in range(2):
            lot = 4 * turn + h
            wait_exchange(lot)
            rest = got_rows(lot, 6)
            main = jnp.concatenate([got_rows(lot, n) for n in range(6)], axis=0)
            side = jnp.concatenate([moved_by(rest, -16 * n) for n in range(6)], axis=0)
            hi, lo = split(jnp.concatenate([main, side], axis=1))
            x_h, x_l = tabs[2, :, : 2 * grid_len], tabs[3, :, : 2 * grid_len]
            w = dot(x_h, hi) + dot(x_h, lo) + dot(x_l, hi)
            w_re, w_im = w[:grid_len], w[grid_len:]
            vw_re, vw_im = v_tab[h] * w_re, v_tab[h] * w_im
            lot = 4 * turn + 2 + h
            if turn == 0:
                dens = jnp.sum(vw_re * w_re + vw_im * w_im, axis=0, keepdims=True)
                dens = jnp.sum(dens[:, :128] + dens[:, 128:], axis=1, keepdims=True)
                row = norm_row if h == 0 else jnp.zeros((1, 128), F32)
                put(lot, 7, jnp.broadcast_to(jnp.where(lane == 2, dens, row), (ga_n, 128)))
            hi, lo = split(jnp.concatenate([vw_re, vw_im], axis=0))
            x_h, x_l = tabs[4, :, : 2 * grid_len], tabs[5, :, : 2 * grid_len]
            back = dot(x_h, hi) + dot(x_h, lo) + dot(x_l, hi)
            for n in range(6):
                put(lot, n, back[n * ga_n : (n + 1) * ga_n, :128])
            put(lot, 6, gather_rest([back[n * ga_n : (n + 1) * ga_n, 128:] for n in range(6)]))
            exchange(lot)

        tot = end_sums(3 + turn)
        prod = coup[...] * tot
        mix_re = jnp.sum(jnp.where(lane64 < proj_n, prod, 0.0), axis=1, keepdims=True)
        mix_im = jnp.sum(jnp.where(lane64 < proj_n, 0.0, prod), axis=1, keepdims=True)
        c_n = None
        if turn == 0:
            diag_row = jnp.where(lane64 == row64, mix_re, jnp.where(lane64 == row64 + proj_n, mix_im, 0.0))
            c_n = jnp.sum(jnp.sum(diag_row, axis=0, keepdims=True) * tot, axis=1, keepdims=True)
        for k in range(tiles):
            lanes = slice(k * 128, k * 128 + 128)
            p_re, p_im = pj[0, :, lanes], pj[1, :, lanes]
            n_re = jnp.sum(p_re * mix_re - p_im * mix_im, axis=0, keepdims=True)
            n_im = jnp.sum(p_im * mix_re + p_re * mix_im, axis=0, keepdims=True)
            hvec[:, lanes] = jnp.concatenate([n_re, n_im], axis=0) + kin_ref[:, lanes] * v[:, lanes]
        for h in range(2):
            lot = 4 * turn + 2 + h
            wait_exchange(lot)
            rest = got_rows(lot, 6)
            left, right = [], []
            for c in range(2):
                mains = [got_rows(lot, c * planes + i) for i in range(planes)]
                for j in range(planes):
                    pieces = []
                    for i in range(planes):
                        piece = moved_by(mains[i], base[i] - 48 * j)
                        if j == 2:
                            late = moved_by(rest, base[i] + 32 - 16 * (c * planes + i))
                            piece = jnp.where(lane32 < base[i] + 32, piece, late)
                        pieces.append(piece)
                    left.append(jnp.where(lane32 < 48, pieces[0], pieces[1]))
                    right.append(pieces[2])
            left, right = jnp.concatenate(left, axis=0).T, jnp.concatenate(right, axis=0).T
            hi, lo = split(jnp.concatenate([left[:grid_len], right[:half_len]], axis=0))
            out = dot(hi, tabs[6]) + dot(lo, tabs[6]) + dot(hi, tabs[7])
            for c in range(2):
                first, second, third = [out[i * half_len : (i + 1) * half_len, c * 128 : c * 128 + 128] for i in range(planes)]
                late = roll(third, 64)
                rows = slice(c * half_len, (c + 1) * half_len)
                rows_lo = slice((2 + c) * half_len, (3 + c) * half_len)
                wide = lane < 96
                hi, lo = split(jnp.concatenate([jnp.where(wide, first, roll(third, 96)), jnp.where(wide, second, late)], axis=1))
                gt[h, rows, :] = hi
                gt[h, rows_lo, :] = lo
                high = late.astype(BF16).astype(F32)
                gt_rest[h, rows, :] = jnp.where(lane < 32, high, roll(late - high, 32)).astype(BF16)
            for k in range(0, pw, 256):
                lanes = slice(k, k + 256)
                q = dot(gt[h], at_g[:256, lanes])
                q = q[:grid_len] + q[grid_len:] + dot(gt_rest[h, :, :64], at_g[256:, lanes])
                q_re, q_im = q[:half_len], q[half_len:]
                e_c = e_tab[h * grid_len : h * grid_len + half_len, lanes]
                e_s = e_tab[h * grid_len + half_len : (h + 1) * grid_len, lanes]
                l_re = jnp.sum(e_c * q_re + e_s * q_im, axis=0, keepdims=True)
                l_im = jnp.sum(e_c * q_im - e_s * q_re, axis=0, keepdims=True)
                hvec[:, lanes] = hvec[:, lanes] + jnp.concatenate([l_re, l_im], axis=0)
        return c_n

    def precondition(r, level):
        ratio = kin_ref[...] / (1.5 * level + 1.0)
        numer = 27.0 + ratio * (18.0 + ratio * (12.0 + 8.0 * ratio))
        square = ratio * ratio
        return r * (numer / (numer + 16.0 * square * square))

    eps = small_eps

    loads[2].wait()
    vecs[0] = jnp.concatenate([cf[0], cf[1]], axis=0)
    c_n = apply_h(0, vecs[0])
    tot = jnp.sum(got_rows(2, 7) + got_rows(3, 7), axis=0, keepdims=True) * (1.0 / total_pw)
    guess_cc = cell(tot, 0)
    guess = (cell(tot, 1) + cell(tot, 2) * (1.0 / grid_len**3) + c_n) / (guess_cc + eps)
    c = vecs[0]
    h0 = hvec[...]
    s = h0 - guess * c
    kc, ks = kin_ref[...] * c, kin_ref[...] * s
    tot = all_sums(0, [fold(c * c), fold(c * s), fold(s * s), fold(kc * c), fold(kc * s), fold(ks * s)])
    cc, cs, ss, kcc, kcs, kss = [cell(tot, n) for n in range(6)]
    shift = (cs - guess * eps) / (cc + eps)
    e0 = guess + shift
    r0 = s - shift * c
    rr = ss - 2.0 * shift * cs + shift * shift * cc
    krr = kss - 2.0 * shift * kcs + shift * shift * kcc
    rc = cs - shift * cc
    krc = kcs - shift * kcc
    p0 = precondition(r0, krr / (rr + eps))
    vecs[1] = r0
    vecs[2] = p0
    vecs[3] = h0

    apply_h(1, vecs[2])
    c, r0, p0, h0 = vecs[0], vecs[1], vecs[2], vecs[3]
    g0 = hvec[...]
    q0 = g0 - e0 * p0
    pairs = [(r0, q0), (r0, p0), (q0, q0), (q0, c), (q0, p0), (c, p0), (p0, p0)]
    prods = [a * b for a, b in pairs]
    tot = all_sums(1, [fold(x) for x in prods] + [fold(x * kin_ref[...]) for x in prods])
    rq, rp, qq, qc, qp, cp, pp = [cell(tot, n) for n in range(7)]
    krq, krp, kqq, kqc, kqp, kcp, kpp = [cell(tot, n) for n in range(7, 14)]
    l0 = -rq / (qq + eps)
    bb = cc + 2.0 * l0 * cp + l0 * l0 * pp
    b_rho = rc + l0 * (qc + rp) + l0 * l0 * qp
    d1 = (b_rho - e0 * eps) / (bb + eps)
    fa, fb, fc = -l0, d1, d1 * l0
    r_dr = fa * rq + fb * rc + fc * rp
    dr_dr = fa * fa * qq + fb * fb * cc + fc * fc * pp + 2.0 * (fa * fb * qc + fa * fc * qp + fb * fc * cp)
    kr_dr = fa * krq + fb * krc + fc * krp
    kdr_dr = fa * fa * kqq + fb * fb * kcc + fc * fc * kpp + 2.0 * (fa * fb * kqc + fa * fc * kqp + fb * fc * kcp)
    wt = r_dr / (dr_dr + eps)
    lm = wt * l0
    bmbm = cc + 2.0 * lm * cp + lm * lm * pp
    bm_rho = rc + lm * (qc + rp) + lm * lm * qp
    dm = (bm_rho - e0 * eps) / (bmbm + eps)
    em = e0 + dm
    mm = rr - 2.0 * wt * r_dr + wt * wt * dr_dr
    kmm = krr - 2.0 * wt * kr_dr + wt * wt * kdr_dr
    bm = c + lm * p0
    hm = h0 + lm * g0
    rm = r0 - wt * (fa * q0 + fb * c + fc * p0)
    sm = r0 + lm * q0 - dm * bm
    p1 = precondition(rm, kmm / (mm + eps))
    vecs[4] = bm
    vecs[5] = hm
    vecs[6] = rm
    vecs[7] = sm
    vecs[8] = p1
    bands[my_band] = jnp.concatenate([bm, p1], axis=0)

    apply_h(2, vecs[8])
    bm, hm, rm, sm, p1 = vecs[4], vecs[5], vecs[6], vecs[7], vecs[8]
    g1 = hvec[...]
    q1 = g1 - em * p1
    start_sums(2, as_row([fold(rm * q1), fold(q1 * q1)]))
    span = bands.at[pl.ds(0, band_n - 1)]
    pltpu.make_async_remote_copy(
        src_ref=span, dst_ref=span, send_sem=send_sem.at[19], recv_sem=recv_sem.at[19],
        device_id={"band": other_bands[0]}, device_id_type=MESH,
    ).wait()
    left = jnp.concatenate([bm, p1, hm, g1], axis=0)
    gram = dot_full(left, jnp.concatenate([bands[j] for j in range(band_n)], axis=0), NT)
    wide = (band_n * 4, 128)
    moved = iota(wide, 0) % 4 * band_n + iota(wide, 0) // 4
    gram = dot_full(gram, jnp.where(moved == iota(wide, 1), 1.0, 0.0))
    pairs = [(sm, sm), (sm, q1), (sm, bm), (sm, p1), (q1, bm), (q1, p1), (bm, bm), (bm, p1), (p1, p1)]
    row = as_row([fold(a * b) for a, b in pairs])
    gram_send[:8, :] = gram
    gram_send[8:, :] = jnp.broadcast_to(row, (8, 128))
    spread_rows(gram_send, gram_recv, 18)
    gram_recv[me] = gram_send[...]
    tot = end_sums(2)
    rq, qq = cell(tot, 0), cell(tot, 1)
    l1 = -rq / (qq + eps)
    lam_send[...] = jnp.broadcast_to(l1, (1, 128))
    spread_band(lam_send, lam_recv.at[my_band], 20)
    lam_recv[my_band] = lam_send[...]
    wait_rows(gram_recv, 18, ga_n - 1, "ga", ga_n, me)
    summed = jnp.sum(gram_recv[...], axis=0) * (1.0 / total_pw)
    gram, tot = summed[:8], summed[8:9]
    ss, sq, sb, sp, qb, qp, bb, bp, pp = [cell(tot, n) for n in range(9)]

    new = bm + l1 * p1
    nb_out[0] = new[0:1]
    nb_out[1] = new[1:2]
    nn = bb + 2.0 * l1 * bp + l1 * l1 * pp
    n_sig = sb + l1 * (sp + qb) + l1 * l1 * qp
    sig_sig = ss + 2.0 * l1 * sq + l1 * l1 * qq
    shift = (n_sig - em * eps) / (nn + eps)
    energy = em + shift
    res = (sig_sig - 2.0 * shift * n_sig + shift * shift * nn) / (nn + eps)

    wait_rows(lam_recv, 20, band_n - 1, "band", band_n, my_band)
    lams = jnp.zeros((1, 128), F32)
    for j in range(band_n):
        lams = jnp.where(lane == j, lam_recv[j], lams)

    def part(rows, v):
        return rows[:, v * band_n : (v + 1) * band_n]

    lam8 = lams[:, :band_n]

    def finish(rows):
        a = rows[0:2] + l1 * rows[2:4]
        against_re = part(a, 0) + lam8 * part(a, 2)
        against_im = part(a, 1) + lam8 * part(a, 3)
        return (against_re[0:1] + against_im[1:2], against_im[0:1] - against_re[1:2])

    cor_re, cor_im = finish(gram[0:4])
    sub_re, sub_im = finish(gram[4:8])
    tail = jnp.concatenate([jnp.broadcast_to(energy, (1, band_n)), jnp.broadcast_to(res, (1, band_n))], axis=0)
    block = jnp.concatenate([cor_re, cor_im, sub_re, sub_im, tail, tail], axis=0)
    small_out[...] = jnp.concatenate([block, jnp.zeros((8, 128 - band_n), F32)], axis=1)


def body(tables, coeffs, cell_map, potential, projectors, strengths, proj_atom, proj_chan):
    ga_n = lax.axis_size("ga")
    band_n = lax.axis_size("band")
    grid_len = potential.shape[0]
    pw = coeffs.shape[2]
    proj_n = proj_atom.shape[0]
    total_pw = pw * ga_n
    vmem = pl.BlockSpec(memory_space=pltpu.VMEM)
    hbm = pl.BlockSpec(memory_space=pltpu.HBM)
    z_tab, tabs = tables
    args = (cell_map.reshape(pw // 128, 128), z_tab, coeffs, tabs, projectors, jnp.transpose(potential, (1, 0, 2)),
            strengths, proj_atom.reshape(1, proj_n), proj_chan.reshape(1, proj_n))
    V = pltpu.VMEM
    scratch = [V(a.shape, a.dtype) for a in args] + [
        V((pw, 3 * 128), BF16), V((320, pw), BF16), V((2 * grid_len, pw), F32),
        V((2, 2 * grid_len, 256), BF16), V((2, grid_len, 128), BF16), V((2, grid_len, 256), F32),
        V((proj_n, 2 * proj_n), F32), V((9, 2, pw), F32), V((2, pw), F32), V((1, pw), F32),
        V((12, ga_n * 8, 128), F32), V((12, ga_n * 8, 128), F32),
        V((6, 1, 128), F32), V((6, ga_n, 1, 128), F32),
        V((16, 128), F32), V((ga_n, 16, 128), F32),
        V((band_n, 4, pw), F32), V((1, 128), F32), V((band_n, 1, 128), F32),
        pltpu.SemaphoreType.DMA((21,)), pltpu.SemaphoreType.DMA((21,)), pltpu.SemaphoreType.DMA((len(args),)),
    ]
    args = [pltpu.with_memory_space_constraint(a, pltpu.HBM) for a in args]
    new_bands, small = pl.pallas_call(
        functools.partial(kernel, (ga_n, band_n, grid_len, total_pw)),
        out_shape=(
            jax.ShapeDtypeStruct((2, 1, pw), F32),
            jax.ShapeDtypeStruct((8, 128), F32),
        ),
        in_specs=[hbm] * len(args),
        out_specs=(vmem, vmem),
        scratch_shapes=scratch,
        compiler_params=pltpu.CompilerParams(collective_id=0, has_side_effects=True, vmem_limit_bytes=24 * 2**20),
    )(*args)

    def deal(nb, sm, nb_o, en_o, re_o, co_o, su_o):
        nb_o[...] = nb[...]
        co_o[0], co_o[1] = sm[0:1, :band_n], sm[1:2, :band_n]
        su_o[0], su_o[1] = sm[2:3, :band_n], sm[3:4, :band_n]
        en_o[...] = sm[4:5, :1]
        re_o[...] = sm[5:6, :1]

    one = jax.ShapeDtypeStruct((1, 1), F32)
    rows = jax.ShapeDtypeStruct((2, 1, band_n), F32)
    new_bands, energy, res, corr, sub = pl.pallas_call(
        deal,
        out_shape=(jax.ShapeDtypeStruct((2, 1, pw), F32), one, one, rows, rows),
        in_specs=[vmem] * 2,
        out_specs=(vmem,) * 5,
        compiler_params=pltpu.CompilerParams(vmem_limit_bytes=2**20),
    )(new_bands, small)
    return new_bands, energy.reshape(1), res.reshape(1), corr, sub


def solution(mesh):
    tables = make_tables(96, mesh.shape["ga"])
    placed = (P(None, "band", "ga"), P("ga"), P(None, "ga", None), P(None, None, "ga"), P(), P(), P())
    return jax.shard_map(
        functools.partial(body, tables),
        mesh=mesh,
        in_specs=placed,
        out_specs=(P(None, "band", "ga"), P("band"), P("band"), P(None, "band", None), P(None, "band", None)),
        check_vma=False,
    )
```

```python
import functools

import jax
import jax.numpy as jnp
import numpy as np
from jax import lax
from jax.experimental import pallas as pl
from jax.experimental.pallas import tpu as pltpu
from jax.sharding import PartitionSpec as P

F32 = jnp.float32
BF16 = jnp.bfloat16
HIGHEST = lax.Precision.HIGHEST
MESH = pl.DeviceIdType.MESH
kin_unit = 0.02
small_eps = 1e-06

NN = (((1,), (0,)), ((), ()))
NT = (((1,), (1,)), ((), ()))
TN = (((0,), (0,)), ((), ()))


def parts_of(table, count):
    out = []
    left = np.asarray(table, np.float64)
    for _ in range(count):
        piece = left.astype(np.float32).astype(BF16)
        out.append(piece)
        left = left - piece.astype(np.float64)
    return out


def make_tables(grid_len, groups):
    planes = grid_len // groups
    natural = np.arange(grid_len)
    slab = (natural % groups) * planes + natural // groups

    def angles(rows, cols):
        return 2.0 * np.pi / grid_len * ((rows[:, None] * cols[None, :]) % grid_len)

    z_ang = angles(natural, natural)
    x_cos, x_sin = np.cos(z_ang), np.sin(z_ang)
    half = grid_len // 2
    z_high, z_low = parts_of(np.concatenate([x_cos[:half], x_sin[:half], x_cos[half:], x_sin[half:]], axis=0), 2)
    y_ang = angles(slab, natural)
    y_cos, y_sin = np.cos(y_ang), np.sin(y_ang)
    pad = np.zeros((grid_len, 128 - grid_len))
    side = np.zeros((2 * grid_len, 256 - 2 * grid_len))
    y_fwd = np.block([[y_cos, pad, -y_sin, pad], [y_sin, pad, y_cos, pad]])
    x_fwd = np.block([[x_cos, -x_sin], [x_sin, x_cos]])
    x_back = np.block([[x_cos, x_sin], [-x_sin, x_cos]]) / grid_len
    x_fwd, x_back = np.concatenate([x_fwd, side], axis=1), np.concatenate([x_back, side], axis=1)
    y_back = y_fwd / grid_len**2
    rest = []
    for tab in (y_fwd, x_fwd, x_back, y_back):
        rest.append(np.concatenate(parts_of(tab, 2), axis=0))
    return [np.concatenate([z_high, z_low], axis=1), np.stack(rest)]


def dot(a, b, dims=NN):
    return lax.dot_general(a, b, dims, preferred_element_type=F32)


def dot_full(a, b, dims=NN):
    return lax.dot_general(a, b, dims, precision=HIGHEST, preferred_element_type=F32)


def dot_tab(tab, hi, lo, dims=NN):
    rows = tab.shape[0] // 2
    both = dot(tab, hi, dims)
    return both[:rows] + both[rows:] + dot(tab[:rows], lo, dims)


def split(x):
    hi = x.astype(BF16)
    return hi, (x - hi.astype(F32)).astype(BF16)


def iota(shape, axis):
    return lax.broadcasted_iota(jnp.int32, shape, axis)


def hops(k):
    return min(k, 4 - k)


def far_first():
    steps = [(i, j) for i in range(4) for j in range(4) if (i, j) != (0, 0)]
    return [[s for s in steps if hops(s[0]) + hops(s[1]) == far] for far in (4, 3, 2, 1)]


def kernel(sizes, cm_far, zt_far, cf_far, tabs_far, pj_far, pot_far, st_far, pa_far, pc_far,
           nb_out, small_out,
           cm, zt, cf, tabs, pj, pot, st, pa, pc, at_s, at_g, e_tab, gt, gt_rest, v_tab, coup, vecs, hvec, kin_ref,
           send, recv, row_send, row_recv, gram_send, gram_recv, bands, lam_send, lam_recv,
           send_sem, recv_sem, load_sem):
    ga_n, band_n, grid_len, total_pw = sizes
    planes = grid_len // ga_n
    me = lax.axis_index("ga")
    my_band = lax.axis_index("band")
    pw = cf.shape[2]
    tiles = pw // 128
    far = (cm_far, zt_far, cf_far, tabs_far, pj_far, pot_far, st_far, pa_far, pc_far)
    near = (cm, zt, cf, tabs, pj, pot, st, pa, pc)
    loads = [pltpu.make_async_copy(a, b, load_sem.at[n]) for n, (a, b) in enumerate(zip(far, near))]
    loads[0].start()
    loads[1].start()

    barrier = pltpu.get_barrier_semaphore()
    m_x, m_y, m_c = me // 8, me // 2 % 4, me % 2

    others = []
    for group in far_first():
        for core in (0, 1):
            others += [((m_x + i) % 4) * 8 + ((m_y + j) % 4) * 2 + core for i, j in group]
    others.append(m_x * 8 + m_y * 2 + 1 - m_c)
    band_order = sorted(range(1, band_n), key=lambda k: -min(k, band_n - k))
    other_bands = [lax.rem(my_band + k, band_n) for k in band_order]

    for other in others:
        pl.semaphore_signal(barrier, inc=1, device_id={"ga": other}, device_id_type=MESH)
    for other in other_bands:
        pl.semaphore_signal(barrier, inc=1, device_id={"band": other}, device_id_type=MESH)

    for load in loads[2:]:
        load.start()
    zeros = jnp.zeros((ga_n, 128), F32)
    for lot in range(12):
        send[lot, pl.ds(7, ga_n, stride=8), :] = zeros
    loads[0].wait()
    loads[1].wait()

    cells = cm[...]
    py = lax.shift_right_logical(cells * 43691, 22)
    z_idx = cells - py * grid_len
    plane = (py >= grid_len).astype(jnp.int32) + (py >= 2 * grid_len).astype(jnp.int32)
    y_idx = py - plane * grid_len
    x_idx = me + ga_n * plane
    py_pad = plane * 128 + y_idx

    def freq(k):
        return jnp.where(2 * k < grid_len, k, k - grid_len).astype(F32)

    kin = kin_unit * (freq(x_idx) * freq(x_idx) + freq(y_idx) * freq(y_idx) + freq(z_idx) * freq(z_idx))
    for k in range(tiles):
        lanes = slice(k * 128, k * 128 + 128)
        kin_ref[:, lanes] = kin[k : k + 1]
    for k in range(0, tiles, 2):
        row = jnp.concatenate([z_idx[k : k + 1], z_idx[k + 1 : k + 2]], axis=1)
        hot = jnp.where(iota((grid_len, 256), 0) == row, 1.0, 0.0).astype(BF16)
        e_tab[:, k * 128 : k * 128 + 256] = dot(zt[...], jnp.concatenate([hot, hot], axis=0))
    upright = jnp.transpose(jnp.concatenate([py_pad, jnp.zeros((128 - tiles, 128), jnp.int32)], axis=0))
    for k in range(tiles):
        hot = (iota((128, 3 * 128), 1) == upright[:, k : k + 1])
        at_s[k * 128 : k * 128 + 128, :] = jnp.where(hot, 1.0, 0.0).astype(BF16)
    half_len = grid_len // 2

    def later_tables():
        for load in loads[5:]:
            load.wait()
        blank = jnp.zeros((grid_len, 128 - grid_len), F32)
        at = iota((grid_len, 128), 1)
        slabs = [jnp.concatenate([pot[j], blank], axis=1) for j in range(planes)]
        for h in range(2):
            first, second, third = [moved_by(slabs[j], 48 * j - 48 * h) for j in range(planes)]
            v_tab[h, :, :128] = jnp.where(at < 48, first, jnp.where(at < 96, second, third))
            v_tab[h, :, 128:] = jnp.where(at < 16, moved_by(slabs[2], -48 * h - 32), 0.0)
        place = jnp.where(plane == 2, jnp.where(y_idx < 32, 96 + y_idx, 192 + y_idx), plane * 128 + y_idx)
        for k in range(tiles):
            lanes = slice(k * 128, k * 128 + 128)
            hot = jnp.where(iota((288, 128), 0) == place[k : k + 1], 1.0, 0.0).astype(BF16)
            at_g[:288, lanes] = hot
            at_g[288:, lanes] = hot[256:]
        chans = st.shape[1]
        sym_rows = st[...].reshape(st.shape[0] * chans, chans)
        slot = pa[...] * chans + pc[...]
        hot_p = jnp.where(iota((proj_n, proj_n), 0) == slot, 1.0, 0.0)
        hot_c = jnp.where(iota((chans, proj_n), 0) == pc[...], 1.0, 0.0)
        reach = dot_full(sym_rows, hot_c)
        reach = jnp.where(iota((proj_n, proj_n), 0) // chans == pa[...], reach, 0.0)
        half = 0.5 * (dot_full(hot_p, reach, TN) + dot_full(reach, hot_p, TN))
        coup[...] = jnp.concatenate([half, half], axis=1)

    proj_n = pa.shape[1]
    lane = iota((1, 128), 1)
    lane32 = iota((ga_n, 128), 1)

    def roll(x, by):
        return pltpu.roll(x, by, 1)

    lane16 = lane32 // 16

    def gather_rest(pieces):
        rest = pieces[0]
        for n in range(1, 6):
            rest = jnp.where(lane16 == n, roll(pieces[n], 16 * n), rest)
        return rest

    def moved_by(x, by):
        return x if by % 128 == 0 else roll(x, by % 128)

    def put(lot, row, value):
        send[lot, pl.ds(row, ga_n, stride=8), :] = value

    def exchange(lot):
        rows = 8 if lot in (2, 3) else 7
        mine = pl.ds(pl.multiple_of(me * 8, 8), rows)
        for other in others:
            pltpu.make_async_remote_copy(
                src_ref=send.at[lot, pl.ds(pl.multiple_of(other * 8, 8), rows), :],
                dst_ref=recv.at[lot, mine, :],
                send_sem=send_sem.at[lot],
                recv_sem=recv_sem.at[lot],
                device_id={"ga": other},
                device_id_type=MESH,
            ).start()
        recv[lot, mine, :] = send[lot, mine, :]

    def wait_exchange(lot):
        span = pl.ds(0, (ga_n - 1) * (8 if lot in (2, 3) else 7))
        pltpu.make_async_remote_copy(
            src_ref=send.at[lot, span, :],
            dst_ref=recv.at[lot, span, :],
            send_sem=send_sem.at[lot],
            recv_sem=recv_sem.at[lot],
            device_id={"ga": others[0]},
            device_id_type=MESH,
        ).wait()

    def got_rows(lot, row):
        return recv[lot, pl.ds(row, ga_n, stride=8), :]

    def spread_rows(ref_send, ref_recv, sem):
        for other in others:
            pltpu.make_async_remote_copy(
                src_ref=ref_send, dst_ref=ref_recv.at[me], send_sem=send_sem.at[sem], recv_sem=recv_sem.at[sem],
                device_id={"ga": other}, device_id_type=MESH,
            ).start()

    def spread_band(ref_send, ref_recv, sem):
        for other in other_bands:
            pltpu.make_async_remote_copy(
                src_ref=ref_send, dst_ref=ref_recv, send_sem=send_sem.at[sem], recv_sem=recv_sem.at[sem],
                device_id={"band": other}, device_id_type=MESH,
            ).start()

    def wait_rows(ref_recv, sem, count, axis, size, mine):
        span = ref_recv.at[pl.ds(0, count)]
        pltpu.make_async_remote_copy(
            src_ref=span, dst_ref=span, send_sem=send_sem.at[sem], recv_sem=recv_sem.at[sem],
            device_id={axis: lax.rem(mine + 1, size)}, device_id_type=MESH,
        ).wait()

    def cell(row, at):
        return jnp.sum(jnp.where(lane == at, row, 0.0), axis=1, keepdims=True)

    def fold(x):
        total = x[:, :128]
        for k in range(1, tiles):
            total = total + x[:, k * 128 : k * 128 + 128]
        return total[0:1] + total[1:2]

    def as_row(folded):
        stack = jnp.concatenate(folded + [jnp.zeros((1, 128), F32)] * (-len(folded) % 8), axis=0)
        col = jnp.sum(stack, axis=1, keepdims=True)
        hit = iota(stack.shape, 0) == iota(stack.shape, 1)
        return jnp.sum(jnp.where(hit, col, 0.0), axis=0, keepdims=True)

    def start_sums(which, row):
        row_send[which] = row
        spread_rows(row_send.at[which], row_recv.at[which], 12 + which)
        row_recv[which, me] = row_send[which]

    def end_sums(which):
        wait_rows(row_recv.at[which], 12 + which, ga_n - 1, "ga", ga_n, me)
        return jnp.sum(row_recv[which], axis=0) * (1.0 / total_pw)

    def all_sums(which, folded):
        start_sums(which, as_row(folded))
        total = end_sums(which)
        return total

    def apply_h(turn, v):
        base = (0, 48, 0)

        def onto_grid(h, start, stop, t_all=None):
            for k in range(start, stop, 256):
                lanes = slice(k, k + 256)
                e_c = e_tab[h * grid_len : h * grid_len + half_len, lanes]
                e_s = e_tab[h * grid_len + half_len : (h + 1) * grid_len, lanes]
                v_re, v_im = v[0:1, lanes], v[1:2, lanes]
                hi_re, lo_re = split(e_c * v_re - e_s * v_im)
                hi_im, lo_im = split(e_s * v_re + e_c * v_im)
                got = dot(jnp.concatenate([hi_re, hi_im, lo_re, lo_im], axis=0), at_s[lanes, :])
                t_all = got if t_all is None else t_all + got
            return t_all

        def along_y(h, t_all):
            if turn == 0 and h == 0:
                loads[3].wait()
            t_all = t_all[:grid_len] + t_all[grid_len:]
            rows = []
            for i in range(planes):
                lanes = slice(i * 128, i * 128 + 128)
                rows.append(jnp.concatenate([t_all[:half_len, lanes], t_all[half_len:, lanes]], axis=1))
            rows.insert(2, jnp.zeros((32, 256), F32))
            hi, lo = split(jnp.concatenate(rows, axis=0))
            u = dot_tab(tabs[0], hi, lo, NT)
            u = (u[:, :128], u[:, 128:])
            rest = []
            for c in range(2):
                for i in range(planes):
                    spread = []
                    for j in range(planes):
                        at = c * grid_len + j * ga_n
                        piece = u[i // 2][at : at + ga_n]
                        if i == 2:
                            piece = jnp.concatenate([piece, jnp.zeros((ga_n, 128 - half_len), F32)], axis=1)
                        spread.append(moved_by(piece, 48 * j - base[i]))
                    put(4 * turn + h, c * planes + i,
                        jnp.where(lane32 < 48, spread[0], jnp.where(lane32 < 96, spread[1], spread[2])))
                    rest.append(spread[2])
            put(4 * turn + h, 6, gather_rest(rest))

        early = 0 * 256
        first = onto_grid(0, 0, pw)
        second = onto_grid(1, 0, early)
        along_y(0, first)
        if turn == 0:
            pl.semaphore_wait(barrier, ga_n - 1 + band_n - 1)
        exchange(4 * turn)
        second = onto_grid(1, early, pw, second)
        along_y(1, second)
        exchange(4 * turn + 1)

        if turn == 0:
            loads[4].wait()
        acc_re = jnp.zeros((proj_n, 128), F32)
        acc_im = jnp.zeros((proj_n, 128), F32)
        for k in range(tiles):
            lanes = slice(k * 128, k * 128 + 128)
            p_re, p_im = pj[0, :, lanes], pj[1, :, lanes]
            v_re, v_im = v[0:1, lanes], v[1:2, lanes]
            acc_re = acc_re + (p_re * v_re + p_im * v_im)
            acc_im = acc_im + (p_re * v_im - p_im * v_re)
        col_re = jnp.sum(acc_re, axis=1, keepdims=True)
        col_im = jnp.sum(acc_im, axis=1, keepdims=True)
        row64, lane64 = iota((proj_n, 128), 0), iota((proj_n, 128), 1)
        diag = jnp.where(lane64 == row64, col_re, jnp.where(lane64 == row64 + proj_n, col_im, 0.0))
        start_sums(3 + turn, jnp.sum(diag, axis=0, keepdims=True))
        norm_row = None
        if turn == 0:
            norm_row = as_row([fold(v * v), fold(v * v * kin_ref[...])])
            later_tables()
        if turn == 2:
            spread_band(bands.at[my_band], bands.at[my_band], 19)
        for h in range(2):
            lot = 4 * turn + h
            wait_exchange(lot)
            rest = got_rows(lot, 6)
            main = jnp.concatenate([got_rows(lot, n) for n in range(6)], axis=0)
            side = jnp.concatenate([moved_by(rest, -16 * n) for n in range(6)], axis=0)
            hi, lo = split(jnp.concatenate([main, side], axis=1))
            w = dot_tab(tabs[1, :, : 2 * grid_len], hi, lo)
            w_re, w_im = w[:grid_len], w[grid_len:]
            vw_re, vw_im = v_tab[h] * w_re, v_tab[h] * w_im
            lot = 4 * turn + 2 + h
            if turn == 0:
                dens = jnp.sum(vw_re * w_re + vw_im * w_im, axis=0, keepdims=True)
                dens = jnp.sum(dens[:, :128] + dens[:, 128:], axis=1, keepdims=True)
                row = norm_row if h == 0 else jnp.zeros((1, 128), F32)
                put(lot, 7, jnp.broadcast_to(jnp.where(lane == 2, dens, row), (ga_n, 128)))
            hi, lo = split(jnp.concatenate([vw_re, vw_im], axis=0))
            back = dot_tab(tabs[2, :, : 2 * grid_len], hi, lo)
            for n in range(6):
                put(lot, n, back[n * ga_n : (n + 1) * ga_n, :128])
            put(lot, 6, gather_rest([back[n * ga_n : (n + 1) * ga_n, 128:] for n in range(6)]))
            exchange(lot)

        tot = end_sums(3 + turn)
        prod = coup[...] * tot
        mix_re = jnp.sum(jnp.where(lane64 < proj_n, prod, 0.0), axis=1, keepdims=True)
        mix_im = jnp.sum(jnp.where(lane64 < proj_n, 0.0, prod), axis=1, keepdims=True)
        c_n = None
        if turn == 0:
            diag_row = jnp.where(lane64 == row64, mix_re, jnp.where(lane64 == row64 + proj_n, mix_im, 0.0))
            c_n = jnp.sum(jnp.sum(diag_row, axis=0, keepdims=True) * tot, axis=1, keepdims=True)
        for k in range(tiles):
            lanes = slice(k * 128, k * 128 + 128)
            p_re, p_im = pj[0, :, lanes], pj[1, :, lanes]
            n_re = jnp.sum(p_re * mix_re - p_im * mix_im, axis=0, keepdims=True)
            n_im = jnp.sum(p_im * mix_re + p_re * mix_im, axis=0, keepdims=True)
            hvec[:, lanes] = jnp.concatenate([n_re, n_im], axis=0) + kin_ref[:, lanes] * v[:, lanes]
        for h in range(2):
            lot = 4 * turn + 2 + h
            wait_exchange(lot)
            rest = got_rows(lot, 6)
            left, right = [], []
            for c in range(2):
                mains = [got_rows(lot, c * planes + i) for i in range(planes)]
                for j in range(planes):
                    pieces = []
                    for i in range(planes):
                        piece = moved_by(mains[i], base[i] - 48 * j)
                        if j == 2:
                            late = moved_by(rest, base[i] + 32 - 16 * (c * planes + i))
                            piece = jnp.where(lane32 < base[i] + 32, piece, late)
                        pieces.append(piece)
                    left.append(jnp.where(lane32 < 48, pieces[0], pieces[1]))
                    right.append(pieces[2])
            left, right = jnp.concatenate(left, axis=0).T, jnp.concatenate(right, axis=0).T
            hi, lo = split(jnp.concatenate([left[:grid_len], right[:half_len]], axis=0))
            rows = hi.shape[0]
            out = dot(jnp.concatenate([hi, lo], axis=0), tabs[3, : 2 * grid_len])
            out = out[:rows] + out[rows:] + dot(hi, tabs[3, 2 * grid_len :])
            for c in range(2):
                first, second, third = [out[i * half_len : (i + 1) * half_len, c * 128 : c * 128 + 128] for i in range(planes)]
                late = roll(third, 64)
                rows = slice(c * half_len, (c + 1) * half_len)
                rows_lo = slice((2 + c) * half_len, (3 + c) * half_len)
                wide = lane < 96
                hi, lo = split(jnp.concatenate([jnp.where(wide, first, roll(third, 96)), jnp.where(wide, second, late)], axis=1))
                gt[h, rows, :] = hi
                gt[h, rows_lo, :] = lo
                high = late.astype(BF16).astype(F32)
                gt_rest[h, rows, :] = jnp.where(lane < 32, high, roll(late - high, 32)).astype(BF16)
            for k in range(0, pw, 256):
                lanes = slice(k, k + 256)
                q = dot(gt[h], at_g[:256, lanes])
                q = q[:grid_len] + q[grid_len:] + dot(gt_rest[h, :, :64], at_g[256:, lanes])
                q_re, q_im = q[:half_len], q[half_len:]
                e_c = e_tab[h * grid_len : h * grid_len + half_len, lanes]
                e_s = e_tab[h * grid_len + half_len : (h + 1) * grid_len, lanes]
                l_re = jnp.sum(e_c * q_re + e_s * q_im, axis=0, keepdims=True)
                l_im = jnp.sum(e_c * q_im - e_s * q_re, axis=0, keepdims=True)
                hvec[:, lanes] = hvec[:, lanes] + jnp.concatenate([l_re, l_im], axis=0)
        return c_n

    def precondition(r, level):
        ratio = kin_ref[...] / (1.5 * level + 1.0)
        numer = 27.0 + ratio * (18.0 + ratio * (12.0 + 8.0 * ratio))
        square = ratio * ratio
        return r * (numer / (numer + 16.0 * square * square))

    eps = small_eps

    loads[2].wait()
    vecs[0] = jnp.concatenate([cf[0], cf[1]], axis=0)
    c_n = apply_h(0, vecs[0])
    tot = jnp.sum(got_rows(2, 7) + got_rows(3, 7), axis=0, keepdims=True) * (1.0 / total_pw)
    guess_cc = cell(tot, 0)
    guess = (cell(tot, 1) + cell(tot, 2) * (1.0 / grid_len**3) + c_n) / (guess_cc + eps)
    c = vecs[0]
    h0 = hvec[...]
    s = h0 - guess * c
    kc, ks = kin_ref[...] * c, kin_ref[...] * s
    tot = all_sums(0, [fold(c * c), fold(c * s), fold(s * s), fold(kc * c), fold(kc * s), fold(ks * s)])
    cc, cs, ss, kcc, kcs, kss = [cell(tot, n) for n in range(6)]
    shift = (cs - guess * eps) / (cc + eps)
    e0 = guess + shift
    r0 = s - shift * c
    rr = ss - 2.0 * shift * cs + shift * shift * cc
    krr = kss - 2.0 * shift * kcs + shift * shift * kcc
    rc = cs - shift * cc
    krc = kcs - shift * kcc
    p0 = precondition(r0, krr / (rr + eps))
    vecs[1] = r0
    vecs[2] = p0
    vecs[3] = h0

    apply_h(1, vecs[2])
    c, r0, p0, h0 = vecs[0], vecs[1], vecs[2], vecs[3]
    g0 = hvec[...]
    q0 = g0 - e0 * p0
    pairs = [(r0, q0), (r0, p0), (q0, q0), (q0, c), (q0, p0), (c, p0), (p0, p0)]
    prods = [a * b for a, b in pairs]
    tot = all_sums(1, [fold(x) for x in prods] + [fold(x * kin_ref[...]) for x in prods])
    rq, rp, qq, qc, qp, cp, pp = [cell(tot, n) for n in range(7)]
    krq, krp, kqq, kqc, kqp, kcp, kpp = [cell(tot, n) for n in range(7, 14)]
    l0 = -rq / (qq + eps)
    bb = cc + 2.0 * l0 * cp + l0 * l0 * pp
    b_rho = rc + l0 * (qc + rp) + l0 * l0 * qp
    d1 = (b_rho - e0 * eps) / (bb + eps)
    fa, fb, fc = -l0, d1, d1 * l0
    r_dr = fa * rq + fb * rc + fc * rp
    dr_dr = fa * fa * qq + fb * fb * cc + fc * fc * pp + 2.0 * (fa * fb * qc + fa * fc * qp + fb * fc * cp)
    kr_dr = fa * krq + fb * krc + fc * krp
    kdr_dr = fa * fa * kqq + fb * fb * kcc + fc * fc * kpp + 2.0 * (fa * fb * kqc + fa * fc * kqp + fb * fc * kcp)
    wt = r_dr / (dr_dr + eps)
    lm = wt * l0
    bmbm = cc + 2.0 * lm * cp + lm * lm * pp
    bm_rho = rc + lm * (qc + rp) + lm * lm * qp
    dm = (bm_rho - e0 * eps) / (bmbm + eps)
    em = e0 + dm
    mm = rr - 2.0 * wt * r_dr + wt * wt * dr_dr
    kmm = krr - 2.0 * wt * kr_dr + wt * wt * kdr_dr
    bm = c + lm * p0
    hm = h0 + lm * g0
    rm = r0 - wt * (fa * q0 + fb * c + fc * p0)
    sm = r0 + lm * q0 - dm * bm
    p1 = precondition(rm, kmm / (mm + eps))
    vecs[4] = bm
    vecs[5] = hm
    vecs[6] = rm
    vecs[7] = sm
    vecs[8] = p1
    bands[my_band] = jnp.concatenate([bm, p1], axis=0)

    apply_h(2, vecs[8])
    bm, hm, rm, sm, p1 = vecs[4], vecs[5], vecs[6], vecs[7], vecs[8]
    g1 = hvec[...]
    q1 = g1 - em * p1
    start_sums(2, as_row([fold(rm * q1), fold(q1 * q1)]))
    span = bands.at[pl.ds(0, band_n - 1)]
    pltpu.make_async_remote_copy(
        src_ref=span, dst_ref=span, send_sem=send_sem.at[19], recv_sem=recv_sem.at[19],
        device_id={"band": other_bands[0]}, device_id_type=MESH,
    ).wait()
    left = jnp.concatenate([bm, p1, hm, g1], axis=0)
    gram = dot_full(left, jnp.concatenate([bands[j] for j in range(band_n)], axis=0), NT)
    wide = (band_n * 4, 128)
    moved = iota(wide, 0) % 4 * band_n + iota(wide, 0) // 4
    gram = dot_full(gram, jnp.where(moved == iota(wide, 1), 1.0, 0.0))
    pairs = [(sm, sm), (sm, q1), (sm, bm), (sm, p1), (q1, bm), (q1, p1), (bm, bm), (bm, p1), (p1, p1)]
    row = as_row([fold(a * b) for a, b in pairs])
    gram_send[:8, :] = gram
    gram_send[8:9, :] = row
    spread_rows(gram_send, gram_recv, 18)
    gram_recv[me] = gram_send[...]
    tot = end_sums(2)
    rq, qq = cell(tot, 0), cell(tot, 1)
    l1 = -rq / (qq + eps)
    lam_send[...] = jnp.broadcast_to(l1, (1, 128))
    spread_band(lam_send, lam_recv.at[my_band], 20)
    lam_recv[my_band] = lam_send[...]
    wait_rows(gram_recv, 18, ga_n - 1, "ga", ga_n, me)
    summed = jnp.sum(gram_recv[...], axis=0) * (1.0 / total_pw)
    gram, tot = summed[:8], summed[8:9]
    ss, sq, sb, sp, qb, qp, bb, bp, pp = [cell(tot, n) for n in range(9)]

    new = bm + l1 * p1
    nb_out[0] = new[0:1]
    nb_out[1] = new[1:2]
    nn = bb + 2.0 * l1 * bp + l1 * l1 * pp
    n_sig = sb + l1 * (sp + qb) + l1 * l1 * qp
    sig_sig = ss + 2.0 * l1 * sq + l1 * l1 * qq
    shift = (n_sig - em * eps) / (nn + eps)
    energy = em + shift
    res = (sig_sig - 2.0 * shift * n_sig + shift * shift * nn) / (nn + eps)

    wait_rows(lam_recv, 20, band_n - 1, "band", band_n, my_band)
    lams = jnp.zeros((1, 128), F32)
    for j in range(band_n):
        lams = jnp.where(lane == j, lam_recv[j], lams)

    def part(rows, v):
        return rows[:, v * band_n : (v + 1) * band_n]

    lam8 = lams[:, :band_n]

    def finish(rows):
        a = rows[0:2] + l1 * rows[2:4]
        against_re = part(a, 0) + lam8 * part(a, 2)
        against_im = part(a, 1) + lam8 * part(a, 3)
        return (against_re[0:1] + against_im[1:2], against_im[0:1] - against_re[1:2])

    cor_re, cor_im = finish(gram[0:4])
    sub_re, sub_im = finish(gram[4:8])
    tail = jnp.concatenate([jnp.broadcast_to(energy, (1, band_n)), jnp.broadcast_to(res, (1, band_n))], axis=0)
    block = jnp.concatenate([cor_re, cor_im, sub_re, sub_im, tail, tail], axis=0)
    small_out[...] = jnp.concatenate([block, jnp.zeros((8, 128 - band_n), F32)], axis=1)


def body(tables, coeffs, cell_map, potential, projectors, strengths, proj_atom, proj_chan):
    ga_n = lax.axis_size("ga")
    band_n = lax.axis_size("band")
    grid_len = potential.shape[0]
    pw = coeffs.shape[2]
    proj_n = proj_atom.shape[0]
    total_pw = pw * ga_n
    vmem = pl.BlockSpec(memory_space=pltpu.VMEM)
    hbm = pl.BlockSpec(memory_space=pltpu.HBM)
    z_tab, tabs = tables
    args = (cell_map.reshape(pw // 128, 128), z_tab, coeffs, tabs, projectors, jnp.transpose(potential, (1, 0, 2)),
            strengths, proj_atom.reshape(1, proj_n), proj_chan.reshape(1, proj_n))
    V = pltpu.VMEM
    scratch = [V(a.shape, a.dtype) for a in args] + [
        V((pw, 3 * 128), BF16), V((320, pw), BF16), V((2 * grid_len, pw), F32),
        V((2, 2 * grid_len, 256), BF16), V((2, grid_len, 128), BF16), V((2, grid_len, 256), F32),
        V((proj_n, 2 * proj_n), F32), V((9, 2, pw), F32), V((2, pw), F32), V((1, pw), F32),
        V((12, ga_n * 8, 128), F32), V((12, ga_n * 8, 128), F32),
        V((6, 1, 128), F32), V((6, ga_n, 1, 128), F32),
        V((9, 128), F32), V((ga_n, 9, 128), F32),
        V((band_n, 4, pw), F32), V((1, 128), F32), V((band_n, 1, 128), F32),
        pltpu.SemaphoreType.DMA((21,)), pltpu.SemaphoreType.DMA((21,)), pltpu.SemaphoreType.DMA((len(args),)),
    ]
    args = [pltpu.with_memory_space_constraint(a, pltpu.HBM) for a in args]
    new_bands, small = pl.pallas_call(
        functools.partial(kernel, (ga_n, band_n, grid_len, total_pw)),
        out_shape=(
            jax.ShapeDtypeStruct((2, 1, pw), F32),
            jax.ShapeDtypeStruct((8, 128), F32),
        ),
        in_specs=[hbm] * len(args),
        out_specs=(vmem, vmem),
        scratch_shapes=scratch,
        compiler_params=pltpu.CompilerParams(collective_id=0, has_side_effects=True, vmem_limit_bytes=24 * 2**20),
    )(*args)

    def deal(nb, sm, nb_o, en_o, re_o, co_o, su_o):
        nb_o[...] = nb[...]
        co_o[0], co_o[1] = sm[0:1, :band_n], sm[1:2, :band_n]
        su_o[0], su_o[1] = sm[2:3, :band_n], sm[3:4, :band_n]
        en_o[...] = sm[4:5, :1]
        re_o[...] = sm[5:6, :1]

    one = jax.ShapeDtypeStruct((1, 1), F32)
    rows = jax.ShapeDtypeStruct((2, 1, band_n), F32)
    new_bands, energy, res, corr, sub = pl.pallas_call(
        deal,
        out_shape=(jax.ShapeDtypeStruct((2, 1, pw), F32), one, one, rows, rows),
        in_specs=[vmem] * 2,
        out_specs=(vmem,) * 5,
        compiler_params=pltpu.CompilerParams(vmem_limit_bytes=2**20),
    )(new_bands, small)
    return new_bands, energy.reshape(1), res.reshape(1), corr, sub


def solution(mesh):
    tables = make_tables(96, mesh.shape["ga"])
    placed = (P(None, "band", "ga"), P("ga"), P(None, "ga", None), P(None, None, "ga"), P(), P(), P())
    return jax.shard_map(
        functools.partial(body, tables),
        mesh=mesh,
        in_specs=placed,
        out_specs=(P(None, "band", "ga"), P("band"), P("band"), P(None, "band", None), P(None, "band", None)),
        check_vma=False,
    )
```

```python
import functools

import jax
import jax.numpy as jnp
import numpy as np
from jax import lax
from jax.experimental import pallas as pl
from jax.experimental.pallas import tpu as pltpu
from jax.sharding import PartitionSpec as P

F32 = jnp.float32
BF16 = jnp.bfloat16
HIGHEST = lax.Precision.HIGHEST
MESH = pl.DeviceIdType.MESH
kin_unit = 0.02
small_eps = 1e-06

NN = (((1,), (0,)), ((), ()))
NT = (((1,), (1,)), ((), ()))
TN = (((0,), (0,)), ((), ()))


def parts_of(table, count):
    out = []
    left = np.asarray(table, np.float64)
    for _ in range(count):
        piece = left.astype(np.float32).astype(BF16)
        out.append(piece)
        left = left - piece.astype(np.float64)
    return out


def make_tables(grid_len, groups):
    planes = grid_len // groups
    natural = np.arange(grid_len)
    slab = (natural % groups) * planes + natural // groups

    def angles(rows, cols):
        return 2.0 * np.pi / grid_len * ((rows[:, None] * cols[None, :]) % grid_len)

    z_ang = angles(natural, natural)
    x_cos, x_sin = np.cos(z_ang), np.sin(z_ang)
    half = 2 * grid_len // 3
    z_high, z_low = parts_of(np.concatenate([x_cos[:half], x_sin[:half], x_cos[half:], x_sin[half:]], axis=0), 2)
    y_ang = angles(slab, natural)
    y_cos, y_sin = np.cos(y_ang), np.sin(y_ang)
    pad = np.zeros((grid_len, 128 - grid_len))
    side = np.zeros((2 * grid_len, 256 - 2 * grid_len))
    y_fwd = np.block([[y_cos, pad, -y_sin, pad], [y_sin, pad, y_cos, pad]])
    x_fwd = np.block([[x_cos, -x_sin], [x_sin, x_cos]])
    x_back = np.block([[x_cos, x_sin], [-x_sin, x_cos]]) / grid_len
    x_fwd, x_back = np.concatenate([x_fwd, side], axis=1), np.concatenate([x_back, side], axis=1)
    y_back = y_fwd / grid_len**2
    rest = []
    for tab in (y_fwd, x_fwd, x_back, y_back):
        rest.append(np.concatenate(parts_of(tab, 2), axis=0))
    return [np.concatenate([z_high, z_low], axis=1), np.stack(rest)]


def dot(a, b, dims=NN):
    return lax.dot_general(a, b, dims, preferred_element_type=F32)


def dot_full(a, b, dims=NN):
    return lax.dot_general(a, b, dims, precision=HIGHEST, preferred_element_type=F32)


def dot_tab(tab, hi, lo, dims=NN):
    rows = tab.shape[0] // 2
    both = dot(tab, hi, dims)
    return both[:rows] + both[rows:] + dot(tab[:rows], lo, dims)


def split(x):
    hi = x.astype(BF16)
    return hi, (x - hi.astype(F32)).astype(BF16)


def iota(shape, axis):
    return lax.broadcasted_iota(jnp.int32, shape, axis)


def hops(k):
    return min(k, 4 - k)


def far_first():
    steps = [(i, j) for i in range(4) for j in range(4) if (i, j) != (0, 0)]
    return [[s for s in steps if hops(s[0]) + hops(s[1]) == far] for far in (4, 3, 2, 1)]


def kernel(sizes, cm_far, zt_far, cf_far, tabs_far, pj_far, pot_far, st_far, pa_far, pc_far,
           nb_out, small_out,
           cm, zt, cf, tabs, pj, pot, st, pa, pc, at_s, at_g, e_tab, gt_big, gt_small, rest_big, rest_small, v_big, v_small, coup, vecs, hvec, kin_ref,
           send_big, recv_big, send_small, recv_small, row_send, row_recv, gram_send, gram_recv, bands, lam_send, lam_recv,
           send_sem, recv_sem, load_sem):
    ga_n, band_n, grid_len, total_pw = sizes
    planes = grid_len // ga_n
    me = lax.axis_index("ga")
    my_band = lax.axis_index("band")
    pw = cf.shape[2]
    tiles = pw // 128
    far = (cm_far, zt_far, cf_far, tabs_far, pj_far, pot_far, st_far, pa_far, pc_far)
    near = (cm, zt, cf, tabs, pj, pot, st, pa, pc)
    loads = [pltpu.make_async_copy(a, b, load_sem.at[n]) for n, (a, b) in enumerate(zip(far, near))]
    loads[0].start()
    loads[1].start()

    barrier = pltpu.get_barrier_semaphore()
    m_x, m_y, m_c = me // 8, me // 2 % 4, me % 2

    others = []
    for group in far_first():
        for core in (0, 1):
            others += [((m_x + i) % 4) * 8 + ((m_y + j) % 4) * 2 + core for i, j in group]
    others.append(m_x * 8 + m_y * 2 + 1 - m_c)
    band_order = sorted(range(1, band_n), key=lambda k: -min(k, band_n - k))
    other_bands = [lax.rem(my_band + k, band_n) for k in band_order]

    for other in others:
        pl.semaphore_signal(barrier, inc=1, device_id={"ga": other}, device_id_type=MESH)
    for other in other_bands:
        pl.semaphore_signal(barrier, inc=1, device_id={"band": other}, device_id_type=MESH)

    for load in loads[2:]:
        load.start()
    loads[0].wait()
    loads[1].wait()

    cells = cm[...]
    py = lax.shift_right_logical(cells * 43691, 22)
    z_idx = cells - py * grid_len
    plane = (py >= grid_len).astype(jnp.int32) + (py >= 2 * grid_len).astype(jnp.int32)
    y_idx = py - plane * grid_len
    x_idx = me + ga_n * plane
    py_pad = plane * 128 + y_idx

    def freq(k):
        return jnp.where(2 * k < grid_len, k, k - grid_len).astype(F32)

    kin = kin_unit * (freq(x_idx) * freq(x_idx) + freq(y_idx) * freq(y_idx) + freq(z_idx) * freq(z_idx))
    for k in range(tiles):
        lanes = slice(k * 128, k * 128 + 128)
        kin_ref[:, lanes] = kin[k : k + 1]
    for k in range(0, tiles, 2):
        row = jnp.concatenate([z_idx[k : k + 1], z_idx[k + 1 : k + 2]], axis=1)
        hot = jnp.where(iota((grid_len, 256), 0) == row, 1.0, 0.0).astype(BF16)
        e_tab[:, k * 128 : k * 128 + 256] = dot(zt[...], jnp.concatenate([hot, hot], axis=0))
    upright = jnp.transpose(jnp.concatenate([py_pad, jnp.zeros((128 - tiles, 128), jnp.int32)], axis=0))
    for k in range(tiles):
        hot = (iota((128, 3 * 128), 1) == upright[:, k : k + 1])
        at_s[k * 128 : k * 128 + 128, :] = jnp.where(hot, 1.0, 0.0).astype(BF16)
    share, share_at = (64, 32), (0, 128)

    def later_tables():
        for load in loads[5:]:
            load.wait()
        blank = jnp.zeros((grid_len, 128 - grid_len), F32)
        at = iota((grid_len, 128), 1)
        slabs = [jnp.concatenate([pot[j], blank], axis=1) for j in range(planes)]
        first, second, third = slabs
        v_big[:, :128] = jnp.where(at < 64, first, roll(second, 64))
        v_big[:, 128:] = jnp.where(at < 64, third, 0.0)
        first, second, third = roll(first, 64), roll(second, 96), third
        late = jnp.where(at < 32, first, jnp.where(at < 64, second, third))
        v_small[...] = jnp.where(at < 96, late, 0.0)
        place = jnp.where(plane == 2, jnp.where(y_idx < 32, 96 + y_idx, 192 + y_idx), plane * 128 + y_idx)
        for k in range(tiles):
            lanes = slice(k * 128, k * 128 + 128)
            hot = jnp.where(iota((288, 128), 0) == place[k : k + 1], 1.0, 0.0).astype(BF16)
            at_g[:288, lanes] = hot
            at_g[288:, lanes] = hot[256:]
        chans = st.shape[1]
        sym_rows = st[...].reshape(st.shape[0] * chans, chans)
        slot = pa[...] * chans + pc[...]
        hot_p = jnp.where(iota((proj_n, proj_n), 0) == slot, 1.0, 0.0)
        hot_c = jnp.where(iota((chans, proj_n), 0) == pc[...], 1.0, 0.0)
        reach = dot_full(sym_rows, hot_c)
        reach = jnp.where(iota((proj_n, proj_n), 0) // chans == pa[...], reach, 0.0)
        half = 0.5 * (dot_full(hot_p, reach, TN) + dot_full(reach, hot_p, TN))
        coup[...] = jnp.concatenate([half, half], axis=1)

    proj_n = pa.shape[1]
    lane = iota((1, 128), 1)
    lane32 = iota((ga_n, 128), 1)

    def roll(x, by):
        return pltpu.roll(x, by, 1)

    low = lane32 < 64

    def moved_by(x, by):
        return x if by % 128 == 0 else roll(x, by % 128)

    def box(lot):
        return (send_big, recv_big, 16) if lot % 2 == 0 else (send_small, recv_small, 8)

    def rows_of(lot):
        return 9 if lot % 2 == 0 else (7 if lot == 3 else 6)

    def put(lot, row, value):
        ref, _, slot = box(lot)
        ref[lot // 2, pl.ds(row, ga_n, stride=slot), :] = value

    def exchange(lot):
        out, into, slot = box(lot)
        n = lot // 2
        mine = pl.ds(pl.multiple_of(me * slot, slot), rows_of(lot))
        for other in others:
            pltpu.make_async_remote_copy(
                src_ref=out.at[n, pl.ds(pl.multiple_of(other * slot, slot), rows_of(lot)), :],
                dst_ref=into.at[n, mine, :],
                send_sem=send_sem.at[lot],
                recv_sem=recv_sem.at[lot],
                device_id={"ga": other},
                device_id_type=MESH,
            ).start()
        into[n, mine, :] = out[n, mine, :]

    def wait_exchange(lot):
        out, into, _ = box(lot)
        span = pl.ds(0, (ga_n - 1) * rows_of(lot))
        pltpu.make_async_remote_copy(
            src_ref=out.at[lot // 2, span, :],
            dst_ref=into.at[lot // 2, span, :],
            send_sem=send_sem.at[lot],
            recv_sem=recv_sem.at[lot],
            device_id={"ga": others[0]},
            device_id_type=MESH,
        ).wait()

    def got_rows(lot, row):
        _, ref, slot = box(lot)
        return ref[lot // 2, pl.ds(row, ga_n, stride=slot), :]

    def spread_rows(ref_send, ref_recv, sem):
        for other in others:
            pltpu.make_async_remote_copy(
                src_ref=ref_send, dst_ref=ref_recv.at[me], send_sem=send_sem.at[sem], recv_sem=recv_sem.at[sem],
                device_id={"ga": other}, device_id_type=MESH,
            ).start()

    def spread_band(ref_send, ref_recv, sem):
        for other in other_bands:
            pltpu.make_async_remote_copy(
                src_ref=ref_send, dst_ref=ref_recv, send_sem=send_sem.at[sem], recv_sem=recv_sem.at[sem],
                device_id={"band": other}, device_id_type=MESH,
            ).start()

    def wait_rows(ref_recv, sem, count, axis, size, mine):
        span = ref_recv.at[pl.ds(0, count)]
        pltpu.make_async_remote_copy(
            src_ref=span, dst_ref=span, send_sem=send_sem.at[sem], recv_sem=recv_sem.at[sem],
            device_id={axis: lax.rem(mine + 1, size)}, device_id_type=MESH,
        ).wait()

    def cell(row, at):
        return jnp.sum(jnp.where(lane == at, row, 0.0), axis=1, keepdims=True)

    def fold(x):
        total = x[:, :128]
        for k in range(1, tiles):
            total = total + x[:, k * 128 : k * 128 + 128]
        return total[0:1] + total[1:2]

    def as_row(folded):
        stack = jnp.concatenate(folded + [jnp.zeros((1, 128), F32)] * (-len(folded) % 8), axis=0)
        col = jnp.sum(stack, axis=1, keepdims=True)
        hit = iota(stack.shape, 0) == iota(stack.shape, 1)
        return jnp.sum(jnp.where(hit, col, 0.0), axis=0, keepdims=True)

    def start_sums(which, row):
        row_send[which] = row
        spread_rows(row_send.at[which], row_recv.at[which], 12 + which)
        row_recv[which, me] = row_send[which]

    def end_sums(which):
        wait_rows(row_recv.at[which], 12 + which, ga_n - 1, "ga", ga_n, me)
        return jnp.sum(row_recv[which], axis=0) * (1.0 / total_pw)

    def all_sums(which, folded):
        start_sums(which, as_row(folded))
        total = end_sums(which)
        return total

    def apply_h(turn, v):
        base = ((0, 64, 0), (0, 32, 64))

        def onto_grid(h):
            count, at = share[h], share_at[h]
            t_all = None
            for k in range(0, pw, 256):
                lanes = slice(k, k + 256)
                e_c = e_tab[at : at + count, lanes]
                e_s = e_tab[at + count : at + 2 * count, lanes]
                v_re, v_im = v[0:1, lanes], v[1:2, lanes]
                hi_re, lo_re = split(e_c * v_re - e_s * v_im)
                hi_im, lo_im = split(e_s * v_re + e_c * v_im)
                got = dot(jnp.concatenate([hi_re, hi_im, lo_re, lo_im], axis=0), at_s[lanes, :])
                t_all = got if t_all is None else t_all + got
            return t_all[: 2 * count] + t_all[2 * count :]

        def along_y(h, t_all):
            count = share[h]
            if turn == 0 and h == 0:
                loads[3].wait()
            rows = []
            for i in range(planes):
                lanes = slice(i * 128, i * 128 + 128)
                rows.append(jnp.concatenate([t_all[:count, lanes], t_all[count:, lanes]], axis=1))
            rows.append(jnp.zeros((64 if h == 0 else 32, 256), F32))
            hi, lo = split(jnp.concatenate(rows, axis=0))
            u = dot_tab(tabs[0], hi, lo, NT)
            lot = 4 * turn + h
            last = None
            for c in range(2):
                for i in range(planes):
                    n = c * planes + i
                    tile = 128 if h == 0 and i == 2 else 0
                    spread = []
                    for j in range(planes):
                        at = c * grid_len + j * ga_n
                        to = 32 * j if h == 1 else (64 * j if j < 2 else 64 * (n % 2))
                        spread.append(moved_by(u[at : at + ga_n, tile : tile + 128], to - base[h][i]))
                    if h == 1:
                        put(lot, n, jnp.where(lane32 < 32, spread[0], jnp.where(low, spread[1], spread[2])))
                        continue
                    put(lot, n, jnp.where(low, spread[0], spread[1]))
                    if n % 2 == 1:
                        put(lot, 6 + n // 2, jnp.where(low, last, spread[2]))
                    last = spread[2]

        first = onto_grid(0)
        along_y(0, first)
        if turn == 0:
            pl.semaphore_wait(barrier, ga_n - 1 + band_n - 1)
        exchange(4 * turn)
        second = onto_grid(1)
        along_y(1, second)
        exchange(4 * turn + 1)

        if turn == 0:
            loads[4].wait()
        acc_re = jnp.zeros((proj_n, 128), F32)
        acc_im = jnp.zeros((proj_n, 128), F32)
        for k in range(tiles):
            lanes = slice(k * 128, k * 128 + 128)
            p_re, p_im = pj[0, :, lanes], pj[1, :, lanes]
            v_re, v_im = v[0:1, lanes], v[1:2, lanes]
            acc_re = acc_re + (p_re * v_re + p_im * v_im)
            acc_im = acc_im + (p_re * v_im - p_im * v_re)
        col_re = jnp.sum(acc_re, axis=1, keepdims=True)
        col_im = jnp.sum(acc_im, axis=1, keepdims=True)
        row64, lane64 = iota((proj_n, 128), 0), iota((proj_n, 128), 1)
        diag = jnp.where(lane64 == row64, col_re, jnp.where(lane64 == row64 + proj_n, col_im, 0.0))
        start_sums(3 + turn, jnp.sum(diag, axis=0, keepdims=True))
        norm_row = dens = None
        if turn == 0:
            norm_row = as_row([fold(v * v), fold(v * v * kin_ref[...])])
            later_tables()
        if turn == 2:
            spread_band(bands.at[my_band], bands.at[my_band], 19)
        for h in range(2):
            lot = 4 * turn + h
            wait_exchange(lot)
            main = jnp.concatenate([got_rows(lot, n) for n in range(6)], axis=0)
            if h == 0:
                rest = [got_rows(lot, 6 + n) for n in range(3)]
                side = [moved_by(rest[n // 2], 64 * (n % 2)) for n in range(6)]
                main = jnp.concatenate([main, jnp.concatenate(side, axis=0)], axis=1)
            hi, lo = split(main)
            w = dot_tab(tabs[1, :, : 2 * grid_len], hi, lo)
            w_re, w_im = w[:grid_len], w[grid_len:]
            v_here = v_small[...] if h else v_big[...]
            vw_re, vw_im = v_here * w_re, v_here * w_im
            lot = 4 * turn + 2 + h
            if turn == 0:
                part = jnp.sum(vw_re * w_re + vw_im * w_im, axis=0, keepdims=True)
                if h == 0:
                    dens = part[:, :128] + part[:, 128:]
                else:
                    dens = jnp.sum(dens + part, axis=1, keepdims=True)
                    put(lot, 6, jnp.broadcast_to(jnp.where(lane == 2, dens, norm_row), (ga_n, 128)))
            hi, lo = split(jnp.concatenate([vw_re, vw_im], axis=0))
            back = dot_tab(tabs[2, :, : 2 * grid_len], hi, lo)
            for n in range(6):
                put(lot, n, back[n * ga_n : (n + 1) * ga_n, :128])
            if h == 0:
                for n in range(0, 6, 2):
                    even, odd = back[n * ga_n : (n + 1) * ga_n, 128:], back[(n + 1) * ga_n : (n + 2) * ga_n, 128:]
                    put(lot, 6 + n // 2, jnp.where(low, even, roll(odd, 64)))
            exchange(lot)

        tot = end_sums(3 + turn)
        prod = coup[...] * tot
        mix_re = jnp.sum(jnp.where(lane64 < proj_n, prod, 0.0), axis=1, keepdims=True)
        mix_im = jnp.sum(jnp.where(lane64 < proj_n, 0.0, prod), axis=1, keepdims=True)
        c_n = None
        if turn == 0:
            diag_row = jnp.where(lane64 == row64, mix_re, jnp.where(lane64 == row64 + proj_n, mix_im, 0.0))
            c_n = jnp.sum(jnp.sum(diag_row, axis=0, keepdims=True) * tot, axis=1, keepdims=True)
        for k in range(tiles):
            lanes = slice(k * 128, k * 128 + 128)
            p_re, p_im = pj[0, :, lanes], pj[1, :, lanes]
            n_re = jnp.sum(p_re * mix_re - p_im * mix_im, axis=0, keepdims=True)
            n_im = jnp.sum(p_im * mix_re + p_re * mix_im, axis=0, keepdims=True)
            hvec[:, lanes] = jnp.concatenate([n_re, n_im], axis=0) + kin_ref[:, lanes] * v[:, lanes]
        for h in range(2):
            lot = 4 * turn + 2 + h
            wait_exchange(lot)
            count, at = share[h], share_at[h]
            gt, gt_rest = (gt_small, rest_small) if h else (gt_big, rest_big)
            if h == 0:
                rest = [got_rows(lot, 6 + n) for n in range(3)]
            left, right = [], []
            for c in range(2):
                mains = [got_rows(lot, c * planes + i) for i in range(planes)]
                for j in range(planes):
                    if h == 1:
                        p = [moved_by(mains[i], 32 * (i - j)) for i in range(planes)]
                        left.append(jnp.where(lane32 < 32, p[0], jnp.where(low, p[1], p[2])))
                        continue
                    p = []
                    for i in range(planes):
                        n = c * planes + i
                        if j < 2:
                            p.append(moved_by(mains[i], base[0][i] - 64 * j))
                        else:
                            p.append(moved_by(rest[n // 2], base[0][i] - 64 * (n % 2)))
                    left.append(jnp.where(low, p[0], p[1]))
                    right.append(p[2])
            turned = jnp.concatenate(left, axis=0).T
            if h == 0:
                turned = jnp.concatenate([turned, jnp.concatenate(right, axis=0).T[:64]], axis=0)
            else:
                turned = turned[:96]
            hi, lo = split(turned)
            rows = hi.shape[0]
            out = dot(jnp.concatenate([hi, lo], axis=0), tabs[3, : 2 * grid_len])
            out = out[:rows] + out[rows:] + dot(hi, tabs[3, 2 * grid_len :])
            for c in range(2):
                first, second, third = [out[i * count : (i + 1) * count, c * 128 : c * 128 + 128] for i in range(planes)]
                late = roll(third, 64)
                rows = slice(c * count, (c + 1) * count)
                rows_lo = slice((2 + c) * count, (3 + c) * count)
                wide = lane < 96
                hi, lo = split(jnp.concatenate([jnp.where(wide, first, roll(third, 96)), jnp.where(wide, second, late)], axis=1))
                gt[rows, :] = hi
                gt[rows_lo, :] = lo
                high = late.astype(BF16).astype(F32)
                gt_rest[rows, :] = jnp.where(lane < 32, high, roll(late - high, 32)).astype(BF16)
            for k in range(0, pw, 256):
                lanes = slice(k, k + 256)
                q = dot(gt[...], at_g[:256, lanes])
                q = q[: 2 * count] + q[2 * count :] + dot(gt_rest[:, :64], at_g[256:, lanes])
                q_re, q_im = q[:count], q[count:]
                e_c = e_tab[at : at + count, lanes]
                e_s = e_tab[at + count : at + 2 * count, lanes]
                l_re = jnp.sum(e_c * q_re + e_s * q_im, axis=0, keepdims=True)
                l_im = jnp.sum(e_c * q_im - e_s * q_re, axis=0, keepdims=True)
                hvec[:, lanes] = hvec[:, lanes] + jnp.concatenate([l_re, l_im], axis=0)
        return c_n

    def precondition(r, level):
        ratio = kin_ref[...] / (1.5 * level + 1.0)
        numer = 27.0 + ratio * (18.0 + ratio * (12.0 + 8.0 * ratio))
        square = ratio * ratio
        return r * (numer / (numer + 16.0 * square * square))

    eps = small_eps

    loads[2].wait()
    vecs[0] = jnp.concatenate([cf[0], cf[1]], axis=0)
    c_n = apply_h(0, vecs[0])
    tot = jnp.sum(got_rows(3, 6), axis=0, keepdims=True) * (1.0 / total_pw)
    guess_cc = cell(tot, 0)
    guess = (cell(tot, 1) + cell(tot, 2) * (1.0 / grid_len**3) + c_n) / (guess_cc + eps)
    c = vecs[0]
    h0 = hvec[...]
    s = h0 - guess * c
    kc, ks = kin_ref[...] * c, kin_ref[...] * s
    tot = all_sums(0, [fold(c * c), fold(c * s), fold(s * s), fold(kc * c), fold(kc * s), fold(ks * s)])
    cc, cs, ss, kcc, kcs, kss = [cell(tot, n) for n in range(6)]
    shift = (cs - guess * eps) / (cc + eps)
    e0 = guess + shift
    r0 = s - shift * c
    rr = ss - 2.0 * shift * cs + shift * shift * cc
    krr = kss - 2.0 * shift * kcs + shift * shift * kcc
    rc = cs - shift * cc
    krc = kcs - shift * kcc
    p0 = precondition(r0, krr / (rr + eps))
    vecs[1] = r0
    vecs[2] = p0
    vecs[3] = h0

    apply_h(1, vecs[2])
    c, r0, p0, h0 = vecs[0], vecs[1], vecs[2], vecs[3]
    g0 = hvec[...]
    q0 = g0 - e0 * p0
    pairs = [(r0, q0), (r0, p0), (q0, q0), (q0, c), (q0, p0), (c, p0), (p0, p0)]
    prods = [a * b for a, b in pairs]
    tot = all_sums(1, [fold(x) for x in prods] + [fold(x * kin_ref[...]) for x in prods])
    rq, rp, qq, qc, qp, cp, pp = [cell(tot, n) for n in range(7)]
    krq, krp, kqq, kqc, kqp, kcp, kpp = [cell(tot, n) for n in range(7, 14)]
    l0 = -rq / (qq + eps)
    bb = cc + 2.0 * l0 * cp + l0 * l0 * pp
    b_rho = rc + l0 * (qc + rp) + l0 * l0 * qp
    d1 = (b_rho - e0 * eps) / (bb + eps)
    fa, fb, fc = -l0, d1, d1 * l0
    r_dr = fa * rq + fb * rc + fc * rp
    dr_dr = fa * fa * qq + fb * fb * cc + fc * fc * pp + 2.0 * (fa * fb * qc + fa * fc * qp + fb * fc * cp)
    kr_dr = fa * krq + fb * krc + fc * krp
    kdr_dr = fa * fa * kqq + fb * fb * kcc + fc * fc * kpp + 2.0 * (fa * fb * kqc + fa * fc * kqp + fb * fc * kcp)
    wt = r_dr / (dr_dr + eps)
    lm = wt * l0
    bmbm = cc + 2.0 * lm * cp + lm * lm * pp
    bm_rho = rc + lm * (qc + rp) + lm * lm * qp
    dm = (bm_rho - e0 * eps) / (bmbm + eps)
    em = e0 + dm
    mm = rr - 2.0 * wt * r_dr + wt * wt * dr_dr
    kmm = krr - 2.0 * wt * kr_dr + wt * wt * kdr_dr
    bm = c + lm * p0
    hm = h0 + lm * g0
    rm = r0 - wt * (fa * q0 + fb * c + fc * p0)
    sm = r0 + lm * q0 - dm * bm
    p1 = precondition(rm, kmm / (mm + eps))
    vecs[4] = bm
    vecs[5] = hm
    vecs[6] = rm
    vecs[7] = sm
    vecs[8] = p1
    bands[my_band] = jnp.concatenate([bm, p1], axis=0)

    apply_h(2, vecs[8])
    bm, hm, rm, sm, p1 = vecs[4], vecs[5], vecs[6], vecs[7], vecs[8]
    g1 = hvec[...]
    q1 = g1 - em * p1
    start_sums(2, as_row([fold(rm * q1), fold(q1 * q1)]))
    span = bands.at[pl.ds(0, band_n - 1)]
    pltpu.make_async_remote_copy(
        src_ref=span, dst_ref=span, send_sem=send_sem.at[19], recv_sem=recv_sem.at[19],
        device_id={"band": other_bands[0]}, device_id_type=MESH,
    ).wait()
    left = jnp.concatenate([bm, p1, hm, g1], axis=0)
    gram = dot_full(left, jnp.concatenate([bands[j] for j in range(band_n)], axis=0), NT)
    wide = (band_n * 4, 128)
    moved = iota(wide, 0) % 4 * band_n + iota(wide, 0) // 4
    gram = dot_full(gram, jnp.where(moved == iota(wide, 1), 1.0, 0.0))
    pairs = [(sm, sm), (sm, q1), (sm, bm), (sm, p1), (q1, bm), (q1, p1), (bm, bm), (bm, p1), (p1, p1)]
    row = as_row([fold(a * b) for a, b in pairs])
    gram_send[:8, :] = gram
    gram_send[8:9, :] = row
    spread_rows(gram_send, gram_recv, 18)
    gram_recv[me] = gram_send[...]
    tot = end_sums(2)
    rq, qq = cell(tot, 0), cell(tot, 1)
    l1 = -rq / (qq + eps)
    lam_send[...] = jnp.broadcast_to(l1, (1, 128))
    spread_band(lam_send, lam_recv.at[my_band], 20)
    lam_recv[my_band] = lam_send[...]
    wait_rows(gram_recv, 18, ga_n - 1, "ga", ga_n, me)
    summed = jnp.sum(gram_recv[...], axis=0) * (1.0 / total_pw)
    gram, tot = summed[:8], summed[8:9]
    ss, sq, sb, sp, qb, qp, bb, bp, pp = [cell(tot, n) for n in range(9)]

    new = bm + l1 * p1
    nb_out[0] = new[0:1]
    nb_out[1] = new[1:2]
    nn = bb + 2.0 * l1 * bp + l1 * l1 * pp
    n_sig = sb + l1 * (sp + qb) + l1 * l1 * qp
    sig_sig = ss + 2.0 * l1 * sq + l1 * l1 * qq
    shift = (n_sig - em * eps) / (nn + eps)
    energy = em + shift
    res = (sig_sig - 2.0 * shift * n_sig + shift * shift * nn) / (nn + eps)

    wait_rows(lam_recv, 20, band_n - 1, "band", band_n, my_band)
    lams = jnp.zeros((1, 128), F32)
    for j in range(band_n):
        lams = jnp.where(lane == j, lam_recv[j], lams)

    def part(rows, v):
        return rows[:, v * band_n : (v + 1) * band_n]

    lam8 = lams[:, :band_n]

    def finish(rows):
        a = rows[0:2] + l1 * rows[2:4]
        against_re = part(a, 0) + lam8 * part(a, 2)
        against_im = part(a, 1) + lam8 * part(a, 3)
        return (against_re[0:1] + against_im[1:2], against_im[0:1] - against_re[1:2])

    cor_re, cor_im = finish(gram[0:4])
    sub_re, sub_im = finish(gram[4:8])
    tail = jnp.concatenate([jnp.broadcast_to(energy, (1, band_n)), jnp.broadcast_to(res, (1, band_n))], axis=0)
    block = jnp.concatenate([cor_re, cor_im, sub_re, sub_im, tail, tail], axis=0)
    small_out[...] = jnp.concatenate([block, jnp.zeros((8, 128 - band_n), F32)], axis=1)


def body(tables, coeffs, cell_map, potential, projectors, strengths, proj_atom, proj_chan):
    ga_n = lax.axis_size("ga")
    band_n = lax.axis_size("band")
    grid_len = potential.shape[0]
    pw = coeffs.shape[2]
    proj_n = proj_atom.shape[0]
    total_pw = pw * ga_n
    vmem = pl.BlockSpec(memory_space=pltpu.VMEM)
    hbm = pl.BlockSpec(memory_space=pltpu.HBM)
    z_tab, tabs = tables
    args = (cell_map.reshape(pw // 128, 128), z_tab, coeffs, tabs, projectors, jnp.transpose(potential, (1, 0, 2)),
            strengths, proj_atom.reshape(1, proj_n), proj_chan.reshape(1, proj_n))
    V = pltpu.VMEM
    scratch = [V(a.shape, a.dtype) for a in args] + [
        V((pw, 3 * 128), BF16), V((320, pw), BF16), V((2 * grid_len, pw), F32),
        V((256, 256), BF16), V((128, 256), BF16), V((128, 128), BF16), V((64, 128), BF16),
        V((grid_len, 256), F32), V((grid_len, 128), F32),
        V((proj_n, 2 * proj_n), F32), V((9, 2, pw), F32), V((2, pw), F32), V((1, pw), F32),
        V((6, ga_n * 16, 128), F32), V((6, ga_n * 16, 128), F32),
        V((6, ga_n * 8, 128), F32), V((6, ga_n * 8, 128), F32),
        V((6, 1, 128), F32), V((6, ga_n, 1, 128), F32),
        V((9, 128), F32), V((ga_n, 9, 128), F32),
        V((band_n, 4, pw), F32), V((1, 128), F32), V((band_n, 1, 128), F32),
        pltpu.SemaphoreType.DMA((21,)), pltpu.SemaphoreType.DMA((21,)), pltpu.SemaphoreType.DMA((len(args),)),
    ]
    args = [pltpu.with_memory_space_constraint(a, pltpu.HBM) for a in args]
    new_bands, small = pl.pallas_call(
        functools.partial(kernel, (ga_n, band_n, grid_len, total_pw)),
        out_shape=(
            jax.ShapeDtypeStruct((2, 1, pw), F32),
            jax.ShapeDtypeStruct((8, 128), F32),
        ),
        in_specs=[hbm] * len(args),
        out_specs=(vmem, vmem),
        scratch_shapes=scratch,
        compiler_params=pltpu.CompilerParams(collective_id=0, has_side_effects=True, vmem_limit_bytes=24 * 2**20),
    )(*args)

    def deal(nb, sm, nb_o, en_o, re_o, co_o, su_o):
        nb_o[...] = nb[...]
        co_o[0], co_o[1] = sm[0:1, :band_n], sm[1:2, :band_n]
        su_o[0], su_o[1] = sm[2:3, :band_n], sm[3:4, :band_n]
        en_o[...] = sm[4:5, :1]
        re_o[...] = sm[5:6, :1]

    one = jax.ShapeDtypeStruct((1, 1), F32)
    rows = jax.ShapeDtypeStruct((2, 1, band_n), F32)
    new_bands, energy, res, corr, sub = pl.pallas_call(
        deal,
        out_shape=(jax.ShapeDtypeStruct((2, 1, pw), F32), one, one, rows, rows),
        in_specs=[vmem] * 2,
        out_specs=(vmem,) * 5,
        compiler_params=pltpu.CompilerParams(vmem_limit_bytes=2**20),
    )(new_bands, small)
    return new_bands, energy.reshape(1), res.reshape(1), corr, sub


def solution(mesh):
    tables = make_tables(96, mesh.shape["ga"])
    placed = (P(None, "band", "ga"), P("ga"), P(None, "ga", None), P(None, None, "ga"), P(), P(), P())
    return jax.shard_map(
        functools.partial(body, tables),
        mesh=mesh,
        in_specs=placed,
        out_specs=(P(None, "band", "ga"), P("band"), P("band"), P(None, "band", None), P(None, "band", None)),
        check_vma=False,
    )
```

```python
import functools

import jax
import jax.numpy as jnp
import numpy as np
from jax import lax
from jax.experimental import pallas as pl
from jax.experimental.pallas import tpu as pltpu
from jax.sharding import PartitionSpec as P

F32 = jnp.float32
BF16 = jnp.bfloat16
HIGHEST = lax.Precision.HIGHEST
MESH = pl.DeviceIdType.MESH
kin_unit = 0.02
small_eps = 1e-06

NN = (((1,), (0,)), ((), ()))
NT = (((1,), (1,)), ((), ()))
TN = (((0,), (0,)), ((), ()))


def parts_of(table, count):
    out = []
    left = np.asarray(table, np.float64)
    for _ in range(count):
        piece = left.astype(np.float32).astype(BF16)
        out.append(piece)
        left = left - piece.astype(np.float64)
    return out


def make_tables(grid_len, groups):
    planes = grid_len // groups
    natural = np.arange(grid_len)
    slab = (natural % groups) * planes + natural // groups

    def angles(rows, cols):
        return 2.0 * np.pi / grid_len * ((rows[:, None] * cols[None, :]) % grid_len)

    z_ang = angles(natural, natural)
    x_cos, x_sin = np.cos(z_ang), np.sin(z_ang)
    half = grid_len // 2
    z_high, z_low = parts_of(np.concatenate([x_cos[:half], x_sin[:half], x_cos[half:], x_sin[half:]], axis=0), 2)
    y_ang = angles(slab, natural)
    y_cos, y_sin = np.cos(y_ang), np.sin(y_ang)
    pad = np.zeros((grid_len, 128 - grid_len))
    side = np.zeros((2 * grid_len, 256 - 2 * grid_len))
    y_fwd = np.block([[y_cos, pad, -y_sin, pad], [y_sin, pad, y_cos, pad]])
    x_fwd = np.block([[x_cos, -x_sin], [x_sin, x_cos]])
    x_back = np.block([[x_cos, x_sin], [-x_sin, x_cos]]) / grid_len
    x_fwd, x_back = np.concatenate([x_fwd, side], axis=1), np.concatenate([x_back, side], axis=1)
    y_back = y_fwd / grid_len**2
    rest = []
    for tab in (y_fwd, x_fwd, x_back, y_back):
        rest.append(np.concatenate(parts_of(tab, 2), axis=0))
    return [np.concatenate([z_high, z_low], axis=1), np.stack(rest)]


def dot(a, b, dims=NN):
    return lax.dot_general(a, b, dims, preferred_element_type=F32)


def dot_full(a, b, dims=NN):
    return lax.dot_general(a, b, dims, precision=HIGHEST, preferred_element_type=F32)


def dot_tab(tab, hi, lo, dims=NN):
    rows = tab.shape[0] // 2
    both = dot(tab, hi, dims)
    return both[:rows] + both[rows:] + dot(tab[:rows], lo, dims)


def split(x):
    hi = x.astype(BF16)
    return hi, (x - hi.astype(F32)).astype(BF16)


def iota(shape, axis):
    return lax.broadcasted_iota(jnp.int32, shape, axis)


def hops(k):
    return min(k, 4 - k)


def far_first():
    steps = [(i, j) for i in range(4) for j in range(4) if (i, j) != (0, 0)]
    return [[s for s in steps if hops(s[0]) + hops(s[1]) == far] for far in (4, 3, 2, 1)]


def kernel(sizes, cm_far, zt_far, cf_far, tabs_far, pj_far, pot_far, st_far, pa_far, pc_far,
           nb_out, small_out,
           cm, zt, cf, tabs, pj, pot, st, pa, pc, at_s, at_g, e_tab, gt, gt_rest, v_tab, coup, vecs, hvec, kin_ref,
           send, recv, row_send, row_recv, gram_send, gram_recv, bands, lam_send, lam_recv,
           send_sem, recv_sem, load_sem):
    ga_n, band_n, grid_len, total_pw = sizes
    planes = grid_len // ga_n
    me = lax.axis_index("ga")
    my_band = lax.axis_index("band")
    pw = cf.shape[2]
    tiles = pw // 128
    far = (cm_far, zt_far, cf_far, tabs_far, pj_far, pot_far, st_far, pa_far, pc_far)
    near = (cm, zt, cf, tabs, pj, pot, st, pa, pc)
    loads = [pltpu.make_async_copy(a, b, load_sem.at[n]) for n, (a, b) in enumerate(zip(far, near))]
    loads[0].start()
    loads[1].start()

    barrier = pltpu.get_barrier_semaphore()
    m_x, m_y, m_c = me // 8, me // 2 % 4, me % 2

    others = []
    for group in far_first():
        for core in (0, 1):
            others += [((m_x + i) % 4) * 8 + ((m_y + j) % 4) * 2 + core for i, j in group]
    others.append(m_x * 8 + m_y * 2 + 1 - m_c)
    band_order = sorted(range(1, band_n), key=lambda k: -min(k, band_n - k))
    other_bands = [lax.rem(my_band + k, band_n) for k in band_order]

    for other in others:
        pl.semaphore_signal(barrier, inc=1, device_id={"ga": other}, device_id_type=MESH)
    for other in other_bands:
        pl.semaphore_signal(barrier, inc=1, device_id={"band": other}, device_id_type=MESH)

    for load in loads[2:]:
        load.start()
    zeros = jnp.zeros((ga_n, 128), F32)
    for lot in range(12):
        send[lot, pl.ds(7, ga_n, stride=8), :] = zeros
    loads[0].wait()
    loads[1].wait()

    cells = cm[...]
    py = lax.shift_right_logical(cells * 43691, 22)
    z_idx = cells - py * grid_len
    plane = (py >= grid_len).astype(jnp.int32) + (py >= 2 * grid_len).astype(jnp.int32)
    y_idx = py - plane * grid_len
    x_idx = me + ga_n * plane
    py_pad = plane * 128 + y_idx

    def freq(k):
        return jnp.where(2 * k < grid_len, k, k - grid_len).astype(F32)

    kin = kin_unit * (freq(x_idx) * freq(x_idx) + freq(y_idx) * freq(y_idx) + freq(z_idx) * freq(z_idx))
    for k in range(tiles):
        lanes = slice(k * 128, k * 128 + 128)
        kin_ref[:, lanes] = kin[k : k + 1]
    for k in range(0, tiles, 2):
        row = jnp.concatenate([z_idx[k : k + 1], z_idx[k + 1 : k + 2]], axis=1)
        hot = jnp.where(iota((grid_len, 256), 0) == row, 1.0, 0.0).astype(BF16)
        e_tab[:, k * 128 : k * 128 + 256] = dot(zt[...], jnp.concatenate([hot, hot], axis=0))
    upright = jnp.transpose(jnp.concatenate([py_pad, jnp.zeros((128 - tiles, 128), jnp.int32)], axis=0))
    for k in range(tiles):
        hot = (iota((128, 3 * 128), 1) == upright[:, k : k + 1])
        at_s[k * 128 : k * 128 + 128, :] = jnp.where(hot, 1.0, 0.0).astype(BF16)
    half_len = grid_len // 2

    def later_tables():
        for load in loads[5:]:
            load.wait()
        blank = jnp.zeros((grid_len, 128 - grid_len), F32)
        at = iota((grid_len, 128), 1)
        slabs = [jnp.concatenate([pot[j], blank], axis=1) for j in range(planes)]
        for h in range(2):
            first, second, third = [moved_by(slabs[j], 48 * j - 48 * h) for j in range(planes)]
            v_tab[h, :, :128] = jnp.where(at < 48, first, jnp.where(at < 96, second, third))
            v_tab[h, :, 128:] = jnp.where(at < 16, moved_by(slabs[2], -48 * h - 32), 0.0)
        place = jnp.where(plane == 2, jnp.where(y_idx < 32, 96 + y_idx, 192 + y_idx), plane * 128 + y_idx)
        for k in range(tiles):
            lanes = slice(k * 128, k * 128 + 128)
            hot = jnp.where(iota((288, 128), 0) == place[k : k + 1], 1.0, 0.0).astype(BF16)
            at_g[:288, lanes] = hot
            at_g[288:, lanes] = hot[256:]
        chans = st.shape[1]
        sym_rows = st[...].reshape(st.shape[0] * chans, chans)
        slot = pa[...] * chans + pc[...]
        hot_p = jnp.where(iota((proj_n, proj_n), 0) == slot, 1.0, 0.0)
        hot_c = jnp.where(iota((chans, proj_n), 0) == pc[...], 1.0, 0.0)
        reach = dot_full(sym_rows, hot_c)
        reach = jnp.where(iota((proj_n, proj_n), 0) // chans == pa[...], reach, 0.0)
        half = 0.5 * (dot_full(hot_p, reach, TN) + dot_full(reach, hot_p, TN))
        coup[...] = jnp.concatenate([half, half], axis=1)

    proj_n = pa.shape[1]
    lane = iota((1, 128), 1)
    lane32 = iota((ga_n, 128), 1)

    def roll(x, by):
        return pltpu.roll(x, by, 1)

    lane16 = lane32 // 16

    def gather_rest(pieces):
        rest = pieces[0]
        for n in range(1, 6):
            rest = jnp.where(lane16 == n, roll(pieces[n], 16 * n), rest)
        return rest

    def moved_by(x, by):
        return x if by % 128 == 0 else roll(x, by % 128)

    def put(lot, row, value):
        send[lot, pl.ds(row, ga_n, stride=8), :] = value

    def exchange(lot, start=0, stop=ga_n - 1):
        rows = 8 if lot in (2, 3) else 7
        mine = pl.ds(pl.multiple_of(me * 8, 8), rows)
        for other in others[start:stop]:
            pltpu.make_async_remote_copy(
                src_ref=send.at[lot, pl.ds(pl.multiple_of(other * 8, 8), rows), :],
                dst_ref=recv.at[lot, mine, :],
                send_sem=send_sem.at[lot],
                recv_sem=recv_sem.at[lot],
                device_id={"ga": other},
                device_id_type=MESH,
            ).start()
        if stop == ga_n - 1:
            recv[lot, mine, :] = send[lot, mine, :]

    def wait_exchange(lot):
        span = pl.ds(0, (ga_n - 1) * (8 if lot in (2, 3) else 7))
        pltpu.make_async_remote_copy(
            src_ref=send.at[lot, span, :],
            dst_ref=recv.at[lot, span, :],
            send_sem=send_sem.at[lot],
            recv_sem=recv_sem.at[lot],
            device_id={"ga": others[0]},
            device_id_type=MESH,
        ).wait()

    def got_rows(lot, row):
        return recv[lot, pl.ds(row, ga_n, stride=8), :]

    def spread_rows(ref_send, ref_recv, sem):
        for other in others:
            pltpu.make_async_remote_copy(
                src_ref=ref_send, dst_ref=ref_recv.at[me], send_sem=send_sem.at[sem], recv_sem=recv_sem.at[sem],
                device_id={"ga": other}, device_id_type=MESH,
            ).start()

    def spread_band(ref_send, ref_recv, sem):
        for other in other_bands:
            pltpu.make_async_remote_copy(
                src_ref=ref_send, dst_ref=ref_recv, send_sem=send_sem.at[sem], recv_sem=recv_sem.at[sem],
                device_id={"band": other}, device_id_type=MESH,
            ).start()

    def wait_rows(ref_recv, sem, count, axis, size, mine):
        span = ref_recv.at[pl.ds(0, count)]
        pltpu.make_async_remote_copy(
            src_ref=span, dst_ref=span, send_sem=send_sem.at[sem], recv_sem=recv_sem.at[sem],
            device_id={axis: lax.rem(mine + 1, size)}, device_id_type=MESH,
        ).wait()

    def cell(row, at):
        return jnp.sum(jnp.where(lane == at, row, 0.0), axis=1, keepdims=True)

    def fold(x):
        total = x[:, :128]
        for k in range(1, tiles):
            total = total + x[:, k * 128 : k * 128 + 128]
        return total[0:1] + total[1:2]

    def as_row(folded):
        stack = jnp.concatenate(folded + [jnp.zeros((1, 128), F32)] * (-len(folded) % 8), axis=0)
        col = jnp.sum(stack, axis=1, keepdims=True)
        hit = iota(stack.shape, 0) == iota(stack.shape, 1)
        return jnp.sum(jnp.where(hit, col, 0.0), axis=0, keepdims=True)

    def start_sums(which, row):
        row_send[which] = row
        spread_rows(row_send.at[which], row_recv.at[which], 12 + which)
        row_recv[which, me] = row_send[which]

    def end_sums(which):
        wait_rows(row_recv.at[which], 12 + which, ga_n - 1, "ga", ga_n, me)
        return jnp.sum(row_recv[which], axis=0) * (1.0 / total_pw)

    def all_sums(which, folded):
        start_sums(which, as_row(folded))
        total = end_sums(which)
        return total

    def apply_h(turn, v):
        base = (0, 48, 0)

        def onto_grid(h, sent=None):
            t_all = None
            for k in range(0, pw, 256):
                lanes = slice(k, k + 256)
                e_c = e_tab[h * grid_len : h * grid_len + half_len, lanes]
                e_s = e_tab[h * grid_len + half_len : (h + 1) * grid_len, lanes]
                v_re, v_im = v[0:1, lanes], v[1:2, lanes]
                hi_re, lo_re = split(e_c * v_re - e_s * v_im)
                hi_im, lo_im = split(e_s * v_re + e_c * v_im)
                got = dot(jnp.concatenate([hi_re, hi_im, lo_re, lo_im], axis=0), at_s[lanes, :])
                t_all = got if t_all is None else t_all + got
                if sent is not None and sent < ga_n - 1:
                    exchange(4 * turn, sent, min(sent + 3, ga_n - 1))
                    sent += 3
            return t_all

        def along_y(h, t_all):
            if turn == 0 and h == 0:
                loads[3].wait()
            t_all = t_all[:grid_len] + t_all[grid_len:]
            rows = []
            for i in range(planes):
                lanes = slice(i * 128, i * 128 + 128)
                rows.append(jnp.concatenate([t_all[:half_len, lanes], t_all[half_len:, lanes]], axis=1))
            rows.insert(2, jnp.zeros((32, 256), F32))
            hi, lo = split(jnp.concatenate(rows, axis=0))
            u = dot_tab(tabs[0], hi, lo, NT)
            u = (u[:, :128], u[:, 128:])
            rest = []
            for c in range(2):
                for i in range(planes):
                    spread = []
                    for j in range(planes):
                        at = c * grid_len + j * ga_n
                        piece = u[i // 2][at : at + ga_n]
                        if i == 2:
                            piece = jnp.concatenate([piece, jnp.zeros((ga_n, 128 - half_len), F32)], axis=1)
                        spread.append(moved_by(piece, 48 * j - base[i]))
                    put(4 * turn + h, c * planes + i,
                        jnp.where(lane32 < 48, spread[0], jnp.where(lane32 < 96, spread[1], spread[2])))
                    rest.append(spread[2])
            put(4 * turn + h, 6, gather_rest(rest))

        first = onto_grid(0)
        along_y(0, first)
        if turn == 0:
            pl.semaphore_wait(barrier, ga_n - 1 + band_n - 1)
        exchange(4 * turn, 0, 10)
        second = onto_grid(1, 10)
        along_y(1, second)
        exchange(4 * turn + 1)

        if turn == 0:
            loads[4].wait()
        acc_re = jnp.zeros((proj_n, 128), F32)
        acc_im = jnp.zeros((proj_n, 128), F32)
        for k in range(tiles):
            lanes = slice(k * 128, k * 128 + 128)
            p_re, p_im = pj[0, :, lanes], pj[1, :, lanes]
            v_re, v_im = v[0:1, lanes], v[1:2, lanes]
            acc_re = acc_re + (p_re * v_re + p_im * v_im)
            acc_im = acc_im + (p_re * v_im - p_im * v_re)
        col_re = jnp.sum(acc_re, axis=1, keepdims=True)
        col_im = jnp.sum(acc_im, axis=1, keepdims=True)
        row64, lane64 = iota((proj_n, 128), 0), iota((proj_n, 128), 1)
        diag = jnp.where(lane64 == row64, col_re, jnp.where(lane64 == row64 + proj_n, col_im, 0.0))
        start_sums(3 + turn, jnp.sum(diag, axis=0, keepdims=True))
        norm_row = None
        if turn == 0:
            norm_row = as_row([fold(v * v), fold(v * v * kin_ref[...])])
            later_tables()
        if turn == 2:
            spread_band(bands.at[my_band], bands.at[my_band], 19)
        for h in range(2):
            lot = 4 * turn + h
            wait_exchange(lot)
            rest = got_rows(lot, 6)
            main = jnp.concatenate([got_rows(lot, n) for n in range(6)], axis=0)
            side = jnp.concatenate([moved_by(rest, -16 * n) for n in range(6)], axis=0)
            hi, lo = split(jnp.concatenate([main, side], axis=1))
            w = dot_tab(tabs[1, :, : 2 * grid_len], hi, lo)
            w_re, w_im = w[:grid_len], w[grid_len:]
            vw_re, vw_im = v_tab[h] * w_re, v_tab[h] * w_im
            lot = 4 * turn + 2 + h
            if turn == 0:
                dens = jnp.sum(vw_re * w_re + vw_im * w_im, axis=0, keepdims=True)
                dens = jnp.sum(dens[:, :128] + dens[:, 128:], axis=1, keepdims=True)
                row = norm_row if h == 0 else jnp.zeros((1, 128), F32)
                put(lot, 7, jnp.broadcast_to(jnp.where(lane == 2, dens, row), (ga_n, 128)))
            hi, lo = split(jnp.concatenate([vw_re, vw_im], axis=0))
            back = dot_tab(tabs[2, :, : 2 * grid_len], hi, lo)
            for n in range(6):
                put(lot, n, back[n * ga_n : (n + 1) * ga_n, :128])
            put(lot, 6, gather_rest([back[n * ga_n : (n + 1) * ga_n, 128:] for n in range(6)]))
            exchange(lot)

        tot = end_sums(3 + turn)
        prod = coup[...] * tot
        mix_re = jnp.sum(jnp.where(lane64 < proj_n, prod, 0.0), axis=1, keepdims=True)
        mix_im = jnp.sum(jnp.where(lane64 < proj_n, 0.0, prod), axis=1, keepdims=True)
        c_n = None
        if turn == 0:
            diag_row = jnp.where(lane64 == row64, mix_re, jnp.where(lane64 == row64 + proj_n, mix_im, 0.0))
            c_n = jnp.sum(jnp.sum(diag_row, axis=0, keepdims=True) * tot, axis=1, keepdims=True)
        for k in range(tiles):
            lanes = slice(k * 128, k * 128 + 128)
            p_re, p_im = pj[0, :, lanes], pj[1, :, lanes]
            n_re = jnp.sum(p_re * mix_re - p_im * mix_im, axis=0, keepdims=True)
            n_im = jnp.sum(p_im * mix_re + p_re * mix_im, axis=0, keepdims=True)
            hvec[:, lanes] = jnp.concatenate([n_re, n_im], axis=0) + kin_ref[:, lanes] * v[:, lanes]
        for h in range(2):
            lot = 4 * turn + 2 + h
            wait_exchange(lot)
            rest = got_rows(lot, 6)
            left, right = [], []
            for c in range(2):
                mains = [got_rows(lot, c * planes + i) for i in range(planes)]
                for j in range(planes):
                    pieces = []
                    for i in range(planes):
                        piece = moved_by(mains[i], base[i] - 48 * j)
                        if j == 2:
                            late = moved_by(rest, base[i] + 32 - 16 * (c * planes + i))
                            piece = jnp.where(lane32 < base[i] + 32, piece, late)
                        pieces.append(piece)
                    left.append(jnp.where(lane32 < 48, pieces[0], pieces[1]))
                    right.append(pieces[2])
            left, right = jnp.concatenate(left, axis=0).T, jnp.concatenate(right, axis=0).T
            hi, lo = split(jnp.concatenate([left[:grid_len], right[:half_len]], axis=0))
            rows = hi.shape[0]
            out = dot(jnp.concatenate([hi, lo], axis=0), tabs[3, : 2 * grid_len])
            out = out[:rows] + out[rows:] + dot(hi, tabs[3, 2 * grid_len :])
            for c in range(2):
                first, second, third = [out[i * half_len : (i + 1) * half_len, c * 128 : c * 128 + 128] for i in range(planes)]
                late = roll(third, 64)
                rows = slice(c * half_len, (c + 1) * half_len)
                rows_lo = slice((2 + c) * half_len, (3 + c) * half_len)
                wide = lane < 96
                hi, lo = split(jnp.concatenate([jnp.where(wide, first, roll(third, 96)), jnp.where(wide, second, late)], axis=1))
                gt[h, rows, :] = hi
                gt[h, rows_lo, :] = lo
                high = late.astype(BF16).astype(F32)
                gt_rest[h, rows, :] = jnp.where(lane < 32, high, roll(late - high, 32)).astype(BF16)
            for k in range(0, pw, 256):
                lanes = slice(k, k + 256)
                q = dot(gt[h], at_g[:256, lanes])
                q = q[:grid_len] + q[grid_len:] + dot(gt_rest[h, :, :64], at_g[256:, lanes])
                q_re, q_im = q[:half_len], q[half_len:]
                e_c = e_tab[h * grid_len : h * grid_len + half_len, lanes]
                e_s = e_tab[h * grid_len + half_len : (h + 1) * grid_len, lanes]
                l_re = jnp.sum(e_c * q_re + e_s * q_im, axis=0, keepdims=True)
                l_im = jnp.sum(e_c * q_im - e_s * q_re, axis=0, keepdims=True)
                hvec[:, lanes] = hvec[:, lanes] + jnp.concatenate([l_re, l_im], axis=0)
        return c_n

    def precondition(r, level):
        ratio = kin_ref[...] / (1.5 * level + 1.0)
        numer = 27.0 + ratio * (18.0 + ratio * (12.0 + 8.0 * ratio))
        square = ratio * ratio
        return r * (numer / (numer + 16.0 * square * square))

    eps = small_eps

    loads[2].wait()
    vecs[0] = jnp.concatenate([cf[0], cf[1]], axis=0)
    c_n = apply_h(0, vecs[0])
    tot = jnp.sum(got_rows(2, 7) + got_rows(3, 7), axis=0, keepdims=True) * (1.0 / total_pw)
    guess_cc = cell(tot, 0)
    guess = (cell(tot, 1) + cell(tot, 2) * (1.0 / grid_len**3) + c_n) / (guess_cc + eps)
    c = vecs[0]
    h0 = hvec[...]
    s = h0 - guess * c
    kc, ks = kin_ref[...] * c, kin_ref[...] * s
    tot = all_sums(0, [fold(c * c), fold(c * s), fold(s * s), fold(kc * c), fold(kc * s), fold(ks * s)])
    cc, cs, ss, kcc, kcs, kss = [cell(tot, n) for n in range(6)]
    shift = (cs - guess * eps) / (cc + eps)
    e0 = guess + shift
    r0 = s - shift * c
    rr = ss - 2.0 * shift * cs + shift * shift * cc
    krr = kss - 2.0 * shift * kcs + shift * shift * kcc
    rc = cs - shift * cc
    krc = kcs - shift * kcc
    p0 = precondition(r0, krr / (rr + eps))
    vecs[1] = r0
    vecs[2] = p0
    vecs[3] = h0

    apply_h(1, vecs[2])
    c, r0, p0, h0 = vecs[0], vecs[1], vecs[2], vecs[3]
    g0 = hvec[...]
    q0 = g0 - e0 * p0
    pairs = [(r0, q0), (r0, p0), (q0, q0), (q0, c), (q0, p0), (c, p0), (p0, p0)]
    prods = [a * b for a, b in pairs]
    tot = all_sums(1, [fold(x) for x in prods] + [fold(x * kin_ref[...]) for x in prods])
    rq, rp, qq, qc, qp, cp, pp = [cell(tot, n) for n in range(7)]
    krq, krp, kqq, kqc, kqp, kcp, kpp = [cell(tot, n) for n in range(7, 14)]
    l0 = -rq / (qq + eps)
    bb = cc + 2.0 * l0 * cp + l0 * l0 * pp
    b_rho = rc + l0 * (qc + rp) + l0 * l0 * qp
    d1 = (b_rho - e0 * eps) / (bb + eps)
    fa, fb, fc = -l0, d1, d1 * l0
    r_dr = fa * rq + fb * rc + fc * rp
    dr_dr = fa * fa * qq + fb * fb * cc + fc * fc * pp + 2.0 * (fa * fb * qc + fa * fc * qp + fb * fc * cp)
    kr_dr = fa * krq + fb * krc + fc * krp
    kdr_dr = fa * fa * kqq + fb * fb * kcc + fc * fc * kpp + 2.0 * (fa * fb * kqc + fa * fc * kqp + fb * fc * kcp)
    wt = r_dr / (dr_dr + eps)
    lm = wt * l0
    bmbm = cc + 2.0 * lm * cp + lm * lm * pp
    bm_rho = rc + lm * (qc + rp) + lm * lm * qp
    dm = (bm_rho - e0 * eps) / (bmbm + eps)
    em = e0 + dm
    mm = rr - 2.0 * wt * r_dr + wt * wt * dr_dr
    kmm = krr - 2.0 * wt * kr_dr + wt * wt * kdr_dr
    bm = c + lm * p0
    hm = h0 + lm * g0
    rm = r0 - wt * (fa * q0 + fb * c + fc * p0)
    sm = r0 + lm * q0 - dm * bm
    p1 = precondition(rm, kmm / (mm + eps))
    vecs[4] = bm
    vecs[5] = hm
    vecs[6] = rm
    vecs[7] = sm
    vecs[8] = p1
    bands[my_band] = jnp.concatenate([bm, p1], axis=0)

    apply_h(2, vecs[8])
    bm, hm, rm, sm, p1 = vecs[4], vecs[5], vecs[6], vecs[7], vecs[8]
    g1 = hvec[...]
    q1 = g1 - em * p1
    start_sums(2, as_row([fold(rm * q1), fold(q1 * q1)]))
    span = bands.at[pl.ds(0, band_n - 1)]
    pltpu.make_async_remote_copy(
        src_ref=span, dst_ref=span, send_sem=send_sem.at[19], recv_sem=recv_sem.at[19],
        device_id={"band": other_bands[0]}, device_id_type=MESH,
    ).wait()
    left = jnp.concatenate([bm, p1, hm, g1], axis=0)
    gram = dot_full(left, jnp.concatenate([bands[j] for j in range(band_n)], axis=0), NT)
    wide = (band_n * 4, 128)
    moved = iota(wide, 0) % 4 * band_n + iota(wide, 0) // 4
    gram = dot_full(gram, jnp.where(moved == iota(wide, 1), 1.0, 0.0))
    pairs = [(sm, sm), (sm, q1), (sm, bm), (sm, p1), (q1, bm), (q1, p1), (bm, bm), (bm, p1), (p1, p1)]
    row = as_row([fold(a * b) for a, b in pairs])
    gram_send[:8, :] = gram
    gram_send[8:9, :] = row
    spread_rows(gram_send, gram_recv, 18)
    gram_recv[me] = gram_send[...]
    tot = end_sums(2)
    rq, qq = cell(tot, 0), cell(tot, 1)
    l1 = -rq / (qq + eps)
    lam_send[...] = jnp.broadcast_to(l1, (1, 128))
    spread_band(lam_send, lam_recv.at[my_band], 20)
    lam_recv[my_band] = lam_send[...]
    wait_rows(gram_recv, 18, ga_n - 1, "ga", ga_n, me)
    summed = jnp.sum(gram_recv[...], axis=0) * (1.0 / total_pw)
    gram, tot = summed[:8], summed[8:9]
    ss, sq, sb, sp, qb, qp, bb, bp, pp = [cell(tot, n) for n in range(9)]

    new = bm + l1 * p1
    nb_out[0] = new[0:1]
    nb_out[1] = new[1:2]
    nn = bb + 2.0 * l1 * bp + l1 * l1 * pp
    n_sig = sb + l1 * (sp + qb) + l1 * l1 * qp
    sig_sig = ss + 2.0 * l1 * sq + l1 * l1 * qq
    shift = (n_sig - em * eps) / (nn + eps)
    energy = em + shift
    res = (sig_sig - 2.0 * shift * n_sig + shift * shift * nn) / (nn + eps)

    wait_rows(lam_recv, 20, band_n - 1, "band", band_n, my_band)
    lams = jnp.zeros((1, 128), F32)
    for j in range(band_n):
        lams = jnp.where(lane == j, lam_recv[j], lams)

    def part(rows, v):
        return rows[:, v * band_n : (v + 1) * band_n]

    lam8 = lams[:, :band_n]

    def finish(rows):
        a = rows[0:2] + l1 * rows[2:4]
        against_re = part(a, 0) + lam8 * part(a, 2)
        against_im = part(a, 1) + lam8 * part(a, 3)
        return (against_re[0:1] + against_im[1:2], against_im[0:1] - against_re[1:2])

    cor_re, cor_im = finish(gram[0:4])
    sub_re, sub_im = finish(gram[4:8])
    tail = jnp.concatenate([jnp.broadcast_to(energy, (1, band_n)), jnp.broadcast_to(res, (1, band_n))], axis=0)
    block = jnp.concatenate([cor_re, cor_im, sub_re, sub_im, tail, tail], axis=0)
    small_out[...] = jnp.concatenate([block, jnp.zeros((8, 128 - band_n), F32)], axis=1)


def body(tables, coeffs, cell_map, potential, projectors, strengths, proj_atom, proj_chan):
    ga_n = lax.axis_size("ga")
    band_n = lax.axis_size("band")
    grid_len = potential.shape[0]
    pw = coeffs.shape[2]
    proj_n = proj_atom.shape[0]
    total_pw = pw * ga_n
    vmem = pl.BlockSpec(memory_space=pltpu.VMEM)
    hbm = pl.BlockSpec(memory_space=pltpu.HBM)
    z_tab, tabs = tables
    args = (cell_map.reshape(pw // 128, 128), z_tab, coeffs, tabs, projectors, jnp.transpose(potential, (1, 0, 2)),
            strengths, proj_atom.reshape(1, proj_n), proj_chan.reshape(1, proj_n))
    V = pltpu.VMEM
    scratch = [V(a.shape, a.dtype) for a in args] + [
        V((pw, 3 * 128), BF16), V((320, pw), BF16), V((2 * grid_len, pw), F32),
        V((2, 2 * grid_len, 256), BF16), V((2, grid_len, 128), BF16), V((2, grid_len, 256), F32),
        V((proj_n, 2 * proj_n), F32), V((9, 2, pw), F32), V((2, pw), F32), V((1, pw), F32),
        V((12, ga_n * 8, 128), F32), V((12, ga_n * 8, 128), F32),
        V((6, 1, 128), F32), V((6, ga_n, 1, 128), F32),
        V((9, 128), F32), V((ga_n, 9, 128), F32),
        V((band_n, 4, pw), F32), V((1, 128), F32), V((band_n, 1, 128), F32),
        pltpu.SemaphoreType.DMA((21,)), pltpu.SemaphoreType.DMA((21,)), pltpu.SemaphoreType.DMA((len(args),)),
    ]
    args = [pltpu.with_memory_space_constraint(a, pltpu.HBM) for a in args]
    new_bands, small = pl.pallas_call(
        functools.partial(kernel, (ga_n, band_n, grid_len, total_pw)),
        out_shape=(
            jax.ShapeDtypeStruct((2, 1, pw), F32),
            jax.ShapeDtypeStruct((8, 128), F32),
        ),
        in_specs=[hbm] * len(args),
        out_specs=(vmem, vmem),
        scratch_shapes=scratch,
        compiler_params=pltpu.CompilerParams(collective_id=0, has_side_effects=True, vmem_limit_bytes=24 * 2**20),
    )(*args)

    def deal(nb, sm, nb_o, en_o, re_o, co_o, su_o):
        nb_o[...] = nb[...]
        co_o[0], co_o[1] = sm[0:1, :band_n], sm[1:2, :band_n]
        su_o[0], su_o[1] = sm[2:3, :band_n], sm[3:4, :band_n]
        en_o[...] = sm[4:5, :1]
        re_o[...] = sm[5:6, :1]

    one = jax.ShapeDtypeStruct((1, 1), F32)
    rows = jax.ShapeDtypeStruct((2, 1, band_n), F32)
    new_bands, energy, res, corr, sub = pl.pallas_call(
        deal,
        out_shape=(jax.ShapeDtypeStruct((2, 1, pw), F32), one, one, rows, rows),
        in_specs=[vmem] * 2,
        out_specs=(vmem,) * 5,
        compiler_params=pltpu.CompilerParams(vmem_limit_bytes=2**20),
    )(new_bands, small)
    return new_bands, energy.reshape(1), res.reshape(1), corr, sub


def solution(mesh):
    tables = make_tables(96, mesh.shape["ga"])
    placed = (P(None, "band", "ga"), P("ga"), P(None, "ga", None), P(None, None, "ga"), P(), P(), P())
    return jax.shard_map(
        functools.partial(body, tables),
        mesh=mesh,
        in_specs=placed,
        out_specs=(P(None, "band", "ga"), P("band"), P("band"), P(None, "band", None), P(None, "band", None)),
        check_vma=False,
    )
```

```python
import functools

import jax
import jax.numpy as jnp
import numpy as np
from jax import lax
from jax.experimental import pallas as pl
from jax.experimental.pallas import tpu as pltpu
from jax.sharding import PartitionSpec as P

F32 = jnp.float32
BF16 = jnp.bfloat16
HOT = jnp.float8_e4m3fn
HIGHEST = lax.Precision.HIGHEST
MESH = pl.DeviceIdType.MESH
kin_unit = 0.02
small_eps = 1e-06

NN = (((1,), (0,)), ((), ()))
NT = (((1,), (1,)), ((), ()))
TN = (((0,), (0,)), ((), ()))


def parts_of(table, count):
    out = []
    left = np.asarray(table, np.float64)
    for _ in range(count):
        piece = left.astype(np.float32).astype(BF16)
        out.append(piece)
        left = left - piece.astype(np.float64)
    return out


def make_tables(grid_len, groups):
    planes = grid_len // groups
    natural = np.arange(grid_len)
    slab = (natural % groups) * planes + natural // groups

    def angles(rows, cols):
        return 2.0 * np.pi / grid_len * ((rows[:, None] * cols[None, :]) % grid_len)

    z_ang = angles(natural, natural)
    x_cos, x_sin = np.cos(z_ang), np.sin(z_ang)
    half = grid_len // 2
    z_high, z_low = parts_of(np.concatenate([x_cos[:half], x_sin[:half], x_cos[half:], x_sin[half:]], axis=0), 2)
    y_ang = angles(slab, natural)
    y_cos, y_sin = np.cos(y_ang), np.sin(y_ang)
    pad = np.zeros((grid_len, 128 - grid_len))
    side = np.zeros((2 * grid_len, 256 - 2 * grid_len))
    y_fwd = np.block([[y_cos, pad, -y_sin, pad], [y_sin, pad, y_cos, pad]])
    x_fwd = np.block([[x_cos, -x_sin], [x_sin, x_cos]])
    x_back = np.block([[x_cos, x_sin], [-x_sin, x_cos]]) / grid_len
    x_fwd, x_back = np.concatenate([x_fwd, side], axis=1), np.concatenate([x_back, side], axis=1)
    y_back = y_fwd / grid_len**2
    rest = []
    for tab in (y_fwd, x_fwd, x_back, y_back):
        rest.append(np.concatenate(parts_of(tab, 2), axis=0))
    return [np.concatenate([z_high, z_low], axis=1), np.stack(rest)]


def dot(a, b, dims=NN):
    return lax.dot_general(a, b, dims, preferred_element_type=F32)


def dot_full(a, b, dims=NN):
    return lax.dot_general(a, b, dims, precision=HIGHEST, preferred_element_type=F32)


def dot_tab(tab, hi, lo, dims=NN):
    rows = tab.shape[0] // 2
    both = dot(tab, hi, dims)
    return both[:rows] + both[rows:] + dot(tab[:rows], lo, dims)


def split(x):
    hi = x.astype(BF16)
    return hi, (x - hi.astype(F32)).astype(BF16)


def iota(shape, axis):
    return lax.broadcasted_iota(jnp.int32, shape, axis)


def hops(k):
    return min(k, 4 - k)


def far_first():
    steps = [(i, j) for i in range(4) for j in range(4) if (i, j) != (0, 0)]
    return [[s for s in steps if hops(s[0]) + hops(s[1]) == far] for far in (4, 3, 2, 1)]


def kernel(sizes, cm_far, zt_far, cf_far, tabs_far, pj_far, pot_far, st_far, pa_far, pc_far,
           nb_out, small_out,
           cm, zt, cf, tabs, pj, pot, st, pa, pc, at_s, at_g, e_tab, gt, gt_rest, v_tab, coup, vecs, hvec, kin_ref,
           send, recv, row_send, row_recv, gram_send, gram_recv, bands, lam_send, lam_recv,
           send_sem, recv_sem, load_sem):
    ga_n, band_n, grid_len, total_pw = sizes
    planes = grid_len // ga_n
    me = lax.axis_index("ga")
    my_band = lax.axis_index("band")
    pw = cf.shape[2]
    tiles = pw // 128
    far = (cm_far, zt_far, cf_far, tabs_far, pj_far, pot_far, st_far, pa_far, pc_far)
    near = (cm, zt, cf, tabs, pj, pot, st, pa, pc)
    loads = [pltpu.make_async_copy(a, b, load_sem.at[n]) for n, (a, b) in enumerate(zip(far, near))]
    loads[0].start()
    loads[1].start()

    barrier = pltpu.get_barrier_semaphore()
    m_x, m_y, m_c = me // 8, me // 2 % 4, me % 2

    others = []
    for group in far_first():
        for core in (0, 1):
            others += [((m_x + i) % 4) * 8 + ((m_y + j) % 4) * 2 + core for i, j in group]
    others.append(m_x * 8 + m_y * 2 + 1 - m_c)
    band_order = sorted(range(1, band_n), key=lambda k: -min(k, band_n - k))
    other_bands = [lax.rem(my_band + k, band_n) for k in band_order]

    for other in others:
        pl.semaphore_signal(barrier, inc=1, device_id={"ga": other}, device_id_type=MESH)
    for other in other_bands:
        pl.semaphore_signal(barrier, inc=1, device_id={"band": other}, device_id_type=MESH)

    for load in loads[2:]:
        load.start()
    zeros = jnp.zeros((ga_n, 128), F32)
    for lot in range(12):
        send[lot, pl.ds(7, ga_n, stride=8), :] = zeros
    loads[0].wait()
    loads[1].wait()

    cells = cm[...]
    py = lax.shift_right_logical(cells * 43691, 22)
    z_idx = cells - py * grid_len
    plane = (py >= grid_len).astype(jnp.int32) + (py >= 2 * grid_len).astype(jnp.int32)
    y_idx = py - plane * grid_len
    x_idx = me + ga_n * plane
    py_pad = plane * 128 + y_idx

    def freq(k):
        return jnp.where(2 * k < grid_len, k, k - grid_len).astype(F32)

    kin = kin_unit * (freq(x_idx) * freq(x_idx) + freq(y_idx) * freq(y_idx) + freq(z_idx) * freq(z_idx))
    for k in range(tiles):
        lanes = slice(k * 128, k * 128 + 128)
        kin_ref[:, lanes] = kin[k : k + 1]
    for k in range(0, tiles, 2):
        row = jnp.concatenate([z_idx[k : k + 1], z_idx[k + 1 : k + 2]], axis=1)
        hot = jnp.where(iota((grid_len, 256), 0) == row, 1.0, 0.0).astype(BF16)
        e_tab[:, k * 128 : k * 128 + 256] = dot(zt[...], jnp.concatenate([hot, hot], axis=0))
    upright = jnp.transpose(jnp.concatenate([py_pad, jnp.zeros((128 - tiles, 128), jnp.int32)], axis=0))
    for k in range(tiles):
        hot = (iota((128, 3 * 128), 1) == upright[:, k : k + 1])
        at_s[k * 128 : k * 128 + 128, :] = jnp.where(hot, 1.0, 0.0).astype(BF16)
    half_len = grid_len // 2

    def later_tables():
        for load in loads[5:]:
            load.wait()
        blank = jnp.zeros((grid_len, 128 - grid_len), F32)
        at = iota((grid_len, 128), 1)
        slabs = [jnp.concatenate([pot[j], blank], axis=1) for j in range(planes)]
        for h in range(2):
            first, second, third = [moved_by(slabs[j], 48 * j - 48 * h) for j in range(planes)]
            v_tab[h, :, :128] = jnp.where(at < 48, first, jnp.where(at < 96, second, third))
            v_tab[h, :, 128:] = jnp.where(at < 16, moved_by(slabs[2], -48 * h - 32), 0.0)
        place = jnp.where(plane == 2, jnp.where(y_idx < 32, 96 + y_idx, 192 + y_idx), plane * 128 + y_idx)
        for k in range(tiles):
            lanes = slice(k * 128, k * 128 + 128)
            hot = jnp.where(iota((288, 128), 0) == place[k : k + 1], 1.0, 0.0).astype(HOT)
            at_g[:288, lanes] = hot
            at_g[288:, lanes] = hot[256:]
        chans = st.shape[1]
        sym_rows = st[...].reshape(st.shape[0] * chans, chans)
        slot = pa[...] * chans + pc[...]
        hot_p = jnp.where(iota((proj_n, proj_n), 0) == slot, 1.0, 0.0)
        hot_c = jnp.where(iota((chans, proj_n), 0) == pc[...], 1.0, 0.0)
        reach = dot_full(sym_rows, hot_c)
        reach = jnp.where(iota((proj_n, proj_n), 0) // chans == pa[...], reach, 0.0)
        half = 0.5 * (dot_full(hot_p, reach, TN) + dot_full(reach, hot_p, TN))
        coup[...] = jnp.concatenate([half, half], axis=1)

    proj_n = pa.shape[1]
    lane = iota((1, 128), 1)
    lane32 = iota((ga_n, 128), 1)

    def roll(x, by):
        return pltpu.roll(x, by, 1)

    lane16 = lane32 // 16

    def gather_rest(pieces):
        rest = pieces[0]
        for n in range(1, 6):
            rest = jnp.where(lane16 == n, roll(pieces[n], 16 * n), rest)
        return rest

    def moved_by(x, by):
        return x if by % 128 == 0 else roll(x, by % 128)

    def put(lot, row, value):
        send[lot, pl.ds(row, ga_n, stride=8), :] = value

    def exchange(lot, start=0, stop=ga_n - 1):
        rows = 8 if lot in (2, 3) else 7
        mine = pl.ds(pl.multiple_of(me * 8, 8), rows)
        for other in others[start:stop]:
            pltpu.make_async_remote_copy(
                src_ref=send.at[lot, pl.ds(pl.multiple_of(other * 8, 8), rows), :],
                dst_ref=recv.at[lot, mine, :],
                send_sem=send_sem.at[lot],
                recv_sem=recv_sem.at[lot],
                device_id={"ga": other},
                device_id_type=MESH,
            ).start()
        if stop == ga_n - 1:
            recv[lot, mine, :] = send[lot, mine, :]

    def wait_exchange(lot):
        span = pl.ds(0, (ga_n - 1) * (8 if lot in (2, 3) else 7))
        pltpu.make_async_remote_copy(
            src_ref=send.at[lot, span, :],
            dst_ref=recv.at[lot, span, :],
            send_sem=send_sem.at[lot],
            recv_sem=recv_sem.at[lot],
            device_id={"ga": others[0]},
            device_id_type=MESH,
        ).wait()

    def got_rows(lot, row):
        return recv[lot, pl.ds(row, ga_n, stride=8), :]

    def spread_rows(ref_send, ref_recv, sem):
        for other in others:
            pltpu.make_async_remote_copy(
                src_ref=ref_send, dst_ref=ref_recv.at[me], send_sem=send_sem.at[sem], recv_sem=recv_sem.at[sem],
                device_id={"ga": other}, device_id_type=MESH,
            ).start()

    def spread_band(ref_send, ref_recv, sem):
        for other in other_bands:
            pltpu.make_async_remote_copy(
                src_ref=ref_send, dst_ref=ref_recv, send_sem=send_sem.at[sem], recv_sem=recv_sem.at[sem],
                device_id={"band": other}, device_id_type=MESH,
            ).start()

    def wait_rows(ref_recv, sem, count, axis, size, mine):
        span = ref_recv.at[pl.ds(0, count)]
        pltpu.make_async_remote_copy(
            src_ref=span, dst_ref=span, send_sem=send_sem.at[sem], recv_sem=recv_sem.at[sem],
            device_id={axis: lax.rem(mine + 1, size)}, device_id_type=MESH,
        ).wait()

    def cell(row, at):
        return jnp.sum(jnp.where(lane == at, row, 0.0), axis=1, keepdims=True)

    def fold(x):
        total = x[:, :128]
        for k in range(1, tiles):
            total = total + x[:, k * 128 : k * 128 + 128]
        return total[0:1] + total[1:2]

    def as_row(folded):
        stack = jnp.concatenate(folded + [jnp.zeros((1, 128), F32)] * (-len(folded) % 8), axis=0)
        col = jnp.sum(stack, axis=1, keepdims=True)
        hit = iota(stack.shape, 0) == iota(stack.shape, 1)
        return jnp.sum(jnp.where(hit, col, 0.0), axis=0, keepdims=True)

    def start_sums(which, row):
        row_send[which] = row
        spread_rows(row_send.at[which], row_recv.at[which], 12 + which)
        row_recv[which, me] = row_send[which]

    def end_sums(which):
        wait_rows(row_recv.at[which], 12 + which, ga_n - 1, "ga", ga_n, me)
        return jnp.sum(row_recv[which], axis=0) * (1.0 / total_pw)

    def all_sums(which, folded):
        start_sums(which, as_row(folded))
        total = end_sums(which)
        return total

    def apply_h(turn, v):
        base = (0, 48, 0)

        def onto_grid(h, sent=None):
            t_all = None
            for k in range(0, pw, 256):
                lanes = slice(k, k + 256)
                e_c = e_tab[h * grid_len : h * grid_len + half_len, lanes]
                e_s = e_tab[h * grid_len + half_len : (h + 1) * grid_len, lanes]
                v_re, v_im = v[0:1, lanes], v[1:2, lanes]
                hi_re, lo_re = split(e_c * v_re - e_s * v_im)
                hi_im, lo_im = split(e_s * v_re + e_c * v_im)
                got = dot(jnp.concatenate([hi_re, hi_im, lo_re, lo_im], axis=0), at_s[lanes, :])
                t_all = got if t_all is None else t_all + got
                if sent is not None and sent < ga_n - 1:
                    exchange(4 * turn, sent, min(sent + 3, ga_n - 1))
                    sent += 3
            return t_all

        def along_y(h, t_all):
            if turn == 0 and h == 0:
                loads[3].wait()
            t_all = t_all[:grid_len] + t_all[grid_len:]
            rows = []
            for i in range(planes):
                lanes = slice(i * 128, i * 128 + 128)
                rows.append(jnp.concatenate([t_all[:half_len, lanes], t_all[half_len:, lanes]], axis=1))
            rows.insert(2, jnp.zeros((32, 256), F32))
            hi, lo = split(jnp.concatenate(rows, axis=0))
            u = dot_tab(tabs[0], hi, lo, NT)
            u = (u[:, :128], u[:, 128:])
            rest = []
            for c in range(2):
                for i in range(planes):
                    spread = []
                    for j in range(planes):
                        at = c * grid_len + j * ga_n
                        piece = u[i // 2][at : at + ga_n]
                        if i == 2:
                            piece = jnp.concatenate([piece, jnp.zeros((ga_n, 128 - half_len), F32)], axis=1)
                        spread.append(moved_by(piece, 48 * j - base[i]))
                    put(4 * turn + h, c * planes + i,
                        jnp.where(lane32 < 48, spread[0], jnp.where(lane32 < 96, spread[1], spread[2])))
                    rest.append(spread[2])
            put(4 * turn + h, 6, gather_rest(rest))

        first = onto_grid(0)
        along_y(0, first)
        if turn == 0:
            pl.semaphore_wait(barrier, ga_n - 1 + band_n - 1)
        exchange(4 * turn, 0, 10)
        second = onto_grid(1, 10)
        along_y(1, second)
        exchange(4 * turn + 1)

        if turn == 0:
            loads[4].wait()
        acc_re = jnp.zeros((proj_n, 128), F32)
        acc_im = jnp.zeros((proj_n, 128), F32)
        for k in range(tiles):
            lanes = slice(k * 128, k * 128 + 128)
            p_re, p_im = pj[0, :, lanes], pj[1, :, lanes]
            v_re, v_im = v[0:1, lanes], v[1:2, lanes]
            acc_re = acc_re + (p_re * v_re + p_im * v_im)
            acc_im = acc_im + (p_re * v_im - p_im * v_re)
        col_re = jnp.sum(acc_re, axis=1, keepdims=True)
        col_im = jnp.sum(acc_im, axis=1, keepdims=True)
        row64, lane64 = iota((proj_n, 128), 0), iota((proj_n, 128), 1)
        diag = jnp.where(lane64 == row64, col_re, jnp.where(lane64 == row64 + proj_n, col_im, 0.0))
        start_sums(3 + turn, jnp.sum(diag, axis=0, keepdims=True))
        norm_row = None
        if turn == 0:
            norm_row = as_row([fold(v * v), fold(v * v * kin_ref[...])])
            later_tables()
        if turn == 2:
            spread_band(bands.at[my_band], bands.at[my_band], 19)
        for h in range(2):
            lot = 4 * turn + h
            wait_exchange(lot)
            rest = got_rows(lot, 6)
            main = jnp.concatenate([got_rows(lot, n) for n in range(6)], axis=0)
            side = jnp.concatenate([moved_by(rest, -16 * n) for n in range(6)], axis=0)
            hi, lo = split(jnp.concatenate([main, side], axis=1))
            w = dot_tab(tabs[1, :, : 2 * grid_len], hi, lo)
            w_re, w_im = w[:grid_len], w[grid_len:]
            vw_re, vw_im = v_tab[h] * w_re, v_tab[h] * w_im
            lot = 4 * turn + 2 + h
            if turn == 0:
                dens = jnp.sum(vw_re * w_re + vw_im * w_im, axis=0, keepdims=True)
                dens = jnp.sum(dens[:, :128] + dens[:, 128:], axis=1, keepdims=True)
                row = norm_row if h == 0 else jnp.zeros((1, 128), F32)
                put(lot, 7, jnp.broadcast_to(jnp.where(lane == 2, dens, row), (ga_n, 128)))
            hi, lo = split(jnp.concatenate([vw_re, vw_im], axis=0))
            back = dot_tab(tabs[2, :, : 2 * grid_len], hi, lo)
            for n in range(6):
                put(lot, n, back[n * ga_n : (n + 1) * ga_n, :128])
            put(lot, 6, gather_rest([back[n * ga_n : (n + 1) * ga_n, 128:] for n in range(6)]))
            exchange(lot)

        tot = end_sums(3 + turn)
        prod = coup[...] * tot
        mix_re = jnp.sum(jnp.where(lane64 < proj_n, prod, 0.0), axis=1, keepdims=True)
        mix_im = jnp.sum(jnp.where(lane64 < proj_n, 0.0, prod), axis=1, keepdims=True)
        c_n = None
        if turn == 0:
            diag_row = jnp.where(lane64 == row64, mix_re, jnp.where(lane64 == row64 + proj_n, mix_im, 0.0))
            c_n = jnp.sum(jnp.sum(diag_row, axis=0, keepdims=True) * tot, axis=1, keepdims=True)
        for k in range(tiles):
            lanes = slice(k * 128, k * 128 + 128)
            p_re, p_im = pj[0, :, lanes], pj[1, :, lanes]
            n_re = jnp.sum(p_re * mix_re - p_im * mix_im, axis=0, keepdims=True)
            n_im = jnp.sum(p_im * mix_re + p_re * mix_im, axis=0, keepdims=True)
            hvec[:, lanes] = jnp.concatenate([n_re, n_im], axis=0) + kin_ref[:, lanes] * v[:, lanes]
        for h in range(2):
            lot = 4 * turn + 2 + h
            wait_exchange(lot)
            rest = got_rows(lot, 6)
            left, right = [], []
            for c in range(2):
                mains = [got_rows(lot, c * planes + i) for i in range(planes)]
                for j in range(planes):
                    pieces = []
                    for i in range(planes):
                        piece = moved_by(mains[i], base[i] - 48 * j)
                        if j == 2:
                            late = moved_by(rest, base[i] + 32 - 16 * (c * planes + i))
                            piece = jnp.where(lane32 < base[i] + 32, piece, late)
                        pieces.append(piece)
                    left.append(jnp.where(lane32 < 48, pieces[0], pieces[1]))
                    right.append(pieces[2])
            left, right = jnp.concatenate(left, axis=0).T, jnp.concatenate(right, axis=0).T
            hi, lo = split(jnp.concatenate([left[:grid_len], right[:half_len]], axis=0))
            rows = hi.shape[0]
            out = dot(jnp.concatenate([hi, lo], axis=0), tabs[3, : 2 * grid_len])
            out = out[:rows] + out[rows:] + dot(hi, tabs[3, 2 * grid_len :])
            for c in range(2):
                first, second, third = [out[i * half_len : (i + 1) * half_len, c * 128 : c * 128 + 128] for i in range(planes)]
                late = roll(third, 64)
                rows = slice(c * half_len, (c + 1) * half_len)
                rows_lo = slice((2 + c) * half_len, (3 + c) * half_len)
                wide = lane < 96
                hi, lo = split(jnp.concatenate([jnp.where(wide, first, roll(third, 96)), jnp.where(wide, second, late)], axis=1))
                gt[h, rows, :] = hi
                gt[h, rows_lo, :] = lo
                high = late.astype(BF16).astype(F32)
                gt_rest[h, rows, :] = jnp.where(lane < 32, high, roll(late - high, 32)).astype(BF16)
            for k in range(0, pw, 256):
                lanes = slice(k, k + 256)
                q = dot(gt[h], at_g[:256, lanes])
                q = q[:grid_len] + q[grid_len:] + dot(gt_rest[h, :, :64], at_g[256:, lanes])
                q_re, q_im = q[:half_len], q[half_len:]
                e_c = e_tab[h * grid_len : h * grid_len + half_len, lanes]
                e_s = e_tab[h * grid_len + half_len : (h + 1) * grid_len, lanes]
                l_re = jnp.sum(e_c * q_re + e_s * q_im, axis=0, keepdims=True)
                l_im = jnp.sum(e_c * q_im - e_s * q_re, axis=0, keepdims=True)
                hvec[:, lanes] = hvec[:, lanes] + jnp.concatenate([l_re, l_im], axis=0)
        return c_n

    def precondition(r, level):
        ratio = kin_ref[...] / (1.5 * level + 1.0)
        numer = 27.0 + ratio * (18.0 + ratio * (12.0 + 8.0 * ratio))
        square = ratio * ratio
        return r * (numer / (numer + 16.0 * square * square))

    eps = small_eps

    loads[2].wait()
    vecs[0] = jnp.concatenate([cf[0], cf[1]], axis=0)
    c_n = apply_h(0, vecs[0])
    tot = jnp.sum(got_rows(2, 7) + got_rows(3, 7), axis=0, keepdims=True) * (1.0 / total_pw)
    guess_cc = cell(tot, 0)
    guess = (cell(tot, 1) + cell(tot, 2) * (1.0 / grid_len**3) + c_n) / (guess_cc + eps)
    c = vecs[0]
    h0 = hvec[...]
    s = h0 - guess * c
    kc, ks = kin_ref[...] * c, kin_ref[...] * s
    tot = all_sums(0, [fold(c * c), fold(c * s), fold(s * s), fold(kc * c), fold(kc * s), fold(ks * s)])
    cc, cs, ss, kcc, kcs, kss = [cell(tot, n) for n in range(6)]
    shift = (cs - guess * eps) / (cc + eps)
    e0 = guess + shift
    r0 = s - shift * c
    rr = ss - 2.0 * shift * cs + shift * shift * cc
    krr = kss - 2.0 * shift * kcs + shift * shift * kcc
    rc = cs - shift * cc
    krc = kcs - shift * kcc
    p0 = precondition(r0, krr / (rr + eps))
    vecs[1] = r0
    vecs[2] = p0
    vecs[3] = h0

    apply_h(1, vecs[2])
    c, r0, p0, h0 = vecs[0], vecs[1], vecs[2], vecs[3]
    g0 = hvec[...]
    q0 = g0 - e0 * p0
    pairs = [(r0, q0), (r0, p0), (q0, q0), (q0, c), (q0, p0), (c, p0), (p0, p0)]
    prods = [a * b for a, b in pairs]
    tot = all_sums(1, [fold(x) for x in prods] + [fold(x * kin_ref[...]) for x in prods])
    rq, rp, qq, qc, qp, cp, pp = [cell(tot, n) for n in range(7)]
    krq, krp, kqq, kqc, kqp, kcp, kpp = [cell(tot, n) for n in range(7, 14)]
    l0 = -rq / (qq + eps)
    bb = cc + 2.0 * l0 * cp + l0 * l0 * pp
    b_rho = rc + l0 * (qc + rp) + l0 * l0 * qp
    d1 = (b_rho - e0 * eps) / (bb + eps)
    fa, fb, fc = -l0, d1, d1 * l0
    r_dr = fa * rq + fb * rc + fc * rp
    dr_dr = fa * fa * qq + fb * fb * cc + fc * fc * pp + 2.0 * (fa * fb * qc + fa * fc * qp + fb * fc * cp)
    kr_dr = fa * krq + fb * krc + fc * krp
    kdr_dr = fa * fa * kqq + fb * fb * kcc + fc * fc * kpp + 2.0 * (fa * fb * kqc + fa * fc * kqp + fb * fc * kcp)
    wt = r_dr / (dr_dr + eps)
    lm = wt * l0
    bmbm = cc + 2.0 * lm * cp + lm * lm * pp
    bm_rho = rc + lm * (qc + rp) + lm * lm * qp
    dm = (bm_rho - e0 * eps) / (bmbm + eps)
    em = e0 + dm
    mm = rr - 2.0 * wt * r_dr + wt * wt * dr_dr
    kmm = krr - 2.0 * wt * kr_dr + wt * wt * kdr_dr
    bm = c + lm * p0
    hm = h0 + lm * g0
    rm = r0 - wt * (fa * q0 + fb * c + fc * p0)
    sm = r0 + lm * q0 - dm * bm
    p1 = precondition(rm, kmm / (mm + eps))
    vecs[4] = bm
    vecs[5] = hm
    vecs[6] = rm
    vecs[7] = sm
    vecs[8] = p1
    bands[my_band] = jnp.concatenate([bm, p1], axis=0)

    apply_h(2, vecs[8])
    bm, hm, rm, sm, p1 = vecs[4], vecs[5], vecs[6], vecs[7], vecs[8]
    g1 = hvec[...]
    q1 = g1 - em * p1
    start_sums(2, as_row([fold(rm * q1), fold(q1 * q1)]))
    span = bands.at[pl.ds(0, band_n - 1)]
    pltpu.make_async_remote_copy(
        src_ref=span, dst_ref=span, send_sem=send_sem.at[19], recv_sem=recv_sem.at[19],
        device_id={"band": other_bands[0]}, device_id_type=MESH,
    ).wait()
    left = jnp.concatenate([bm, p1, hm, g1], axis=0)
    gram = dot_full(left, jnp.concatenate([bands[j] for j in range(band_n)], axis=0), NT)
    wide = (band_n * 4, 128)
    moved = iota(wide, 0) % 4 * band_n + iota(wide, 0) // 4
    gram = dot_full(gram, jnp.where(moved == iota(wide, 1), 1.0, 0.0))
    pairs = [(sm, sm), (sm, q1), (sm, bm), (sm, p1), (q1, bm), (q1, p1), (bm, bm), (bm, p1), (p1, p1)]
    row = as_row([fold(a * b) for a, b in pairs])
    gram_send[:8, :] = gram
    gram_send[8:9, :] = row
    spread_rows(gram_send, gram_recv, 18)
    gram_recv[me] = gram_send[...]
    tot = end_sums(2)
    rq, qq = cell(tot, 0), cell(tot, 1)
    l1 = -rq / (qq + eps)
    lam_send[...] = jnp.broadcast_to(l1, (1, 128))
    spread_band(lam_send, lam_recv.at[my_band], 20)
    lam_recv[my_band] = lam_send[...]
    wait_rows(gram_recv, 18, ga_n - 1, "ga", ga_n, me)
    summed = jnp.sum(gram_recv[...], axis=0) * (1.0 / total_pw)
    gram, tot = summed[:8], summed[8:9]
    ss, sq, sb, sp, qb, qp, bb, bp, pp = [cell(tot, n) for n in range(9)]

    new = bm + l1 * p1
    nb_out[0] = new[0:1]
    nb_out[1] = new[1:2]
    nn = bb + 2.0 * l1 * bp + l1 * l1 * pp
    n_sig = sb + l1 * (sp + qb) + l1 * l1 * qp
    sig_sig = ss + 2.0 * l1 * sq + l1 * l1 * qq
    shift = (n_sig - em * eps) / (nn + eps)
    energy = em + shift
    res = (sig_sig - 2.0 * shift * n_sig + shift * shift * nn) / (nn + eps)

    wait_rows(lam_recv, 20, band_n - 1, "band", band_n, my_band)
    lams = jnp.zeros((1, 128), F32)
    for j in range(band_n):
        lams = jnp.where(lane == j, lam_recv[j], lams)

    def part(rows, v):
        return rows[:, v * band_n : (v + 1) * band_n]

    lam8 = lams[:, :band_n]

    def finish(rows):
        a = rows[0:2] + l1 * rows[2:4]
        against_re = part(a, 0) + lam8 * part(a, 2)
        against_im = part(a, 1) + lam8 * part(a, 3)
        return (against_re[0:1] + against_im[1:2], against_im[0:1] - against_re[1:2])

    cor_re, cor_im = finish(gram[0:4])
    sub_re, sub_im = finish(gram[4:8])
    tail = jnp.concatenate([jnp.broadcast_to(energy, (1, band_n)), jnp.broadcast_to(res, (1, band_n))], axis=0)
    block = jnp.concatenate([cor_re, cor_im, sub_re, sub_im, tail, tail], axis=0)
    small_out[...] = jnp.concatenate([block, jnp.zeros((8, 128 - band_n), F32)], axis=1)


def body(tables, coeffs, cell_map, potential, projectors, strengths, proj_atom, proj_chan):
    ga_n = lax.axis_size("ga")
    band_n = lax.axis_size("band")
    grid_len = potential.shape[0]
    pw = coeffs.shape[2]
    proj_n = proj_atom.shape[0]
    total_pw = pw * ga_n
    vmem = pl.BlockSpec(memory_space=pltpu.VMEM)
    hbm = pl.BlockSpec(memory_space=pltpu.HBM)
    z_tab, tabs = tables
    args = (cell_map.reshape(pw // 128, 128), z_tab, coeffs, tabs, projectors, jnp.transpose(potential, (1, 0, 2)),
            strengths, proj_atom.reshape(1, proj_n), proj_chan.reshape(1, proj_n))
    V = pltpu.VMEM
    scratch = [V(a.shape, a.dtype) for a in args] + [
        V((pw, 3 * 128), BF16), V((320, pw), HOT), V((2 * grid_len, pw), F32),
        V((2, 2 * grid_len, 256), BF16), V((2, grid_len, 128), BF16), V((2, grid_len, 256), F32),
        V((proj_n, 2 * proj_n), F32), V((9, 2, pw), F32), V((2, pw), F32), V((1, pw), F32),
        V((12, ga_n * 8, 128), F32), V((12, ga_n * 8, 128), F32),
        V((6, 1, 128), F32), V((6, ga_n, 1, 128), F32),
        V((9, 128), F32), V((ga_n, 9, 128), F32),
        V((band_n, 4, pw), F32), V((1, 128), F32), V((band_n, 1, 128), F32),
        pltpu.SemaphoreType.DMA((21,)), pltpu.SemaphoreType.DMA((21,)), pltpu.SemaphoreType.DMA((len(args),)),
    ]
    args = [pltpu.with_memory_space_constraint(a, pltpu.HBM) for a in args]
    new_bands, small = pl.pallas_call(
        functools.partial(kernel, (ga_n, band_n, grid_len, total_pw)),
        out_shape=(
            jax.ShapeDtypeStruct((2, 1, pw), F32),
            jax.ShapeDtypeStruct((8, 128), F32),
        ),
        in_specs=[hbm] * len(args),
        out_specs=(vmem, vmem),
        scratch_shapes=scratch,
        compiler_params=pltpu.CompilerParams(collective_id=0, has_side_effects=True, vmem_limit_bytes=24 * 2**20),
    )(*args)

    def deal(nb, sm, nb_o, en_o, re_o, co_o, su_o):
        nb_o[...] = nb[...]
        co_o[0], co_o[1] = sm[0:1, :band_n], sm[1:2, :band_n]
        su_o[0], su_o[1] = sm[2:3, :band_n], sm[3:4, :band_n]
        en_o[...] = sm[4:5, :1]
        re_o[...] = sm[5:6, :1]

    one = jax.ShapeDtypeStruct((1, 1), F32)
    rows = jax.ShapeDtypeStruct((2, 1, band_n), F32)
    new_bands, energy, res, corr, sub = pl.pallas_call(
        deal,
        out_shape=(jax.ShapeDtypeStruct((2, 1, pw), F32), one, one, rows, rows),
        in_specs=[vmem] * 2,
        out_specs=(vmem,) * 5,
        compiler_params=pltpu.CompilerParams(vmem_limit_bytes=2**20),
    )(new_bands, small)
    return new_bands, energy.reshape(1), res.reshape(1), corr, sub


def solution(mesh):
    tables = make_tables(96, mesh.shape["ga"])
    placed = (P(None, "band", "ga"), P("ga"), P(None, "ga", None), P(None, None, "ga"), P(), P(), P())
    return jax.shard_map(
        functools.partial(body, tables),
        mesh=mesh,
        in_specs=placed,
        out_specs=(P(None, "band", "ga"), P("band"), P("band"), P(None, "band", None), P(None, "band", None)),
        check_vma=False,
    )
```
